256 devices in a mesh: px: 16 (over z, y_hi), py: 16 (over x, y_lo, core).
Axes of the slice: x: 4, y: 4 (y_hi: 2, y_lo: 2; y = y_hi * 2 + y_lo), z: 8, core: 2. Of those that a mesh axis runs over, the one named last changes fastest.
Arguments:
- flow_field: bfloat16 [64, 128, 128, 128], P(None, 'px', 'py'), may hold values from -6 to 6
- cotangent: bfloat16 [64, 128, 128, 128], P(None, 'px', 'py'), may hold values from -6 to 6
- tucker_core: float32 [16, 16, 8, 8, 8], replicated, may hold values from -6 to 6
- in_factor: float32 [64, 16], replicated, may hold values from -0.75 to 0.75
- out_factor: float32 [64, 16], replicated, may hold values from -1.5 to 1.5
- first_factor: float32 [32, 8], replicated, may hold values from -2 to 2
- second_factor: float32 [32, 8], replicated, may hold values from -2 to 2
- third_factor: float32 [32, 8], replicated, may hold values from -2 to 2
Outputs:
- output_field: bfloat16 [64, 128, 128, 128], P(None, 'px', 'py')
- core_grad: float32 [16, 16, 8, 8, 8], replicated
- in_grad: float32 [64, 16], replicated
- out_grad: float32 [64, 16], replicated
- first_grad: float32 [32, 8], replicated
- second_grad: float32 [32, 8], replicated
- third_grad: float32 [32, 8], replicated
The draws below stay inside these ranges and needn't reach their ends.
All inputs are finite; a program needn't handle non-finite values.
Results may differ from the reference program's by a relative error of at most 0.001.
Values sent between devices are 32-bit elements; how exact they have to be, the bound alone decides.
A program may use at most 128 MiB of HBM per device.

```python
import jax
import jax.numpy as jnp
from jax import lax

C = 64
NX = 128
NY = 128
NZ = 128
M1 = 32
M2 = 32
M3 = 32
RI = 16
RO = 16
R1 = 8
R2 = 8
R3 = 8


def block_scale(rng, extent, cuts, low, high):
    def one(position, shards_of):
        heights = jax.random.uniform(jax.random.fold_in(jax.random.fold_in(rng, 6), position), (shards_of,), jnp.float32, low / len(cuts), high / len(cuts))
        return jnp.repeat(jnp.exp(heights), extent[position] // shards_of).reshape((-1,) + (1,) * (len(extent) - position - 1))

    level = one(*cuts[0])
    for cut in cuts[1:]:
        level = level * one(*cut)
    return level


def centred(rng, shape, width, bound, pieces=(), kind=jnp.bfloat16):
    result = jax.random.normal(rng, shape, jnp.float32) * width
    if len(pieces) > 0:
        result = block_scale(rng, shape, pieces, -0.22, 0.18) * result
    return jnp.clip(result, min=-bound, max=bound).astype(kind)


def setup_inputs(seed: int = 0) -> dict:
    key_list = jax.random.split(jax.random.key(seed), 9)
    flow_field = centred(key_list[0], (C, NX, NY, NZ), 1.0, 6.0, ((1, 16), (2, 16)))
    cotangent = centred(key_list[1], (C, NX, NY, NZ), 1.0, 6.0, ((1, 16), (2, 16)))
    tucker_core = centred(key_list[2], (RI, RO, R1, R2, R3), (0.3 * ((NX * NY * NZ) // (2 * M1 * M2 * M3)) ** 0.5), 6.0, (), jnp.float32)
    in_factor = centred(key_list[3], (C, RI), C ** -0.5, 0.75, (), jnp.float32)
    out_factor = centred(key_list[4], (C, RO), RO ** -0.5, 1.5, (), jnp.float32)
    first_factor = centred(key_list[5], (M1, R1), R1 ** -0.5, 2.0, (), jnp.float32)
    second_factor = centred(key_list[6], (M2, R2), R2 ** -0.5, 2.0, (), jnp.float32)
    third_factor = centred(key_list[7], (M3, R3), R3 ** -0.5, 2.0, (), jnp.float32)
    return dict(flow_field=flow_field, cotangent=cotangent, tucker_core=tucker_core, in_factor=in_factor, out_factor=out_factor, first_factor=first_factor, second_factor=second_factor, third_factor=third_factor)


HIGHEST = lax.Precision.HIGHEST

def kept_index(count, length):
    half_count = count // 2
    return jnp.concatenate([jnp.arange(half_count), jnp.arange(length - half_count, length)]).astype(jnp.int32)

def spectrum(plane):
    whole = jnp.fft.rfftn(plane, axes=(0, 1, 2))
    rows_kept = kept_index(M1, NX)
    cols_kept = kept_index(M2, NY)
    trimmed = whole[rows_kept][:, cols_kept][:, :, :M3]
    return jnp.stack([jnp.real(trimmed), jnp.imag(trimmed)])

def to_grid(modes):
    values = modes[0] + 1j * modes[1]
    whole = jnp.zeros((NX, NY, NZ // 2 + 1), values.dtype)
    rows_kept = kept_index(M1, NX)
    cols_kept = kept_index(M2, NY)
    depth_kept = jnp.arange(M3).astype(jnp.int32)
    whole = whole.at[rows_kept[:, None, None], cols_kept[None, :, None], depth_kept[None, None, :]].set(values)
    return jnp.fft.irfftn(whole, s=(NX, NY, NZ), axes=(0, 1, 2))

def mixing(tucker_core, in_factor, out_factor, first_factor, second_factor, third_factor, spectra):
    partial_core = jnp.einsum('abrst,mt->abrsm', tucker_core, third_factor, precision=HIGHEST)
    partial_core = jnp.einsum('abrsm,ks->abrkm', partial_core, second_factor, precision=HIGHEST)
    kernel = jnp.einsum('abrkm,jr->abjkm', partial_core, first_factor, precision=HIGHEST)
    lifted = jnp.einsum('ia,ipjkm->apjkm', in_factor, spectra, precision=HIGHEST)
    mixed = jnp.einsum('abjkm,apjkm->bpjkm', kernel, lifted, precision=HIGHEST)
    return jnp.einsum('ob,bpjkm->opjkm', out_factor, mixed, precision=HIGHEST)

def reference(flow_field, cotangent, tucker_core, in_factor, out_factor, first_factor, second_factor, third_factor):
    spectra = lax.map(lambda plane: spectrum(plane.astype(jnp.float32)), flow_field)
    weights = jnp.where(jnp.arange(M3) == 0, 1.0, 2.0).astype(jnp.float32)
    inverse_count = 1.0 / (NX * NY * NZ)
    back = lax.map(lambda plane: spectrum(plane.astype(jnp.float32)), cotangent) * (weights * inverse_count)

    def forward(core_arg, in_arg, out_arg, first_arg, second_arg, third_arg):
        return mixing(core_arg, in_arg, out_arg, first_arg, second_arg, third_arg, spectra)
    joined, pullback = jax.vjp(forward, tucker_core, in_factor, out_factor, first_factor, second_factor, third_factor)
    grads = pullback(back)
    output_field = lax.map(lambda modes: to_grid(modes).astype(jnp.bfloat16), joined)
    return (output_field, grads[0], grads[1], grads[2], grads[3], grads[4], grads[5])
```

```python
import math

import jax
import jax.numpy as jnp
from jax import lax
from jax.sharding import PartitionSpec as P

NX = 128
NY = 128
NZ = 128
M1 = 32
M2 = 32
M3 = 32


HIGHEST = lax.Precision.HIGHEST


def turn_table(count, length):
    position = jnp.arange(count)
    frequency = jnp.where(position < count // 2, position, position - count)
    cells_at = jnp.arange(length)
    phase = frequency[None, :] * cells_at[:, None] % length
    angle = 2.0 * math.pi / length * phase.astype(jnp.float32)
    cosine = jnp.cos(angle)
    sine = jnp.sin(angle)
    upper = jnp.stack([cosine, -sine], axis=1)
    lower = jnp.stack([sine, cosine], axis=1)
    return jnp.stack([upper, lower])


def depth_table(length, count):
    cells_at = jnp.arange(length)
    frequency = jnp.arange(count)
    phase = cells_at[:, None] * frequency[None, :] % length
    angle = 2.0 * math.pi / length * phase.astype(jnp.float32)
    return jnp.concatenate([jnp.cos(angle), -jnp.sin(angle)], axis=1)


def to_modes(fields, depth_tables):
    across = turn_table(M2, NY)
    along = turn_table(M1, NX)
    spectra = []
    for member, z_table in zip(fields, depth_tables):
        channels, rows_here, cols_here, depth_len = member.shape
        flat = jnp.dot(
            member.reshape(-1, depth_len).astype(jnp.float32), z_table, precision=HIGHEST
        )
        spectra.append(flat.reshape(channels, rows_here, cols_here, 2, M3))
    members = lax.all_to_all(tuple(spectra), "py", split_axis=4, concat_axis=2, tiled=True)
    lines = tuple(
        (jnp.einsum("cxypm,pyqk->cxqkm", member, across, precision=HIGHEST) for member in members)
    )
    members = lax.all_to_all(lines, "px", split_axis=3, concat_axis=1, tiled=True)
    return tuple(
        (jnp.einsum("cxpkm,pxqj->cqjkm", member, along, precision=HIGHEST) for member in members)
    )


def to_space(modes, depth_weights):
    across = turn_table(M2, NY)
    along = turn_table(M1, NX)
    depth_base = depth_table(NZ, M3).T.reshape(2, M3, NZ)
    lines = tuple(
        (jnp.einsum("cqjkm,pxqj->cpxkm", member, along, precision=HIGHEST) for member in modes)
    )
    members = lax.all_to_all(lines, "px", split_axis=2, concat_axis=3, tiled=True)
    columns = tuple(
        (jnp.einsum("cqxkm,pyqk->cpxym", member, across, precision=HIGHEST) for member in members)
    )
    members = lax.all_to_all(columns, "py", split_axis=3, concat_axis=4, tiled=True)
    return tuple(
        (
            jnp.einsum(
                "cpxyk,pkn->cxyn", member, depth_base * weight_row[None, :, None], precision=HIGHEST
            )
            for member, weight_row in zip(members, depth_weights)
        )
    )


def shards(
    flow_field,
    cotangent,
    tucker_core,
    in_factor,
    out_factor,
    first_factor,
    second_factor,
    third_factor,
):
    inverse_count = 1.0 / (NX * NY * NZ)
    weights = jnp.where(jnp.arange(M3) == 0, 1.0, 2.0).astype(jnp.float32)
    base_table = depth_table(NZ, M3)
    block_second = M2 // lax.axis_size("px")
    block_third = M3 // lax.axis_size("py")
    start_second = lax.axis_index("px") * block_second
    start_third = lax.axis_index("py") * block_third
    second_rows = lax.dynamic_slice_in_dim(second_factor, start_second, block_second, 0)
    third_rows = lax.dynamic_slice_in_dim(third_factor, start_third, block_third, 0)
    scale = lax.dynamic_slice_in_dim(weights, start_third, block_third, 0) * inverse_count

    field = flow_field.astype(jnp.float32)
    cot = cotangent.astype(jnp.float32)
    field_low = jnp.einsum("cxyz,ca->axyz", field, in_factor, precision=HIGHEST)
    cot_low = jnp.einsum("oxyz,ob->bxyz", cot, out_factor, precision=HIGHEST)
    lifted, back_mixed = to_modes((field_low, cot_low), (base_table, base_table))
    back_mixed = back_mixed * scale

    two_thirds = jnp.einsum("ks,mt->stkm", second_rows, third_rows, precision=HIGHEST)
    partial = jnp.einsum("abrst,stkm->abrkm", tucker_core, two_thirds, precision=HIGHEST)
    kernel = jnp.einsum("abrkm,jr->abjkm", partial, first_factor, precision=HIGHEST)
    mixed = jnp.einsum("abjkm,apjkm->bpjkm", kernel, lifted, precision=HIGHEST)
    back_lifted = jnp.einsum("abjkm,bpjkm->apjkm", kernel, back_mixed, precision=HIGHEST)
    ones = jnp.ones_like(weights)
    grid, adjoint = to_space((mixed * scale, back_lifted), (ones, ones))
    output_field = jnp.einsum("ob,bxyz->oxyz", out_factor, grid, precision=HIGHEST).astype(jnp.bfloat16)
    grad_in = jnp.einsum("cxyz,axyz->ca", field, adjoint, precision=HIGHEST)
    grad_out = jnp.einsum("oxyz,bxyz->ob", cot, grid, precision=HIGHEST)

    grad_kernel = jnp.einsum("bpjkm,apjkm->abjkm", back_mixed, lifted, precision=HIGHEST)
    rows = jnp.einsum("abjkm,jr->abrkm", grad_kernel, first_factor, precision=HIGHEST)
    grad_first = jnp.einsum("abjkm,abrkm->jr", grad_kernel, partial, precision=HIGHEST)
    pair = jnp.einsum("abrkm,abrst->kmst", rows, tucker_core, precision=HIGHEST)
    grad_second = jnp.einsum("kmst,mt->ks", pair, third_rows, precision=HIGHEST)
    grad_third = jnp.einsum("kmst,ks->mt", pair, second_rows, precision=HIGHEST)
    grad_second = lax.dynamic_update_slice_in_dim(jnp.zeros_like(second_factor), grad_second, start_second, 0)
    grad_third = lax.dynamic_update_slice_in_dim(jnp.zeros_like(third_factor), grad_third, start_third, 0)

    share = jnp.einsum("abrkm,mt->bakrt", rows, third_rows, precision=HIGHEST)
    share = lax.psum_scatter(share, "py", scatter_dimension=0, tiled=True)
    every = lax.all_gather(share, "px", axis=2, tiled=True)
    mine = jnp.einsum("bakrt,ks->barst", every, second_factor, precision=HIGHEST)
    grad_core = lax.all_gather(mine.reshape(1, 16, 512), "py", axis=0, tiled=True)
    grad_core = grad_core.transpose(1, 0, 2).reshape(16, 16, 8, 8, 8)

    small = jnp.concatenate([v.reshape(-1) for v in (grad_in, grad_out, grad_first, grad_second, grad_third)])
    small = lax.psum(lax.psum(small, "py"), "px")
    totals = []
    at = 0
    for v in (grad_in, grad_out, grad_first, grad_second, grad_third):
        totals.append(small[at : at + v.size].reshape(v.shape))
        at += v.size
    return (output_field, grad_core, totals[0], totals[1], totals[2], totals[3], totals[4])


def solution(mesh):
    return jax.shard_map(
        shards,
        mesh=mesh,
        in_specs=(
            P(None, "px", "py", None),
            P(None, "px", "py", None),
            P(),
            P(),
            P(),
            P(),
            P(),
            P(),
        ),
        out_specs=(P(None, "px", "py", None), P(), P(), P(), P(), P(), P()),
        check_vma=False,
    )
```

```python
import functools
import math

import jax
import jax.numpy as jnp
import numpy as np
from jax import lax
from jax.experimental import pallas as pl
from jax.experimental.pallas import tpu as pltpu
from jax.sharding import PartitionSpec as P

F32 = jnp.float32
BF16 = jnp.bfloat16
HIGHEST = lax.Precision.HIGHEST
MESH = pl.DeviceIdType.MESH
COUNT = 16
CELLS = 128
SCALE = 1.0 / (CELLS * CELLS * CELLS)
NN = ((1,), (0,))
NT = ((1,), (1,))


def halves(table):
    high = table.astype(np.float32).astype(jnp.bfloat16)
    low = (table - high.astype(np.float64)).astype(np.float32).astype(jnp.bfloat16)
    return np.stack([high, low])


def depth_rows():
    row = np.arange(128)[:, None]
    lane = np.arange(256)[None, :]
    mode = row // 8 * 2 + row % 2
    angle = 2.0 * math.pi / CELLS * (mode * (lane % 128) % CELLS)
    value = np.where(row // 2 % 2 == 0, np.cos(angle), -np.sin(angle))
    return np.where(row // 4 % 2 == lane // 128, value, 0.0)


def short_transform(rows, row_of, col_of):
    row = np.arange(rows)[:, None]
    col = np.arange(rows)[None, :]
    part_out, freq, rest_out = row_of(row)
    part_in, block, rest_in = col_of(col)
    angle = 2.0 * math.pi / 16 * (freq * block % 16)
    sine = np.where(part_out == 0, 1.0, -1.0) * np.sin(angle)
    value = np.where(part_out == part_in, np.cos(angle), sine)
    return np.where(rest_out == rest_in, value, 0.0)


def second_rows():
    return short_transform(
        128,
        lambda r: (r // 64, r // 4 % 16, r % 4),
        lambda c: (c // 2 % 2, c // 8, c // 4 % 2 * 2 + c % 2),
    )


def first_rows():
    return short_transform(
        256,
        lambda r: (r // 128, r // 4 % 16, r // 64 % 2 * 4 + r % 4),
        lambda c: (c // 8 % 2, c // 16, c // 2 % 2 * 4 + c // 4 % 2 * 2 + c % 2),
    )


def twiddles():
    row = np.arange(64)[:, None]
    lane = np.arange(128)[None, :]
    tables = []
    for high in range(2):
        angle = 2.0 * math.pi / CELLS * ((row // 4 - 16 * high) * (lane // 16))
        tables.append(np.stack([np.cos(angle), np.sin(angle)]))
    return np.stack(tables).astype(np.float32)


def gather_lanes():
    row = np.arange(1024)[:, None]
    lane = np.arange(128)[None, :]
    return ((row // 128 == lane // 16) & (row % 16 == lane % 16)).astype(np.float32).astype(jnp.bfloat16)


def split(value):
    high = value.astype(BF16)
    return high, (value - high.astype(F32)).astype(BF16)


def mul(a, b, dims=NN):
    return lax.dot_general(a, b, (dims, ((), ())), preferred_element_type=F32)


def exact(a, b, dims=NN):
    return lax.dot_general(a, b, (dims, ((), ())), precision=HIGHEST, preferred_element_type=F32)


def mul3(a, b, dims=NN):
    return mul(a[0], b[0], dims) + mul(a[0], b[1], dims) + mul(a[1], b[0], dims)


def pair(ref):
    return ref[0], ref[1]


def iota(shape, axis):
    return lax.broadcasted_iota(jnp.int32, shape, axis)


def hot(test):
    return jnp.where(test, 1.0, 0.0).astype(F32)


def kernel(
    field, cot, core, in_t, out_t, first_t, second_t, third_t,
    tz, a1, a1t, a2, a2t, tw, spread, collect,
    out_ref, core_out, small_out,
    m_in, m_out, back_map, s1, r1, wide, s2, r2, s3, r3, s4, r4,
    kern, grad, s5, r8, s6, r9, s7, cg, spread_second, phi, acc, ts, r5, t2, r6, t3, r7,
    send, recv,
):
    px = lax.axis_index("px")
    py = lax.axis_index("py")

    def along_y(peer):
        return (px, peer)

    def along_x(peer):
        return (peer, py)

    barrier = pltpu.get_barrier_semaphore()

    def greet(d, carry):
        pl.semaphore_signal(barrier, inc=1, device_id=along_y(lax.rem(py + d, COUNT)), device_id_type=MESH)
        pl.semaphore_signal(barrier, inc=1, device_id=along_x(lax.rem(px + d, COUNT)), device_id_type=MESH)
        return carry

    lax.fori_loop(1, COUNT, greet, 0)

    def copy(phase, me, peer, device, source, target, slot):
        return pltpu.make_async_remote_copy(
            src_ref=source(peer),
            dst_ref=target(slot),
            send_sem=send.at[phase, peer],
            recv_sem=recv.at[phase, slot],
            device_id=device(peer),
            device_id_type=MESH,
        )

    def each(me, act):
        def body(d, carry):
            act(lax.rem(me + d, COUNT))
            return carry

        lax.fori_loop(1, COUNT, body, 0)

    sends = []

    def start(phase, me, device, source, target):
        each(me, lambda peer: copy(phase, me, peer, device, source, target, me).start())
        sends.append((phase, me, device, source, target))

    def arrive(phase, me, device, source, target):
        each(me, lambda peer: copy(phase, me, peer, device, source, target, peer).wait_recv())

    def rows8(ref):
        return lambda i: ref.at[pl.ds(pl.multiple_of(i * 8, 8), 8)]

    def slab(ref):
        return lambda i: ref.at[i]

    def block(ref):
        return lambda i: ref.at[lax.div(i, 8), :, lax.rem(i, 8)]

    def whole(ref):
        return lambda i: ref

    lane = iota((16, 512), 1)
    repeat = hot(iota((64, 512), 1) // 8 == iota((64, 512), 0))
    for f, factor in enumerate((in_t, out_t)):
        wide_factor = exact(factor[...], repeat)
        full = jnp.concatenate([jnp.where(lane % 8 == y, wide_factor, 0.0) for y in range(8)], axis=0)
        high, low = split(full)
        m_in[f, 0:128] = high
        m_in[f, 128:256] = low
        if f == 1:
            high, low = split(full.T)
            back_map[0] = high
            back_map[1] = low

    tz_pair = pair(tz)

    def depth_step(x, carry):
        parts = []
        for f, source in enumerate((field, cot)):
            rows = source[:, pl.ds(x, 1)].astype(F32).reshape(512, 128).astype(BF16)
            both = mul(m_in[f], rows)
            parts.append(both[0:128] + both[128:256])
        s1[:, pl.ds(pl.multiple_of(x * 128, 128), 128)] = mul3(
            tz_pair, split(jnp.concatenate(parts, axis=1)), NT
        )
        return carry

    lax.fori_loop(0, 8, depth_step, 0)
    pl.semaphore_wait(barrier, 2 * (COUNT - 1))
    start(0, py, along_y, rows8(s1), rows8(r1))
    own = pl.ds(pl.multiple_of(py * 8, 8), 8)
    r1[own] = s1[own]

    mode = iota((32, 128), 1)
    row32 = iota((32, 128), 0)
    t1 = exact(first_t[...], hot(mode // 4 == row32))
    t2f = exact(second_t[...], hot(mode // 2 % 2 + 2 * px == row32))
    t3f = exact(third_t[...], hot(mode % 2 + 2 * py == row32))
    tiles = []
    for r in range(8):
        for s in range(8):
            tiles.append(t3f * (t1[r : r + 1] * t2f[s : s + 1]))
    phi_pair = split(jnp.concatenate(tiles, axis=0))
    core_pair = split(core[...])
    kern[...] = mul3(core_pair, phi_pair).reshape(16, 16, 128)
    spread_second[...] = exact(second_t[...], hot(iota((32, 2048), 1) // 64 == iota((32, 2048), 0)))

    arrive(0, py, along_y, rows8(s1), rows8(r1))
    middle = mul3(pair(a1), split(r1[...]))
    for x in range(8):
        real = middle[0:64, x * 128 : (x + 1) * 128]
        imag = middle[64:128, x * 128 : (x + 1) * 128]
        for h in range(2):
            cosine, sine = tw[h, 0], tw[h, 1]
            for p, value in enumerate((cosine * real + sine * imag, cosine * imag - sine * real)):
                high, low = split(value)
                at = slice(h * 128 + p * 64, h * 128 + p * 64 + 64)
                wide[at, x * 128 : (x + 1) * 128] = high
                wide[at, 1024 + x * 128 : 1024 + (x + 1) * 128] = low
    gathered = mul(wide[:, 0:1024], collect[...]) + mul(wide[:, 1024:2048], collect[...])
    s2[...] = gathered.reshape(2, 2, 8, 8, 128)
    start(1, px, along_x, block(s2), slab(r2))
    r2[px] = s2[lax.div(px, 8), :, lax.rem(px, 8)]

    arrive(1, px, along_x, block(s2), slab(r2))
    middle = mul3(pair(a2), split(r2[...].reshape(256, 128)))
    parts = []
    for p in range(2):
        for f in range(2):
            real = middle[f * 64 : f * 64 + 64]
            imag = middle[128 + f * 64 : 128 + f * 64 + 64]
            for h in range(2):
                cosine, sine = tw[h, 0], tw[h, 1]
                parts.append(cosine * real + sine * imag if p == 0 else cosine * imag - sine * real)
    high, low = split(jnp.concatenate(parts, axis=0))
    ones = hot(iota((16, 128), 1) % 16 == iota((16, 128), 0)).astype(BF16)
    modes = mul(ones, high, NT) + mul(ones, low, NT)

    depth_mode = iota((1, 128), 1) % 2 + 2 * py
    scale = jnp.where(depth_mode == 0, 1.0, 2.0).astype(F32) * SCALE
    lifted = [modes[:, p * 256 : p * 256 + 128] for p in range(2)]
    back = [modes[:, p * 256 + 128 : p * 256 + 256] * scale for p in range(2)]
    mixed = [jnp.zeros((16, 128), F32) for p in range(2)]
    lifted_back = [jnp.zeros((16, 128), F32) for p in range(2)]
    for i in range(16):
        over_a = kern[:, i]
        over_b = kern[i]
        for p in range(2):
            mixed[p] = mixed[p] + over_a * lifted[p][i : i + 1]
            lifted_back[p] = lifted_back[p] + over_b * back[p][i : i + 1]
    modes = jnp.concatenate([mixed[0] * scale, lifted_back[0], mixed[1] * scale, lifted_back[1]], axis=1)

    opened = jnp.concatenate([modes] * 8, axis=0).T
    parts = []
    for p in range(2):
        for f in range(2):
            total = None
            for h in range(2):
                cosine, sine = tw[h, 0], tw[h, 1]
                real = opened[f * 128 + h * 64 : f * 128 + h * 64 + 64]
                imag = opened[256 + f * 128 + h * 64 : 256 + f * 128 + h * 64 + 64]
                term = cosine * real - sine * imag if p == 0 else sine * real + cosine * imag
                total = term if total is None else total + term
            parts.append(total)
    s3[...] = mul3(pair(a2t), split(jnp.concatenate(parts, axis=0))).reshape(16, 2, 8, 128)
    start(2, px, along_x, slab(s3), block(r3))
    r3[lax.div(px, 8), :, lax.rem(px, 8)] = s3[px]

    for b in range(16):
        grad[b] = lifted[0] * back[0][b : b + 1] + lifted[1] * back[1][b : b + 1]
    grad_pair = split(grad[...].reshape(256, 128))
    tiles = []
    for k in range(2):
        kept = hot(iota((8, 128), 1) // 2 % 2 == k) * t3f
        for r in range(8):
            tiles.append(kept * t1[r : r + 1])
    s5[...] = mul3(grad_pair, split(jnp.concatenate(tiles, axis=0)), NT).reshape(16, 16, 128)
    start(3, py, along_y, slab(s5), slab(r8))
    r8[py] = s5[py]

    pulled = mul3(split(core[...].T), grad_pair)
    by_first = []
    by_second = [jnp.zeros((8, 128), F32) for s in range(8)]
    by_third = jnp.zeros((8, 128), F32)
    for r in range(8):
        total = jnp.zeros((8, 128), F32)
        for s in range(8):
            tile = pulled[(r * 8 + s) * 8 : (r * 8 + s) * 8 + 8]
            total = total + tile * t2f[s : s + 1]
            by_second[s] = by_second[s] + tile * t1[r : r + 1]
        by_first.append(total)
        by_third = by_third + total * t1[r : r + 1]
    fold = hot(iota((8, 64), 1) // 8 == iota((8, 64), 0))
    first_rows8 = exact(fold, jnp.concatenate([t * t3f for t in by_first], axis=0))
    second_rows8 = exact(fold, jnp.concatenate([t * t3f for t in by_second], axis=0))
    row = iota((128, 128), 0)
    col = iota((128, 128), 1)
    factor_grads = (
        exact(first_rows8, hot(row // 4 == col))
        + exact(second_rows8, hot(row // 2 % 2 + 2 * px + 32 == col))
        + exact(by_third, hot(row % 2 + 2 * py + 64 == col))
    )

    arrive(2, px, along_x, slab(s3), block(r3))
    back_pair = split(r3[...].reshape(256, 128))
    for x in range(8):
        places = spread[:, x * 128 : (x + 1) * 128]
        opened = mul(back_pair[0], places) + mul(back_pair[1], places)
        parts = []
        for p in range(2):
            total = None
            for h in range(2):
                cosine, sine = tw[h, 0], tw[h, 1]
                real = opened[h * 128 : h * 128 + 64]
                imag = opened[h * 128 + 64 : h * 128 + 128]
                term = cosine * real - sine * imag if p == 0 else sine * real + cosine * imag
                total = term if total is None else total + term
            parts.append(total)
        s4[:, x * 128 : (x + 1) * 128] = mul3(pair(a1t), split(jnp.concatenate(parts, axis=0)))
    start(4, py, along_y, rows8(s4), rows8(r4))
    r4[own] = s4[own]

    arrive(3, py, along_y, slab(s5), slab(r8))
    total = r8[0]
    for q in range(1, 16):
        total = total + r8[q]
    s6[...] = total
    start(5, px, along_x, whole(s6), slab(r9))
    r9[px] = s6[...]

    arrive(4, py, along_y, rows8(s4), rows8(r4))
    acc[...] = jnp.zeros_like(acc)

    def depth_back(x, carry):
        rows = r4[:, pl.ds(pl.multiple_of(x * 128, 128), 128)].T
        grids = mul3(split(rows), tz_pair)
        grid_pair = split(grids[:, 0:128])
        adjoint_pair = split(grids[:, 128:256])
        out_ref[:, pl.ds(x, 1)] = mul3(pair(back_map), grid_pair).reshape(64, 1, 8, 128).astype(BF16)
        for f, (source, values) in enumerate(((field, adjoint_pair), (cot, grid_pair))):
            given = source[:, pl.ds(x, 1)].astype(F32).reshape(512, 128).astype(BF16)
            acc[f] = acc[f] + mul(given, values[0], NT) + mul(given, values[1], NT)
        return carry

    lax.fori_loop(0, 8, depth_back, 0)
    kept = hot(iota((512, 128), 0) % 8 == iota((512, 128), 1) // 16)
    sums = [jnp.sum((acc[f] * kept).reshape(64, 8, 128), axis=1) for f in range(2)]
    high, low = split(jnp.concatenate(sums, axis=0))
    channel_grads = mul(ones, high, NT) + mul(ones, low, NT)
    packed = jnp.concatenate([channel_grads, factor_grads, jnp.zeros((8, 128), F32)], axis=0)
    for q in range(16):
        ts[q] = packed[2 * q : 2 * q + 2]
    start(6, py, along_y, slab(ts), slab(r5))
    r5[py] = ts[py]

    arrive(5, px, along_x, whole(s6), slab(r9))
    totals = [jnp.zeros((16, 128), F32) for s in range(8)]
    for q in range(16):
        received = r9[q]
        for s in range(8):
            totals[s] = totals[s] + received * spread_second[s : s + 1, q * 128 : (q + 1) * 128]
    totals = [t + pltpu.roll(t, 64, 1) for t in totals]
    left = iota((16, 128), 1) < 64
    for u in range(4):
        s7[:, u * 128 : (u + 1) * 128] = jnp.where(left, totals[2 * u], totals[2 * u + 1])
    start(7, py, along_y, whole(s7), slab(cg))
    cg[py] = s7[...]

    arrive(6, py, along_y, slab(ts), slab(r5))
    t2[...] = jnp.sum(r5[...], axis=0)
    start(8, px, along_x, whole(t2), slab(r6))
    r6[px] = t2[...]
    arrive(8, px, along_x, whole(t2), slab(r6))
    t3[...] = jnp.sum(r6[...], axis=0)
    start(9, py, along_y, whole(t3), slab(r7))
    r7[py] = t3[...]
    arrive(9, py, along_y, whole(t3), slab(r7))
    small_out[...] = r7[...]
    arrive(7, py, along_y, whole(s7), slab(cg))
    core_out[...] = cg[...]
    for phase, me, device, source, target in sends:
        each(
            me,
            lambda peer, phase=phase, me=me, device=device, source=source, target=target: copy(
                phase, me, peer, device, source, target, me
            ).wait_send(),
        )


def shards(field, cot, core, in_factor, out_factor, first, second, third):
    constants = [
        jnp.asarray(c)
        for c in (
            halves(depth_rows()),
            halves(second_rows()),
            halves(second_rows().T),
            halves(first_rows()),
            halves(first_rows().T),
            twiddles(),
            np.ascontiguousarray(gather_lanes().T),
            gather_lanes(),
        )
    ]
    core = core.transpose(1, 0, 2, 3, 4).reshape(256, 512)
    vmem = pl.BlockSpec(memory_space=pltpu.VMEM)
    scratch = [
        pltpu.VMEM((2, 256, 512), BF16),
        pltpu.VMEM((1, 8, 128), F32),
        pltpu.VMEM((2, 512, 128), BF16),
        pltpu.VMEM((128, 1024), F32),
        pltpu.VMEM((128, 1024), F32),
        pltpu.VMEM((256, 2048), BF16),
        pltpu.VMEM((2, 2, 8, 8, 128), F32),
        pltpu.VMEM((16, 2, 8, 128), F32),
        pltpu.VMEM((16, 2, 8, 128), F32),
        pltpu.VMEM((2, 2, 8, 8, 128), F32),
        pltpu.VMEM((128, 1024), F32),
        pltpu.VMEM((128, 1024), F32),
        pltpu.VMEM((16, 16, 128), F32),
        pltpu.VMEM((16, 16, 128), F32),
        pltpu.VMEM((16, 16, 128), F32),
        pltpu.VMEM((16, 16, 128), F32),
        pltpu.VMEM((16, 128), F32),
        pltpu.VMEM((16, 16, 128), F32),
        pltpu.VMEM((16, 512), F32),
        pltpu.VMEM((16, 16, 512), F32),
        pltpu.VMEM((8, 2048), F32),
        pltpu.VMEM((8, 128), F32),
        pltpu.VMEM((2, 512, 128), F32),
        pltpu.VMEM((16, 2, 128), F32),
        pltpu.VMEM((16, 2, 128), F32),
        pltpu.VMEM((2, 128), F32),
        pltpu.VMEM((16, 2, 128), F32),
        pltpu.VMEM((2, 128), F32),
        pltpu.VMEM((16, 2, 128), F32),
        pltpu.SemaphoreType.DMA((10, COUNT)),
        pltpu.SemaphoreType.DMA((10, COUNT)),
    ]
    output, grad_core, small = pl.pallas_call(
        kernel,
        out_shape=(
            jax.ShapeDtypeStruct((64, 8, 8, 128), BF16),
            jax.ShapeDtypeStruct((16, 16, 512), F32),
            jax.ShapeDtypeStruct((16, 2, 128), F32),
        ),
        in_specs=[vmem] * (8 + len(constants)),
        out_specs=[vmem] * 3,
        scratch_shapes=scratch,
        compiler_params=pltpu.CompilerParams(
            collective_id=0, has_side_effects=True, vmem_limit_bytes=48 * 1024 * 1024
        ),
        name="tucker_step",
    )(field, cot, core, in_factor.T, out_factor.T, first.T, second.T, third.T, *constants)
    grad_core = grad_core.reshape(16, 16, 8, 8, 8).transpose(1, 0, 3, 2, 4)
    small = small.reshape(32, 128)
    return (
        output,
        grad_core,
        small[0:16, 0:64].T,
        small[0:16, 64:128].T,
        small[16:24, 0:32].T,
        small[16:24, 32:64].T,
        small[16:24, 64:96].T,
    )


def solution(mesh):
    grid = P(None, "px", "py", None)
    return jax.shard_map(
        shards,
        mesh=mesh,
        in_specs=(grid, grid) + (P(),) * 6,
        out_specs=(grid,) + (P(),) * 6,
        check_vma=False,
    )
```

```python
import functools
import math

import jax
import jax.numpy as jnp
import numpy as np
from jax import lax
from jax.experimental import pallas as pl
from jax.experimental.pallas import tpu as pltpu
from jax.sharding import PartitionSpec as P

F32 = jnp.float32
BF16 = jnp.bfloat16
HIGHEST = lax.Precision.HIGHEST
MESH = pl.DeviceIdType.MESH
COUNT = 16
CELLS = 128
SCALE = 1.0 / (CELLS * CELLS * CELLS)
NN = ((1,), (0,))
NT = ((1,), (1,))


def halves(table):
    high = table.astype(np.float32).astype(jnp.bfloat16)
    low = (table - high.astype(np.float64)).astype(np.float32).astype(jnp.bfloat16)
    return np.stack([high, low])


def depth_rows():
    row = np.arange(128)[:, None]
    lane = np.arange(256)[None, :]
    mode = row // 8 * 2 + row % 2
    angle = 2.0 * math.pi / CELLS * (mode * (lane % 128) % CELLS)
    value = np.where(row // 2 % 2 == 0, np.cos(angle), -np.sin(angle))
    return np.where(row // 4 % 2 == lane // 128, value, 0.0)


def short_transform(rows, row_of, col_of):
    row = np.arange(rows)[:, None]
    col = np.arange(rows)[None, :]
    part_out, freq, rest_out = row_of(row)
    part_in, block, rest_in = col_of(col)
    angle = 2.0 * math.pi / 16 * (freq * block % 16)
    sine = np.where(part_out == 0, 1.0, -1.0) * np.sin(angle)
    value = np.where(part_out == part_in, np.cos(angle), sine)
    return np.where(rest_out == rest_in, value, 0.0)


def second_rows():
    return short_transform(
        128,
        lambda r: (r // 64, r // 4 % 16, r % 4),
        lambda c: (c // 2 % 2, c // 8, c // 4 % 2 * 2 + c % 2),
    )


def first_rows():
    return short_transform(
        256,
        lambda r: (r // 128, r // 4 % 16, r // 64 % 2 * 4 + r % 4),
        lambda c: (c // 8 % 2, c // 16, c // 2 % 2 * 4 + c // 4 % 2 * 2 + c % 2),
    )


def twiddles():
    row = np.arange(64)[:, None]
    lane = np.arange(128)[None, :]
    tables = []
    for high in range(2):
        angle = 2.0 * math.pi / CELLS * ((row // 4 - 16 * high) * (lane // 16))
        tables.append(np.stack([np.cos(angle), np.sin(angle)]))
    return np.stack(tables).astype(np.float32)


def gather_lanes():
    row = np.arange(1024)[:, None]
    lane = np.arange(128)[None, :]
    return ((row // 128 == lane // 16) & (row % 16 == lane % 16)).astype(np.float32).astype(jnp.bfloat16)


def split(value):
    high = value.astype(BF16)
    return high, (value - high.astype(F32)).astype(BF16)


def mul(a, b, dims=NN):
    return lax.dot_general(a, b, (dims, ((), ())), preferred_element_type=F32)


def exact(a, b, dims=NN):
    return lax.dot_general(a, b, (dims, ((), ())), precision=HIGHEST, preferred_element_type=F32)


def mul3(a, b, dims=NN):
    return mul(a[0], b[0], dims) + mul(a[0], b[1], dims) + mul(a[1], b[0], dims)


def pair(ref):
    return ref[0], ref[1]


def iota(shape, axis):
    return lax.broadcasted_iota(jnp.int32, shape, axis)


def hot(test):
    return jnp.where(test, 1.0, 0.0).astype(F32)


def kernel(
    field_h, cot_h, core_h, in_h, out_h, first_h, second_h, third_h,
    tz_h, a1_h, a1t_h, a2_h, a2t_h, tw_h, spread_h, collect_h,
    out_ref, core_out, small_out,
    field, cot, core_n, in_t, out_t, first_t, second_t, third_t,
    tz, a1, a1t, a2, a2t, tw, spread, collect, core,
    m_in, m_out, back_map, s1, r1, wide, s2, r2, s3, r3, s4, r4,
    kern, grad, s5, r8, s6, r9, s7, cg, spread_second, phi, acc, ts, r5, t2, r6, t3, r7,
    send, recv, loads,
):
    px = lax.axis_index("px")
    py = lax.axis_index("py")

    def along_y(peer):
        return (px, peer)

    def along_x(peer):
        return (peer, py)

    barrier = pltpu.get_barrier_semaphore()

    def greet(d, carry):
        pl.semaphore_signal(barrier, inc=1, device_id=along_y(lax.rem(py + d, COUNT)), device_id_type=MESH)
        pl.semaphore_signal(barrier, inc=1, device_id=along_x(lax.rem(px + d, COUNT)), device_id_type=MESH)
        return carry

    staged = (
        (in_h, in_t), (out_h, out_t), (field_h, field), (cot_h, cot), (tz_h, tz),
        (first_h, first_t), (second_h, second_t), (third_h, third_t), (a1_h, a1), (tw_h, tw), (collect_h, collect),
        (core_h, core_n), (a2_h, a2), (a2t_h, a2t), (spread_h, spread), (a1t_h, a1t),
    )
    copies = [pltpu.make_async_copy(far, near, loads.at[i]) for i, (far, near) in enumerate(staged)]
    for c in copies:
        c.start()
    lax.fori_loop(1, COUNT, greet, 0)

    def copy(phase, me, peer, device, source, target, slot):
        return pltpu.make_async_remote_copy(
            src_ref=source(peer),
            dst_ref=target(slot),
            send_sem=send.at[phase, peer],
            recv_sem=recv.at[phase, slot],
            device_id=device(peer),
            device_id_type=MESH,
        )

    def each(me, act):
        def body(d, carry):
            act(lax.rem(me + d, COUNT))
            return carry

        lax.fori_loop(1, COUNT, body, 0)

    sends = []

    def start(phase, me, device, source, target):
        each(me, lambda peer: copy(phase, me, peer, device, source, target, me).start())
        sends.append((phase, me, device, source, target))

    def arrive(phase, me, device, source, target):
        each(me, lambda peer: copy(phase, me, peer, device, source, target, peer).wait_recv())

    def rows8(ref):
        return lambda i: ref.at[pl.ds(pl.multiple_of(i * 8, 8), 8)]

    def slab(ref):
        return lambda i: ref.at[i]

    def block(ref):
        return lambda i: ref.at[lax.div(i, 8), :, lax.rem(i, 8)]

    def whole(ref):
        return lambda i: ref

    copies[0].wait()
    copies[1].wait()

    lane = iota((16, 512), 1)
    repeat = hot(iota((64, 512), 1) // 8 == iota((64, 512), 0))
    for f, factor in enumerate((in_t, out_t)):
        wide_factor = exact(factor[...], repeat)
        full = jnp.concatenate([jnp.where(lane % 8 == y, wide_factor, 0.0) for y in range(8)], axis=0)
        high, low = split(full)
        m_in[f, 0:128] = high
        m_in[f, 128:256] = low
        if f == 1:
            high, low = split(full.T)
            back_map[0] = high
            back_map[1] = low

    for c in copies[2:5]:
        c.wait()
    tz_pair = pair(tz)

    def depth_step(x, carry):
        parts = []
        for f, source in enumerate((field, cot)):
            rows = source[:, pl.ds(x, 1)].astype(F32).reshape(512, 128).astype(BF16)
            both = mul(m_in[f], rows)
            parts.append(both[0:128] + both[128:256])
        s1[:, pl.ds(pl.multiple_of(x * 128, 128), 128)] = mul3(
            tz_pair, split(jnp.concatenate(parts, axis=1)), NT
        )
        return carry

    lax.fori_loop(0, 8, depth_step, 0)
    pl.semaphore_wait(barrier, 2 * (COUNT - 1))
    start(0, py, along_y, rows8(s1), rows8(r1))
    own = pl.ds(pl.multiple_of(py * 8, 8), 8)
    r1[own] = s1[own]

    for c in copies[5:]:
        c.wait()

    mode = iota((32, 128), 1)
    row32 = iota((32, 128), 0)
    t1 = exact(first_t[...], hot(mode // 4 == row32))
    t2f = exact(second_t[...], hot(mode // 2 % 2 + 2 * px == row32))
    t3f = exact(third_t[...], hot(mode % 2 + 2 * py == row32))
    tiles = []
    for r in range(8):
        for s in range(8):
            tiles.append(t3f * (t1[r : r + 1] * t2f[s : s + 1]))
    phi_pair = split(jnp.concatenate(tiles, axis=0))
    for a in range(16):
        core[:, a] = core_n[a].T
    core_flat = core[...].reshape(256, 512)
    core_pair = split(core_flat)
    kern[...] = mul3(core_pair, phi_pair).reshape(16, 16, 128)
    spread_second[...] = exact(second_t[...], hot(iota((32, 2048), 1) // 64 == iota((32, 2048), 0)))

    arrive(0, py, along_y, rows8(s1), rows8(r1))
    middle = mul3(pair(a1), split(r1[...]))
    for x in range(8):
        real = middle[0:64, x * 128 : (x + 1) * 128]
        imag = middle[64:128, x * 128 : (x + 1) * 128]
        for h in range(2):
            cosine, sine = tw[h, 0], tw[h, 1]
            for p, value in enumerate((cosine * real + sine * imag, cosine * imag - sine * real)):
                high, low = split(value)
                at = slice(h * 128 + p * 64, h * 128 + p * 64 + 64)
                wide[at, x * 128 : (x + 1) * 128] = high
                wide[at, 1024 + x * 128 : 1024 + (x + 1) * 128] = low
    gathered = mul(wide[:, 0:1024], collect[...]) + mul(wide[:, 1024:2048], collect[...])
    s2[...] = gathered.reshape(2, 2, 8, 8, 128)
    start(1, px, along_x, block(s2), slab(r2))
    r2[px] = s2[lax.div(px, 8), :, lax.rem(px, 8)]

    arrive(1, px, along_x, block(s2), slab(r2))
    middle = mul3(pair(a2), split(r2[...].reshape(256, 128)))
    parts = []
    for p in range(2):
        for f in range(2):
            real = middle[f * 64 : f * 64 + 64]
            imag = middle[128 + f * 64 : 128 + f * 64 + 64]
            for h in range(2):
                cosine, sine = tw[h, 0], tw[h, 1]
                parts.append(cosine * real + sine * imag if p == 0 else cosine * imag - sine * real)
    high, low = split(jnp.concatenate(parts, axis=0))
    ones = hot(iota((16, 128), 1) % 16 == iota((16, 128), 0)).astype(BF16)
    modes = mul(ones, high, NT) + mul(ones, low, NT)

    depth_mode = iota((1, 128), 1) % 2 + 2 * py
    scale = jnp.where(depth_mode == 0, 1.0, 2.0).astype(F32) * SCALE
    lifted = [modes[:, p * 256 : p * 256 + 128] for p in range(2)]
    back = [modes[:, p * 256 + 128 : p * 256 + 256] * scale for p in range(2)]
    mixed = [jnp.zeros((16, 128), F32) for p in range(2)]
    lifted_back = [jnp.zeros((16, 128), F32) for p in range(2)]
    for i in range(16):
        over_a = kern[:, i]
        over_b = kern[i]
        for p in range(2):
            mixed[p] = mixed[p] + over_a * lifted[p][i : i + 1]
            lifted_back[p] = lifted_back[p] + over_b * back[p][i : i + 1]
    modes = jnp.concatenate([mixed[0] * scale, lifted_back[0], mixed[1] * scale, lifted_back[1]], axis=1)

    opened = jnp.concatenate([modes] * 8, axis=0).T
    parts = []
    for p in range(2):
        for f in range(2):
            total = None
            for h in range(2):
                cosine, sine = tw[h, 0], tw[h, 1]
                real = opened[f * 128 + h * 64 : f * 128 + h * 64 + 64]
                imag = opened[256 + f * 128 + h * 64 : 256 + f * 128 + h * 64 + 64]
                term = cosine * real - sine * imag if p == 0 else sine * real + cosine * imag
                total = term if total is None else total + term
            parts.append(total)
    s3[...] = mul3(pair(a2t), split(jnp.concatenate(parts, axis=0))).reshape(16, 2, 8, 128)
    start(2, px, along_x, slab(s3), block(r3))
    r3[lax.div(px, 8), :, lax.rem(px, 8)] = s3[px]

    for b in range(16):
        grad[b] = lifted[0] * back[0][b : b + 1] + lifted[1] * back[1][b : b + 1]
    grad_pair = split(grad[...].reshape(256, 128))
    tiles = []
    for k in range(2):
        kept = hot(iota((8, 128), 1) // 2 % 2 == k) * t3f
        for r in range(8):
            tiles.append(kept * t1[r : r + 1])
    s5[...] = mul3(grad_pair, split(jnp.concatenate(tiles, axis=0)), NT).reshape(16, 16, 128)
    start(3, py, along_y, slab(s5), slab(r8))
    r8[py] = s5[py]

    pulled = mul3(split(core[...].reshape(256, 512).T), grad_pair)
    by_first = []
    by_second = [jnp.zeros((8, 128), F32) for s in range(8)]
    by_third = jnp.zeros((8, 128), F32)
    for r in range(8):
        total = jnp.zeros((8, 128), F32)
        for s in range(8):
            tile = pulled[(r * 8 + s) * 8 : (r * 8 + s) * 8 + 8]
            total = total + tile * t2f[s : s + 1]
            by_second[s] = by_second[s] + tile * t1[r : r + 1]
        by_first.append(total)
        by_third = by_third + total * t1[r : r + 1]
    fold = hot(iota((8, 64), 1) // 8 == iota((8, 64), 0))
    first_rows8 = exact(fold, jnp.concatenate([t * t3f for t in by_first], axis=0))
    second_rows8 = exact(fold, jnp.concatenate([t * t3f for t in by_second], axis=0))
    row = iota((128, 128), 0)
    col = iota((128, 128), 1)
    factor_grads = (
        exact(first_rows8, hot(row // 4 == col))
        + exact(second_rows8, hot(row // 2 % 2 + 2 * px + 32 == col))
        + exact(by_third, hot(row % 2 + 2 * py + 64 == col))
    )

    arrive(2, px, along_x, slab(s3), block(r3))
    back_pair = split(r3[...].reshape(256, 128))
    for x in range(8):
        places = spread[:, x * 128 : (x + 1) * 128]
        opened = mul(back_pair[0], places) + mul(back_pair[1], places)
        parts = []
        for p in range(2):
            total = None
            for h in range(2):
                cosine, sine = tw[h, 0], tw[h, 1]
                real = opened[h * 128 : h * 128 + 64]
                imag = opened[h * 128 + 64 : h * 128 + 128]
                term = cosine * real - sine * imag if p == 0 else sine * real + cosine * imag
                total = term if total is None else total + term
            parts.append(total)
        s4[:, x * 128 : (x + 1) * 128] = mul3(pair(a1t), split(jnp.concatenate(parts, axis=0)))
    start(4, py, along_y, rows8(s4), rows8(r4))
    r4[own] = s4[own]

    arrive(3, py, along_y, slab(s5), slab(r8))
    total = r8[0]
    for q in range(1, 16):
        total = total + r8[q]
    s6[...] = total
    start(5, px, along_x, whole(s6), slab(r9))
    r9[px] = s6[...]

    arrive(4, py, along_y, rows8(s4), rows8(r4))
    acc[...] = jnp.zeros_like(acc)

    def depth_back(x, carry):
        rows = r4[:, pl.ds(pl.multiple_of(x * 128, 128), 128)].T
        grids = mul3(split(rows), tz_pair)
        grid_pair = split(grids[:, 0:128])
        adjoint_pair = split(grids[:, 128:256])
        out_ref[:, pl.ds(x, 1)] = mul3(pair(back_map), grid_pair).reshape(64, 1, 8, 128).astype(BF16)
        for f, (source, values) in enumerate(((field, adjoint_pair), (cot, grid_pair))):
            given = source[:, pl.ds(x, 1)].astype(F32).reshape(512, 128).astype(BF16)
            acc[f] = acc[f] + mul(given, values[0], NT) + mul(given, values[1], NT)
        return carry

    lax.fori_loop(0, 8, depth_back, 0)
    kept = hot(iota((512, 128), 0) % 8 == iota((512, 128), 1) // 16)
    sums = [jnp.sum((acc[f] * kept).reshape(64, 8, 128), axis=1) for f in range(2)]
    high, low = split(jnp.concatenate(sums, axis=0))
    channel_grads = mul(ones, high, NT) + mul(ones, low, NT)
    packed = jnp.concatenate([channel_grads, factor_grads, jnp.zeros((8, 128), F32)], axis=0)
    for q in range(16):
        ts[q] = packed[2 * q : 2 * q + 2]
    start(6, py, along_y, slab(ts), slab(r5))
    r5[py] = ts[py]

    arrive(5, px, along_x, whole(s6), slab(r9))
    totals = [jnp.zeros((16, 128), F32) for s in range(8)]
    for q in range(16):
        received = r9[q]
        for s in range(8):
            totals[s] = totals[s] + received * spread_second[s : s + 1, q * 128 : (q + 1) * 128]
    totals = [t + pltpu.roll(t, 64, 1) for t in totals]
    left = iota((16, 128), 1) < 64
    for u in range(4):
        s7[:, u * 128 : (u + 1) * 128] = jnp.where(left, totals[2 * u], totals[2 * u + 1])
    start(7, py, along_y, whole(s7), slab(cg))
    cg[py] = s7[...]

    arrive(6, py, along_y, slab(ts), slab(r5))
    t2[...] = jnp.sum(r5[...], axis=0)
    start(8, px, along_x, whole(t2), slab(r6))
    r6[px] = t2[...]
    arrive(8, px, along_x, whole(t2), slab(r6))
    t3[...] = jnp.sum(r6[...], axis=0)
    start(9, py, along_y, whole(t3), slab(r7))
    r7[py] = t3[...]
    arrive(9, py, along_y, whole(t3), slab(r7))
    small_out[...] = r7[...]
    arrive(7, py, along_y, whole(s7), slab(cg))
    core_out[...] = cg[...]
    for phase, me, device, source, target in sends:
        each(
            me,
            lambda peer, phase=phase, me=me, device=device, source=source, target=target: copy(
                phase, me, peer, device, source, target, me
            ).wait_send(),
        )


def finish(
    output, packed, small,
    output_h, core_h, in_h, out_h, first_h, second_h, third_h,
    core, grad_in, grad_out, grad_first, grad_second, grad_third, done,
):
    copies = [pltpu.make_async_copy(output, output_h, done.at[0])]
    copies[0].start()
    grad_in[...] = small[0:16, 0:64]
    grad_out[...] = small[0:16, 64:128]
    grad_first[...] = small[16:24, 0:32]
    grad_second[...] = small[16:24, 32:64]
    grad_third[...] = small[16:24, 64:96]
    for a in range(16):
        rows = packed[:, a].T.reshape(8, 8, 8, 16)
        for s in range(8):
            for r in range(8):
                core[a, (r * 8 + s) * 8 : (r * 8 + s) * 8 + 8] = rows[s, r]
        copies.append(pltpu.make_async_copy(core.at[a], core_h.at[a], done.at[1 + a]))
        copies[-1].start()
    pairs = ((grad_in, in_h), (grad_out, out_h), (grad_first, first_h), (grad_second, second_h), (grad_third, third_h))
    for i, (near, far) in enumerate(pairs):
        copies.append(pltpu.make_async_copy(near, far, done.at[17 + i]))
        copies[-1].start()
    for c in copies:
        c.wait()


def shards(field, cot, core, in_factor, out_factor, first, second, third):
    constants = [
        jnp.asarray(c)
        for c in (
            halves(depth_rows()),
            halves(second_rows()),
            halves(second_rows().T),
            halves(first_rows()),
            halves(first_rows().T),
            twiddles(),
            np.ascontiguousarray(gather_lanes().T),
            gather_lanes(),
        )
    ]
    operands = (
        field,
        cot,
        core.transpose(0, 2, 3, 4, 1).reshape(16, 512, 16),
        in_factor.T,
        out_factor.T,
        first.T,
        second.T,
        third.T,
        *constants,
    )
    vmem = pl.BlockSpec(memory_space=pltpu.VMEM)
    hbm = pl.BlockSpec(memory_space=pltpu.HBM)
    scratch = [pltpu.VMEM(v.shape, v.dtype) for v in operands] + [
        pltpu.VMEM((16, 16, 512), F32),
        pltpu.VMEM((2, 256, 512), BF16),
        pltpu.VMEM((1, 8, 128), F32),
        pltpu.VMEM((2, 512, 128), BF16),
        pltpu.VMEM((128, 1024), F32),
        pltpu.VMEM((128, 1024), F32),
        pltpu.VMEM((256, 2048), BF16),
        pltpu.VMEM((2, 2, 8, 8, 128), F32),
        pltpu.VMEM((16, 2, 8, 128), F32),
        pltpu.VMEM((16, 2, 8, 128), F32),
        pltpu.VMEM((2, 2, 8, 8, 128), F32),
        pltpu.VMEM((128, 1024), F32),
        pltpu.VMEM((128, 1024), F32),
        pltpu.VMEM((16, 16, 128), F32),
        pltpu.VMEM((16, 16, 128), F32),
        pltpu.VMEM((16, 16, 128), F32),
        pltpu.VMEM((16, 16, 128), F32),
        pltpu.VMEM((16, 128), F32),
        pltpu.VMEM((16, 16, 128), F32),
        pltpu.VMEM((16, 512), F32),
        pltpu.VMEM((16, 16, 512), F32),
        pltpu.VMEM((8, 2048), F32),
        pltpu.VMEM((8, 128), F32),
        pltpu.VMEM((2, 512, 128), F32),
        pltpu.VMEM((16, 2, 128), F32),
        pltpu.VMEM((16, 2, 128), F32),
        pltpu.VMEM((2, 128), F32),
        pltpu.VMEM((16, 2, 128), F32),
        pltpu.VMEM((2, 128), F32),
        pltpu.VMEM((16, 2, 128), F32),
        pltpu.SemaphoreType.DMA((10, COUNT)),
        pltpu.SemaphoreType.DMA((10, COUNT)),
        pltpu.SemaphoreType.DMA((len(operands),)),
    ]
    output, grad_core, small = pl.pallas_call(
        kernel,
        out_shape=(
            jax.ShapeDtypeStruct((64, 8, 8, 128), BF16),
            jax.ShapeDtypeStruct((16, 16, 512), F32),
            jax.ShapeDtypeStruct((16, 2, 128), F32),
        ),
        in_specs=[hbm] * len(operands),
        out_specs=[vmem] * 3,
        scratch_shapes=scratch,
        compiler_params=pltpu.CompilerParams(
            collective_id=0, has_side_effects=True, vmem_limit_bytes=67043328
        ),
        name="tucker_step",
    )(*operands)
    shapes = ((64, 8, 8, 128), (16, 512, 16), (16, 64), (16, 64), (8, 32), (8, 32), (8, 32))
    output, grad_core, *grads = pl.pallas_call(
        finish,
        out_shape=tuple(jax.ShapeDtypeStruct(v, BF16 if i == 0 else F32) for i, v in enumerate(shapes)),
        in_specs=[vmem] * 3,
        out_specs=[hbm] * 7,
        scratch_shapes=[pltpu.VMEM(v, F32) for v in shapes[1:]] + [pltpu.SemaphoreType.DMA((22,))],
        compiler_params=pltpu.CompilerParams(vmem_limit_bytes=67043328),
        name="finish",
    )(output, grad_core, small.reshape(32, 128))
    grad_core = grad_core.reshape(16, 8, 8, 8, 16).transpose(0, 4, 1, 2, 3)
    return (output, grad_core, *[g.T for g in grads])


def solution(mesh):
    grid = P(None, "px", "py", None)
    return jax.shard_map(
        shards,
        mesh=mesh,
        in_specs=(grid, grid) + (P(),) * 6,
        out_specs=(grid,) + (P(),) * 6,
        check_vma=False,
    )
```

```python
import functools
import math

import jax
import jax.numpy as jnp
import numpy as np
from jax import lax
from jax.experimental import pallas as pl
from jax.experimental.pallas import tpu as pltpu
from jax.sharding import PartitionSpec as P

F32 = jnp.float32
BF16 = jnp.bfloat16
HIGHEST = lax.Precision.HIGHEST
MESH = pl.DeviceIdType.MESH
COUNT = 16
CELLS = 128
SCALE = 1.0 / (CELLS * CELLS * CELLS)
NN = ((1,), (0,))
NT = ((1,), (1,))


def halves(table):
    high = table.astype(np.float32).astype(jnp.bfloat16)
    low = (table - high.astype(np.float64)).astype(np.float32).astype(jnp.bfloat16)
    return np.stack([high, low])


def depth_rows():
    row = np.arange(128)[:, None]
    lane = np.arange(256)[None, :]
    mode = row // 8 * 2 + row % 2
    angle = 2.0 * math.pi / CELLS * (mode * (lane % 128) % CELLS)
    value = np.where(row // 2 % 2 == 0, np.cos(angle), -np.sin(angle))
    return np.where(row // 4 % 2 == lane // 128, value, 0.0)


def short_transform(rows, row_of, col_of):
    row = np.arange(rows)[:, None]
    col = np.arange(rows)[None, :]
    part_out, freq, rest_out = row_of(row)
    part_in, block, rest_in = col_of(col)
    angle = 2.0 * math.pi / 16 * (freq * block % 16)
    sine = np.where(part_out == 0, 1.0, -1.0) * np.sin(angle)
    value = np.where(part_out == part_in, np.cos(angle), sine)
    return np.where(rest_out == rest_in, value, 0.0)


def second_rows():
    return short_transform(
        128,
        lambda r: (r // 64, r // 4 % 16, r % 4),
        lambda c: (c // 2 % 2, c // 8, c // 4 % 2 * 2 + c % 2),
    )


def first_rows():
    return short_transform(
        256,
        lambda r: (r // 128, r // 4 % 16, r // 64 % 2 * 4 + r % 4),
        lambda c: (c // 8 % 2, c // 16, c // 2 % 2 * 4 + c // 4 % 2 * 2 + c % 2),
    )


def twiddles():
    row = np.arange(64)[:, None]
    lane = np.arange(128)[None, :]
    tables = []
    for high in range(2):
        angle = 2.0 * math.pi / CELLS * ((row // 4 - 16 * high) * (lane // 16))
        tables.append(np.stack([np.cos(angle), np.sin(angle)]))
    return np.stack(tables).astype(np.float32)


def gather_lanes():
    row = np.arange(1024)[:, None]
    lane = np.arange(128)[None, :]
    return ((row // 128 == lane // 16) & (row % 16 == lane % 16)).astype(np.float32).astype(jnp.bfloat16)


def split(value):
    high = value.astype(BF16)
    return high, (value - high.astype(F32)).astype(BF16)


def mul(a, b, dims=NN):
    return lax.dot_general(a, b, (dims, ((), ())), preferred_element_type=F32)


def exact(a, b, dims=NN):
    return lax.dot_general(a, b, (dims, ((), ())), precision=HIGHEST, preferred_element_type=F32)


def mul3(a, b, dims=NN):
    return mul(a[0], b[0], dims) + mul(a[0], b[1], dims) + mul(a[1], b[0], dims)


def pair(ref):
    return ref[0], ref[1]


def iota(shape, axis):
    return lax.broadcasted_iota(jnp.int32, shape, axis)


def hot(test):
    return jnp.where(test, 1.0, 0.0).astype(F32)


def kernel(
    field_h, cot_h, core_h, in_h, out_h, first_h, second_h, third_h,
    tz_h, a1_h, a1t_h, a2_h, a2t_h, tw_h, spread_h, collect_h,
    output_h, packed_h, small_h,
    field, cot, core_n, in_t, out_t, first_t, second_t, third_t,
    tz, a1, a1t, a2, a2t, tw, spread, collect, core,
    m_in, back_map, given, s1, r1, s2, r2, s3, r3, s4, r4,
    kern, grad, s5, r8, s6, r9, s7, cg, spread_second, grids, output, ts, r5, t2, r6, small,
    send, recv, loads,
):
    px = lax.axis_index("px")
    py = lax.axis_index("py")
    barrier = pltpu.get_barrier_semaphore()

    def along_y(peer):
        return (px, peer)

    def along_x(peer):
        return (peer, py)

    staged = (
        (in_h, in_t), (out_h, out_t), (field_h, field), (cot_h, cot), (tz_h, tz),
        (first_h, first_t), (second_h, second_t), (third_h, third_t), (a1_h, a1), (tw_h, tw), (collect_h, collect),
        (core_h, core_n), (a2_h, a2), (a2t_h, a2t), (spread_h, spread), (a1t_h, a1t),
    )
    copies = [pltpu.make_async_copy(far, near, loads.at[i]) for i, (far, near) in enumerate(staged)]
    for c in copies:
        c.start()

    def greet(d, carry):
        pl.semaphore_signal(barrier, inc=1, device_id=along_y(lax.rem(py + d, COUNT)), device_id_type=MESH)
        pl.semaphore_signal(barrier, inc=1, device_id=along_x(lax.rem(px + d, COUNT)), device_id_type=MESH)
        return carry

    lax.fori_loop(1, COUNT, greet, 0)
    waits = []

    def start(phase, axis, source, target, every):
        me, device = (py, along_y) if axis == "y" else (px, along_x)

        def body(d, carry):
            peer = lax.rem(me + d, COUNT)
            pltpu.make_async_remote_copy(
                src_ref=source(peer),
                dst_ref=target(me),
                send_sem=send.at[phase],
                recv_sem=recv.at[phase],
                device_id=device(peer),
                device_id_type=MESH,
            ).start()
            return carry

        lax.fori_loop(1, COUNT, body, 0)
        total = pltpu.make_async_remote_copy(
            src_ref=every,
            dst_ref=every,
            send_sem=send.at[phase],
            recv_sem=recv.at[phase],
            device_id=device(lax.rem(me + 1, COUNT)),
            device_id_type=MESH,
        )
        waits.append(total)
        return total

    def rows8(ref, lanes):
        return lambda i: ref.at[pl.ds(pl.multiple_of(i * 8, 8), 8), lanes]

    def slab(ref, *rest):
        return lambda i: ref.at[(i, *rest)] if rest else ref.at[i]

    def block(ref):
        return lambda i: ref.at[lax.div(i, 8), :, lax.rem(i, 8)]

    def whole(ref):
        return lambda i: ref

    chunks = [pl.ds(c * 256, 256) for c in range(4)]
    own = pl.ds(pl.multiple_of(py * 8, 8), 8)

    copies[0].wait()
    copies[1].wait()
    lane = iota((16, 512), 1)
    repeat = hot(iota((64, 512), 1) // 8 == iota((64, 512), 0))
    maps = []
    for f, factor in enumerate((in_t, out_t)):
        wide_factor = exact(factor[...], repeat)
        maps.append(jnp.concatenate([jnp.where(lane % 8 == y, wide_factor, 0.0) for y in range(8)], axis=0))
        high, low = split(maps[f])
        m_in[f, 0:128] = high
        m_in[f, 128:256] = low

    for c in copies[2:5]:
        c.wait()
    tz_pair = pair(tz)
    outward = []
    for c in range(4):
        lifted = []
        for f, source in enumerate((field, cot)):
            for x in range(2):
                rows = source[:, 2 * c + x].astype(F32).reshape(512, 128).astype(BF16)
                given[f, :, (2 * c + x) * 128 : (2 * c + x + 1) * 128] = rows
            both = mul(m_in[f], given[f, :, c * 256 : (c + 1) * 256])
            lifted.append(both[0:128] + both[128:256])
        for x in range(2):
            both = jnp.concatenate([v[:, x * 128 : (x + 1) * 128] for v in lifted], axis=1)
            s1[:, (2 * c + x) * 128 : (2 * c + x + 1) * 128] = mul3(tz_pair, split(both), NT)
        if c == 0:
            pl.semaphore_wait(barrier, 2 * (COUNT - 1))
        outward.append(
            start(c, "y", rows8(s1, chunks[c]), rows8(r1, chunks[c]), r1.at[pl.ds(0, 120), chunks[c]])
        )
        r1[own, c * 256 : (c + 1) * 256] = s1[own, c * 256 : (c + 1) * 256]
    for c in copies[5:]:
        c.wait()

    mode = iota((32, 128), 1)
    row32 = iota((32, 128), 0)
    t1 = exact(first_t[...], hot(mode // 4 == row32))
    t2f = exact(second_t[...], hot(mode // 2 % 2 + 2 * px == row32))
    t3f = exact(third_t[...], hot(mode % 2 + 2 * py == row32))
    tiles = []
    for r in range(8):
        for s in range(8):
            tiles.append(t3f * (t1[r : r + 1] * t2f[s : s + 1]))
    phi_pair = split(jnp.concatenate(tiles, axis=0))
    for a in range(16):
        core[:, a] = core_n[a].T
    kern[...] = mul3(split(core[...].reshape(256, 512)), phi_pair).reshape(16, 16, 128)
    spread_second[...] = exact(second_t[...], hot(iota((32, 2048), 1) // 64 == iota((32, 2048), 0)))
    high, low = split(maps[1].T)
    back_map[0] = high
    back_map[1] = low

    a1_pair = pair(a1)
    gathered = jnp.zeros((256, 128), F32)
    for c in range(4):
        outward[c].wait_recv()
        middle = mul3(a1_pair, split(r1[:, c * 256 : (c + 1) * 256]))
        turned = []
        for x in range(2):
            real = middle[0:64, x * 128 : (x + 1) * 128]
            imag = middle[64:128, x * 128 : (x + 1) * 128]
            parts = []
            for h in range(2):
                cosine, sine = tw[h, 0], tw[h, 1]
                parts += [cosine * real + sine * imag, cosine * imag - sine * real]
            turned.append(jnp.concatenate(parts, axis=0))
        high, low = split(jnp.concatenate(turned, axis=1))
        places = collect[c * 256 : (c + 1) * 256]
        gathered = gathered + (mul(high, places) + mul(low, places))
    s2[...] = gathered.reshape(2, 2, 8, 8, 128)
    across = start(4, "x", block(s2), slab(r2), r2.at[pl.ds(0, 15)])
    r2[px] = s2[lax.div(px, 8), :, lax.rem(px, 8)]

    across.wait_recv()
    middle = mul3(pair(a2), split(r2[...].reshape(256, 128)))
    parts = []
    for p in range(2):
        for f in range(2):
            real = middle[f * 64 : f * 64 + 64]
            imag = middle[128 + f * 64 : 128 + f * 64 + 64]
            for h in range(2):
                cosine, sine = tw[h, 0], tw[h, 1]
                parts.append(cosine * real + sine * imag if p == 0 else cosine * imag - sine * real)
    high, low = split(jnp.concatenate(parts, axis=0))
    ones = hot(iota((16, 128), 1) % 16 == iota((16, 128), 0)).astype(BF16)
    modes = mul(ones, high, NT) + mul(ones, low, NT)

    depth_mode = iota((1, 128), 1) % 2 + 2 * py
    scale = jnp.where(depth_mode == 0, 1.0, 2.0).astype(F32) * SCALE
    lifted = [modes[:, p * 256 : p * 256 + 128] for p in range(2)]
    back = [modes[:, p * 256 + 128 : p * 256 + 256] * scale for p in range(2)]
    mixed = [jnp.zeros((16, 128), F32) for p in range(2)]
    lifted_back = [jnp.zeros((16, 128), F32) for p in range(2)]
    for i in range(16):
        over_a = kern[:, i]
        over_b = kern[i]
        for p in range(2):
            mixed[p] = mixed[p] + over_a * lifted[p][i : i + 1]
            lifted_back[p] = lifted_back[p] + over_b * back[p][i : i + 1]
    modes = jnp.concatenate([mixed[0] * scale, lifted_back[0], mixed[1] * scale, lifted_back[1]], axis=1)

    opened = jnp.concatenate([modes] * 8, axis=0).T
    parts = []
    for p in range(2):
        for f in range(2):
            total = None
            for h in range(2):
                cosine, sine = tw[h, 0], tw[h, 1]
                real = opened[f * 128 + h * 64 : f * 128 + h * 64 + 64]
                imag = opened[256 + f * 128 + h * 64 : 256 + f * 128 + h * 64 + 64]
                term = cosine * real - sine * imag if p == 0 else sine * real + cosine * imag
                total = term if total is None else total + term
            parts.append(total)
    s3[...] = mul3(pair(a2t), split(jnp.concatenate(parts, axis=0))).reshape(16, 2, 8, 128)
    across = start(5, "x", slab(s3), block(r3), s3.at[pl.ds(0, 15)])
    r3[lax.div(px, 8), :, lax.rem(px, 8)] = s3[px]

    for b in range(16):
        grad[b] = lifted[0] * back[0][b : b + 1] + lifted[1] * back[1][b : b + 1]
    grad_pair = split(grad[...].reshape(256, 128))
    tiles = []
    for k in range(2):
        kept = hot(iota((8, 128), 1) // 2 % 2 == k) * t3f
        for r in range(8):
            tiles.append(kept * t1[r : r + 1])
    s5[:, 0:16] = mul3(grad_pair, split(jnp.concatenate(tiles, axis=0)), NT).reshape(16, 16, 128)

    pulled = mul3(split(core[...].reshape(256, 512).T), grad_pair)
    by_first = []
    by_second = [jnp.zeros((8, 128), F32) for s in range(8)]
    by_third = jnp.zeros((8, 128), F32)
    for r in range(8):
        total = jnp.zeros((8, 128), F32)
        for s in range(8):
            tile = pulled[(r * 8 + s) * 8 : (r * 8 + s) * 8 + 8]
            total = total + tile * t2f[s : s + 1]
            by_second[s] = by_second[s] + tile * t1[r : r + 1]
        by_first.append(total)
        by_third = by_third + total * t1[r : r + 1]
    fold = hot(iota((8, 64), 1) // 8 == iota((8, 64), 0))
    first_rows8 = exact(fold, jnp.concatenate([t * t3f for t in by_first], axis=0))
    second_rows8 = exact(fold, jnp.concatenate([t * t3f for t in by_second], axis=0))
    row = iota((128, 128), 0)
    col = iota((128, 128), 1)
    factor_grads = (
        exact(first_rows8, hot(row // 4 == col))
        + exact(second_rows8, hot(row // 2 % 2 + 2 * px + 32 == col))
        + exact(by_third, hot(row % 2 + 2 * py + 64 == col))
    )
    for b in range(16):
        s5[b, 16:24] = factor_grads
    shares = start(6, "y", slab(s5), slab(r8), r8.at[pl.ds(0, 15)])
    r8[py] = s5[py]

    across.wait_recv()
    back_pair = split(r3[...].reshape(256, 128))
    a1t_pair = pair(a1t)
    inward = []
    for c in range(4):
        places = spread[:, c * 256 : (c + 1) * 256]
        opened = mul(back_pair[0], places) + mul(back_pair[1], places)
        turned = []
        for x in range(2):
            parts = []
            for p in range(2):
                total = None
                for h in range(2):
                    cosine, sine = tw[h, 0], tw[h, 1]
                    real = opened[h * 128 : h * 128 + 64, x * 128 : (x + 1) * 128]
                    imag = opened[h * 128 + 64 : h * 128 + 128, x * 128 : (x + 1) * 128]
                    term = cosine * real - sine * imag if p == 0 else sine * real + cosine * imag
                    total = term if total is None else total + term
                parts.append(total)
            turned.append(jnp.concatenate(parts, axis=0))
        s4[:, c * 256 : (c + 1) * 256] = mul3(a1t_pair, split(jnp.concatenate(turned, axis=1)))
        inward.append(
            start(7 + c, "y", rows8(s4, chunks[c]), rows8(r4, chunks[c]), r4.at[pl.ds(0, 120), chunks[c]])
        )
        r4[own, c * 256 : (c + 1) * 256] = s4[own, c * 256 : (c + 1) * 256]

        if c == 0:
            shares.wait_recv()
            total = r8[0]
            for q in range(1, 16):
                total = total + r8[q]
            s6[...] = total
            halves_in = start(11, "x", whole(s6), slab(r9), r9.at[pl.ds(0, 15)])
            r9[px] = s6[...]

    halves_in.wait_recv()
    totals = [jnp.zeros((16, 128), F32) for s in range(8)]
    factor_grads = r9[0, 16:24]
    for q in range(16):
        received = r9[q, 0:16]
        if q > 0:
            factor_grads = factor_grads + r9[q, 16:24]
        for s in range(8):
            totals[s] = totals[s] + received * spread_second[s : s + 1, q * 128 : (q + 1) * 128]
    small[16:24] = factor_grads
    totals = [t + pltpu.roll(t, 64, 1) for t in totals]
    left = iota((16, 128), 1) < 64
    for u in range(4):
        s7[:, u * 128 : (u + 1) * 128] = jnp.where(left, totals[2 * u], totals[2 * u + 1])

    def gather(phase, first):
        part = pl.ds(first, 8)
        return start(phase, "y", lambda i: s7.at[part], slab(cg, part), cg.at[pl.ds(0, 15), part])

    upper = gather(12, 0)
    cg[py] = s7[...]

    sums = [jnp.zeros((512, 128), F32) for f in range(2)]
    for c in range(4):
        inward[c].wait_recv()
        values = [[], []]
        for x in range(2):
            rows = r4[:, (2 * c + x) * 128 : (2 * c + x + 1) * 128].T
            both = mul3(split(rows), tz_pair)
            for f in range(2):
                values[f].append(split(both[:, (1 - f) * 128 : (2 - f) * 128]))
            grids[2 * c + x, 0], grids[2 * c + x, 1] = values[1][x]
        for f in range(2):
            rows = given[f, :, c * 256 : (c + 1) * 256]
            for h in range(2):
                sums[f] = sums[f] + mul(rows, jnp.concatenate([v[h] for v in values[f]], axis=1), NT)
    kept = hot(iota((512, 128), 0) % 8 == iota((512, 128), 1) // 16)
    sums = [jnp.sum((v * kept).reshape(64, 8, 128), axis=1) for v in sums]
    high, low = split(jnp.concatenate(sums, axis=0))
    ts[...] = mul(ones, high, NT) + mul(ones, low, NT)
    tail = start(14, "y", whole(ts), slab(r5), r5.at[pl.ds(0, 15)])
    r5[py] = ts[...]
    lower = gather(13, 8)

    back_maps = pair(back_map)

    def emit(x, carry):
        output[:, pl.ds(x, 1)] = mul3(back_maps, (grids[x, 0], grids[x, 1])).reshape(64, 1, 8, 128).astype(BF16)
        return carry

    lax.fori_loop(0, 4, emit, 0)

    tail.wait_recv()
    total = r5[0]
    for q in range(1, 16):
        total = total + r5[q]
    t2[...] = total
    tail = start(15, "x", whole(t2), slab(r6), r6.at[pl.ds(0, 15)])
    r6[px] = t2[...]
    lax.fori_loop(4, 8, emit, 0)
    done = [pltpu.make_async_copy(output, output_h, loads.at[0])]
    done[0].start()
    upper.wait_recv()
    lower.wait_recv()
    done.append(pltpu.make_async_copy(cg, packed_h, loads.at[1]))
    done[1].start()
    tail.wait_recv()
    total = r6[0]
    for q in range(1, 16):
        total = total + r6[q]
    small[0:16] = total
    done.append(pltpu.make_async_copy(small, small_h, loads.at[2]))
    done[2].start()
    for c in waits:
        c.wait_send()
    for c in done:
        c.wait()


def finish(
    output_i, packed_i, small_i,
    output_h, core_h, in_h, out_h, first_h, second_h, third_h,
    output, packed, small, core, grad_in, grad_out, grad_first, grad_second, grad_third, done,
):
    loads = (
        pltpu.make_async_copy(packed_i, packed, done.at[22]),
        pltpu.make_async_copy(small_i, small, done.at[23]),
        pltpu.make_async_copy(output_i, output, done.at[24]),
    )
    for c in loads:
        c.start()
    loads[0].wait()
    copies = []
    for a in range(16):
        rows = packed[:, a].T.reshape(8, 8, 8, 16)
        for s in range(8):
            for r in range(8):
                core[a, (r * 8 + s) * 8 : (r * 8 + s) * 8 + 8] = rows[s, r]
        copies.append(pltpu.make_async_copy(core.at[a], core_h.at[a], done.at[1 + a]))
        copies[-1].start()
        if a == 8:
            loads[1].wait()
            loads[2].wait()
            copies.append(pltpu.make_async_copy(output, output_h, done.at[0]))
            copies[-1].start()
    grad_in[...] = small[0:16, 0:64]
    grad_out[...] = small[0:16, 64:128]
    grad_first[...] = small[16:24, 0:32]
    grad_second[...] = small[16:24, 32:64]
    grad_third[...] = small[16:24, 64:96]
    pairs = ((grad_in, in_h), (grad_out, out_h), (grad_first, first_h), (grad_second, second_h), (grad_third, third_h))
    for i, (near, far) in enumerate(pairs):
        copies.append(pltpu.make_async_copy(near, far, done.at[17 + i]))
        copies[-1].start()
    for c in copies:
        c.wait()


def shards(field, cot, core, in_factor, out_factor, first, second, third):
    constants = [
        jnp.asarray(c)
        for c in (
            halves(depth_rows()),
            halves(second_rows()),
            halves(second_rows().T),
            halves(first_rows()),
            halves(first_rows().T),
            twiddles(),
            np.ascontiguousarray(gather_lanes().T),
            gather_lanes(),
        )
    ]
    operands = (
        field,
        cot,
        core.transpose(0, 2, 3, 4, 1).reshape(16, 512, 16),
        in_factor.T,
        out_factor.T,
        first.T,
        second.T,
        third.T,
        *constants,
    )
    hbm = pl.BlockSpec(memory_space=pltpu.HBM)
    scratch = [pltpu.VMEM(v.shape, v.dtype) for v in operands] + [
        pltpu.VMEM((16, 16, 512), F32),
        pltpu.VMEM((2, 256, 512), BF16),
        pltpu.VMEM((2, 512, 128), BF16),
        pltpu.VMEM((2, 512, 1024), BF16),
        pltpu.VMEM((128, 1024), F32),
        pltpu.VMEM((128, 1024), F32),
        pltpu.VMEM((2, 2, 8, 8, 128), F32),
        pltpu.VMEM((16, 2, 8, 128), F32),
        pltpu.VMEM((16, 2, 8, 128), F32),
        pltpu.VMEM((2, 2, 8, 8, 128), F32),
        pltpu.VMEM((128, 1024), F32),
        pltpu.VMEM((128, 1024), F32),
        pltpu.VMEM((16, 16, 128), F32),
        pltpu.VMEM((16, 16, 128), F32),
        pltpu.VMEM((16, 24, 128), F32),
        pltpu.VMEM((16, 24, 128), F32),
        pltpu.VMEM((24, 128), F32),
        pltpu.VMEM((16, 24, 128), F32),
        pltpu.VMEM((16, 512), F32),
        pltpu.VMEM((16, 16, 512), F32),
        pltpu.VMEM((8, 2048), F32),
        pltpu.VMEM((8, 2, 128, 128), BF16),
        pltpu.VMEM((64, 8, 8, 128), BF16),
        pltpu.VMEM((16, 128), F32),
        pltpu.VMEM((16, 16, 128), F32),
        pltpu.VMEM((16, 128), F32),
        pltpu.VMEM((16, 16, 128), F32),
        pltpu.VMEM((24, 128), F32),
        pltpu.SemaphoreType.DMA((16,)),
        pltpu.SemaphoreType.DMA((16,)),
        pltpu.SemaphoreType.DMA((len(operands),)),
    ]
    stages = (
        jax.ShapeDtypeStruct((64, 8, 8, 128), BF16),
        jax.ShapeDtypeStruct((16, 16, 512), F32),
        jax.ShapeDtypeStruct((24, 128), F32),
    )
    step = pl.pallas_call(
        kernel,
        out_shape=stages,
        in_specs=[hbm] * len(operands),
        out_specs=[hbm] * 3,
        scratch_shapes=scratch,
        compiler_params=pltpu.CompilerParams(
            collective_id=0, has_side_effects=True, vmem_limit_bytes=67043328
        ),
        name="tucker_step",
    )(*operands)
    shapes = ((64, 8, 8, 128), (16, 512, 16), (16, 64), (16, 64), (8, 32), (8, 32), (8, 32))
    output, grad_core, *grads = pl.pallas_call(
        finish,
        out_shape=tuple(jax.ShapeDtypeStruct(v, BF16 if i == 0 else F32) for i, v in enumerate(shapes)),
        in_specs=[hbm] * 3,
        out_specs=[hbm] * 7,
        scratch_shapes=[pltpu.VMEM(v.shape, v.dtype) for v in stages]
        + [pltpu.VMEM(v, F32) for v in shapes[1:]]
        + [pltpu.SemaphoreType.DMA((25,))],
        compiler_params=pltpu.CompilerParams(vmem_limit_bytes=67043328),
        name="finish",
    )(*step)
    grad_core = grad_core.reshape(16, 8, 8, 8, 16).transpose(0, 4, 1, 2, 3)
    return (output, grad_core, *[g.T for g in grads])


def solution(mesh):
    grid = P(None, "px", "py", None)
    return jax.shard_map(
        shards,
        mesh=mesh,
        in_specs=(grid, grid) + (P(),) * 6,
        out_specs=(grid,) + (P(),) * 6,
        check_vma=False,
    )
```

```python
import functools
import math

import jax
import jax.numpy as jnp
import numpy as np
from jax import lax
from jax.experimental import pallas as pl
from jax.experimental.pallas import tpu as pltpu
from jax.sharding import PartitionSpec as P

F32 = jnp.float32
BF16 = jnp.bfloat16
HIGHEST = lax.Precision.HIGHEST
MESH = pl.DeviceIdType.MESH
COUNT = 16
CELLS = 128
SCALE = 1.0 / (CELLS * CELLS * CELLS)
NN = ((1,), (0,))
FAR_FIRST_Y = sorted(
    ((x, y, c) for x in range(4) for y in range(2) for c in range(2) if x or y or c),
    key=lambda o: -(min(o[0], 4 - o[0]) + o[1]),
)
FAR_FIRST_X = sorted(
    ((z, y) for z in range(8) for y in range(2) if z or y),
    key=lambda o: -(min(o[0], 8 - o[0]) + 2 * o[1]),
)
NT = ((1,), (1,))


def halves(table):
    high = table.astype(np.float32).astype(jnp.bfloat16)
    low = (table - high.astype(np.float64)).astype(np.float32).astype(jnp.bfloat16)
    return np.stack([high, low])


def depth_rows():
    row = np.arange(128)[:, None]
    lane = np.arange(256)[None, :]
    mode = row // 8 * 2 + row % 2
    angle = 2.0 * math.pi / CELLS * (mode * (lane % 128) % CELLS)
    value = np.where(row // 2 % 2 == 0, np.cos(angle), -np.sin(angle))
    return np.where(row // 4 % 2 == lane // 128, value, 0.0)


def short_transform(rows, row_of, col_of):
    row = np.arange(rows)[:, None]
    col = np.arange(rows)[None, :]
    part_out, freq, rest_out = row_of(row)
    part_in, block, rest_in = col_of(col)
    angle = 2.0 * math.pi / 16 * (freq * block % 16)
    sine = np.where(part_out == 0, 1.0, -1.0) * np.sin(angle)
    value = np.where(part_out == part_in, np.cos(angle), sine)
    return np.where(rest_out == rest_in, value, 0.0)


def second_rows():
    return short_transform(
        128,
        lambda r: (r // 64, r // 4 % 16, r % 4),
        lambda c: (c // 2 % 2, c // 8, c // 4 % 2 * 2 + c % 2),
    )


def first_rows():
    return short_transform(
        256,
        lambda r: (r // 128, r // 4 % 16, r // 64 % 2 * 4 + r % 4),
        lambda c: (c // 8 % 2, c // 16, c // 2 % 2 * 4 + c // 4 % 2 * 2 + c % 2),
    )


def twiddles():
    row = np.arange(64)[:, None]
    lane = np.arange(128)[None, :]
    tables = []
    for high in range(2):
        angle = 2.0 * math.pi / CELLS * ((row // 4 - 16 * high) * (lane // 16))
        tables.append(np.stack([np.cos(angle), np.sin(angle)]))
    return np.stack(tables).astype(np.float32)


def gather_lanes():
    row = np.arange(1024)[:, None]
    lane = np.arange(128)[None, :]
    return ((row // 128 == lane // 16) & (row % 16 == lane % 16)).astype(np.float32).astype(jnp.bfloat16)


def split(value):
    high = value.astype(BF16)
    return high, (value - high.astype(F32)).astype(BF16)


def mul(a, b, dims=NN):
    return lax.dot_general(a, b, (dims, ((), ())), preferred_element_type=F32)


def exact(a, b, dims=NN):
    return lax.dot_general(a, b, (dims, ((), ())), precision=HIGHEST, preferred_element_type=F32)


def mul3(a, b, dims=NN):
    return mul(a[0], b[0], dims) + mul(a[0], b[1], dims) + mul(a[1], b[0], dims)


def pair(ref):
    return ref[0], ref[1]


def iota(shape, axis):
    return lax.broadcasted_iota(jnp.int32, shape, axis)


def hot(test):
    return jnp.where(test, 1.0, 0.0).astype(F32)


def kernel(
    field_h, cot_h, core_h, in_h, out_h, first_h, second_h, third_h,
    tz_h, a1_h, a1t_h, a2_h, a2t_h, tw_h, spread_h, collect_h,
    output_h, packed_h, small_h,
    field, cot, core_n, in_t, out_t, first_t, second_t, third_t,
    tz, a1, a1t, a2, a2t, tw, spread, collect, core,
    m_in, back_map, given, s1, r1, s2, r2, s3, r3, s4, r4,
    kern, grad, s5, r8, s6, r9, s7, cg, spread_second, grids, output, ts, r5, t2, r6, small,
    send, recv, loads,
):
    px = lax.axis_index("px")
    py = lax.axis_index("py")
    barrier = pltpu.get_barrier_semaphore()

    def along_y(peer):
        return (px, peer)

    def along_x(peer):
        return (peer, py)

    staged = (
        (in_h, in_t), (out_h, out_t), (field_h, field), (cot_h, cot), (tz_h, tz),
        (first_h, first_t), (second_h, second_t), (third_h, third_t), (a1_h, a1), (tw_h, tw), (collect_h, collect),
        (core_h, core_n), (a2_h, a2), (a2t_h, a2t), (spread_h, spread), (a1t_h, a1t),
    )
    copies = [pltpu.make_async_copy(far, near, loads.at[i]) for i, (far, near) in enumerate(staged)]
    for c in copies:
        c.start()

    def greet(d, carry):
        pl.semaphore_signal(barrier, inc=1, device_id=along_y(lax.rem(py + d, COUNT)), device_id_type=MESH)
        pl.semaphore_signal(barrier, inc=1, device_id=along_x(lax.rem(px + d, COUNT)), device_id_type=MESH)
        return carry

    lax.fori_loop(1, COUNT, greet, 0)
    waits = []

    x_at = [lax.rem(lax.div(py, 4) + d, 4) * 4 for d in range(4)]
    y_at = [lax.rem(lax.rem(lax.div(py, 2), 2) + d, 2) * 2 for d in range(2)]
    core_at = [lax.rem(lax.rem(py, 2) + d, 2) for d in range(2)]
    z_at = [lax.rem(lax.div(px, 2) + d, 8) * 2 for d in range(8)]
    far_at = [lax.rem(lax.rem(px, 2) + d, 2) for d in range(2)]
    peers_y = [x_at[x] + y_at[y] + core_at[c] for x, y, c in FAR_FIRST_Y]
    peers_x = [z_at[z] + far_at[y] for z, y in FAR_FIRST_X]

    def start(phase, axis, source, target, every):
        me, device, peers = (py, along_y, peers_y) if axis == "y" else (px, along_x, peers_x)
        for peer in peers:
            pltpu.make_async_remote_copy(
                src_ref=source(peer),
                dst_ref=target(me),
                send_sem=send.at[phase],
                recv_sem=recv.at[phase],
                device_id=device(peer),
                device_id_type=MESH,
            ).start()
        total = pltpu.make_async_remote_copy(
            src_ref=every,
            dst_ref=every,
            send_sem=send.at[phase],
            recv_sem=recv.at[phase],
            device_id=device(peers[0]),
            device_id_type=MESH,
        )
        waits.append(total)
        return total

    def rows8(ref, lanes):
        return lambda i: ref.at[pl.ds(pl.multiple_of(i * 8, 8), 8), lanes]

    def slab(ref, *rest):
        return lambda i: ref.at[(i, *rest)] if rest else ref.at[i]

    def block(ref):
        return lambda i: ref.at[lax.div(i, 8), :, lax.rem(i, 8)]

    def whole(ref):
        return lambda i: ref

    chunks = [pl.ds(c * 256, 256) for c in range(4)]
    own = pl.ds(pl.multiple_of(py * 8, 8), 8)

    copies[0].wait()
    copies[1].wait()
    lane = iota((16, 512), 1)
    repeat = hot(iota((64, 512), 1) // 8 == iota((64, 512), 0))
    maps = []
    for f, factor in enumerate((in_t, out_t)):
        wide_factor = exact(factor[...], repeat)
        maps.append(jnp.concatenate([jnp.where(lane % 8 == y, wide_factor, 0.0) for y in range(8)], axis=0))
        high, low = split(maps[f])
        m_in[f, 0:128] = high
        m_in[f, 128:256] = low

    for c in copies[2:5]:
        c.wait()
    tz_pair = pair(tz)
    outward = []
    for c in range(4):
        lifted = []
        for f, source in enumerate((field, cot)):
            for x in range(2):
                rows = source[:, 2 * c + x].astype(F32).reshape(512, 128).astype(BF16)
                given[f, :, (2 * c + x) * 128 : (2 * c + x + 1) * 128] = rows
            both = mul(m_in[f], given[f, :, c * 256 : (c + 1) * 256])
            lifted.append(both[0:128] + both[128:256])
        for x in range(2):
            both = jnp.concatenate([v[:, x * 128 : (x + 1) * 128] for v in lifted], axis=1)
            s1[:, (2 * c + x) * 128 : (2 * c + x + 1) * 128] = mul3(tz_pair, split(both), NT)
        if c == 0:
            pl.semaphore_wait(barrier, 2 * (COUNT - 1))
        outward.append(
            start(c, "y", rows8(s1, chunks[c]), rows8(r1, chunks[c]), r1.at[pl.ds(0, 120), chunks[c]])
        )
        r1[own, c * 256 : (c + 1) * 256] = s1[own, c * 256 : (c + 1) * 256]
    for c in copies[5:]:
        c.wait()

    mode = iota((32, 128), 1)
    row32 = iota((32, 128), 0)
    t1 = exact(first_t[...], hot(mode // 4 == row32))
    t2f = exact(second_t[...], hot(mode // 2 % 2 + 2 * px == row32))
    t3f = exact(third_t[...], hot(mode % 2 + 2 * py == row32))
    tiles = []
    for r in range(8):
        for s in range(8):
            tiles.append(t3f * (t1[r : r + 1] * t2f[s : s + 1]))
    phi_pair = split(jnp.concatenate(tiles, axis=0))
    for a in range(16):
        core[:, a] = core_n[a].T
    kern[...] = mul3(split(core[...].reshape(256, 512)), phi_pair).reshape(16, 16, 128)
    spread_second[...] = exact(second_t[...], hot(iota((32, 2048), 1) // 64 == iota((32, 2048), 0)))
    high, low = split(maps[1].T)
    back_map[0] = high
    back_map[1] = low

    a1_pair = pair(a1)
    gathered = jnp.zeros((256, 128), F32)
    for c in range(4):
        outward[c].wait_recv()
        middle = mul3(a1_pair, split(r1[:, c * 256 : (c + 1) * 256]))
        turned = []
        for x in range(2):
            real = middle[0:64, x * 128 : (x + 1) * 128]
            imag = middle[64:128, x * 128 : (x + 1) * 128]
            parts = []
            for h in range(2):
                cosine, sine = tw[h, 0], tw[h, 1]
                parts += [cosine * real + sine * imag, cosine * imag - sine * real]
            turned.append(jnp.concatenate(parts, axis=0))
        high, low = split(jnp.concatenate(turned, axis=1))
        places = collect[c * 256 : (c + 1) * 256]
        gathered = gathered + (mul(high, places) + mul(low, places))
    s2[...] = gathered.reshape(2, 2, 8, 8, 128)
    across = start(4, "x", block(s2), slab(r2), r2.at[pl.ds(0, 15)])
    r2[px] = s2[lax.div(px, 8), :, lax.rem(px, 8)]

    across.wait_recv()
    middle = mul3(pair(a2), split(r2[...].reshape(256, 128)))
    parts = []
    for p in range(2):
        for f in range(2):
            real = middle[f * 64 : f * 64 + 64]
            imag = middle[128 + f * 64 : 128 + f * 64 + 64]
            for h in range(2):
                cosine, sine = tw[h, 0], tw[h, 1]
                parts.append(cosine * real + sine * imag if p == 0 else cosine * imag - sine * real)
    high, low = split(jnp.concatenate(parts, axis=0))
    ones = hot(iota((16, 128), 1) % 16 == iota((16, 128), 0)).astype(BF16)
    modes = mul(ones, high, NT) + mul(ones, low, NT)

    depth_mode = iota((1, 128), 1) % 2 + 2 * py
    scale = jnp.where(depth_mode == 0, 1.0, 2.0).astype(F32) * SCALE
    lifted = [modes[:, p * 256 : p * 256 + 128] for p in range(2)]
    back = [modes[:, p * 256 + 128 : p * 256 + 256] * scale for p in range(2)]
    mixed = [jnp.zeros((16, 128), F32) for p in range(2)]
    lifted_back = [jnp.zeros((16, 128), F32) for p in range(2)]
    for i in range(16):
        over_a = kern[:, i]
        over_b = kern[i]
        for p in range(2):
            mixed[p] = mixed[p] + over_a * lifted[p][i : i + 1]
            lifted_back[p] = lifted_back[p] + over_b * back[p][i : i + 1]
    modes = jnp.concatenate([mixed[0] * scale, lifted_back[0], mixed[1] * scale, lifted_back[1]], axis=1)

    opened = jnp.concatenate([modes] * 8, axis=0).T
    parts = []
    for p in range(2):
        for f in range(2):
            total = None
            for h in range(2):
                cosine, sine = tw[h, 0], tw[h, 1]
                real = opened[f * 128 + h * 64 : f * 128 + h * 64 + 64]
                imag = opened[256 + f * 128 + h * 64 : 256 + f * 128 + h * 64 + 64]
                term = cosine * real - sine * imag if p == 0 else sine * real + cosine * imag
                total = term if total is None else total + term
            parts.append(total)
    s3[...] = mul3(pair(a2t), split(jnp.concatenate(parts, axis=0))).reshape(16, 2, 8, 128)
    across = start(5, "x", slab(s3), block(r3), s3.at[pl.ds(0, 15)])
    r3[lax.div(px, 8), :, lax.rem(px, 8)] = s3[px]

    for b in range(16):
        grad[b] = lifted[0] * back[0][b : b + 1] + lifted[1] * back[1][b : b + 1]
    grad_pair = split(grad[...].reshape(256, 128))
    tiles = []
    for k in range(2):
        kept = hot(iota((8, 128), 1) // 2 % 2 == k) * t3f
        for r in range(8):
            tiles.append(kept * t1[r : r + 1])
    s5[:, 0:16] = mul3(grad_pair, split(jnp.concatenate(tiles, axis=0)), NT).reshape(16, 16, 128)

    pulled = mul3(split(core[...].reshape(256, 512).T), grad_pair)
    by_first = []
    by_second = [jnp.zeros((8, 128), F32) for s in range(8)]
    by_third = jnp.zeros((8, 128), F32)
    for r in range(8):
        total = jnp.zeros((8, 128), F32)
        for s in range(8):
            tile = pulled[(r * 8 + s) * 8 : (r * 8 + s) * 8 + 8]
            total = total + tile * t2f[s : s + 1]
            by_second[s] = by_second[s] + tile * t1[r : r + 1]
        by_first.append(total)
        by_third = by_third + total * t1[r : r + 1]
    fold = hot(iota((8, 64), 1) // 8 == iota((8, 64), 0))
    first_rows8 = exact(fold, jnp.concatenate([t * t3f for t in by_first], axis=0))
    second_rows8 = exact(fold, jnp.concatenate([t * t3f for t in by_second], axis=0))
    row = iota((128, 128), 0)
    col = iota((128, 128), 1)
    factor_grads = (
        exact(first_rows8, hot(row // 4 == col))
        + exact(second_rows8, hot(row // 2 % 2 + 2 * px + 32 == col))
        + exact(by_third, hot(row % 2 + 2 * py + 64 == col))
    )
    for b in range(16):
        s5[b, 16:24] = factor_grads
    shares = start(6, "y", slab(s5), slab(r8), r8.at[pl.ds(0, 15)])
    r8[py] = s5[py]

    across.wait_recv()
    back_pair = split(r3[...].reshape(256, 128))
    a1t_pair = pair(a1t)
    inward = []
    for c in range(4):
        places = spread[:, c * 256 : (c + 1) * 256]
        opened = mul(back_pair[0], places) + mul(back_pair[1], places)
        turned = []
        for x in range(2):
            parts = []
            for p in range(2):
                total = None
                for h in range(2):
                    cosine, sine = tw[h, 0], tw[h, 1]
                    real = opened[h * 128 : h * 128 + 64, x * 128 : (x + 1) * 128]
                    imag = opened[h * 128 + 64 : h * 128 + 128, x * 128 : (x + 1) * 128]
                    term = cosine * real - sine * imag if p == 0 else sine * real + cosine * imag
                    total = term if total is None else total + term
                parts.append(total)
            turned.append(jnp.concatenate(parts, axis=0))
        s4[:, c * 256 : (c + 1) * 256] = mul3(a1t_pair, split(jnp.concatenate(turned, axis=1)))
        inward.append(
            start(7 + c, "y", rows8(s4, chunks[c]), rows8(r4, chunks[c]), r4.at[pl.ds(0, 120), chunks[c]])
        )
        r4[own, c * 256 : (c + 1) * 256] = s4[own, c * 256 : (c + 1) * 256]

        if c == 0:
            shares.wait_recv()
            total = r8[0]
            for q in range(1, 16):
                total = total + r8[q]
            s6[...] = total
            r9[px] = total
    halves_in = start(11, "x", whole(s6), slab(r9), r9.at[pl.ds(0, 15)])

    sums = [jnp.zeros((512, 128), F32) for f in range(2)]
    for c in range(4):
        inward[c].wait_recv()
        values = [[], []]
        for x in range(2):
            rows = r4[:, (2 * c + x) * 128 : (2 * c + x + 1) * 128].T
            both = mul3(split(rows), tz_pair)
            for f in range(2):
                values[f].append(split(both[:, (1 - f) * 128 : (2 - f) * 128]))
            grids[2 * c + x, 0], grids[2 * c + x, 1] = values[1][x]
        for f in range(2):
            rows = given[f, :, c * 256 : (c + 1) * 256]
            for h in range(2):
                sums[f] = sums[f] + mul(rows, jnp.concatenate([v[h] for v in values[f]], axis=1), NT)
    kept = hot(iota((512, 128), 0) % 8 == iota((512, 128), 1) // 16)
    sums = [jnp.sum((v * kept).reshape(64, 8, 128), axis=1) for v in sums]
    high, low = split(jnp.concatenate(sums, axis=0))
    ts[...] = mul(ones, high, NT) + mul(ones, low, NT)
    tail = start(14, "y", whole(ts), slab(r5), r5.at[pl.ds(0, 15)])
    r5[py] = ts[...]

    halves_in.wait_recv()
    totals = [jnp.zeros((16, 128), F32) for s in range(8)]
    factor_grads = r9[0, 16:24]
    for q in range(16):
        received = r9[q, 0:16]
        if q > 0:
            factor_grads = factor_grads + r9[q, 16:24]
        for s in range(8):
            totals[s] = totals[s] + received * spread_second[s : s + 1, q * 128 : (q + 1) * 128]
    small[16:24] = factor_grads
    totals = [t + pltpu.roll(t, 64, 1) for t in totals]
    left = iota((16, 128), 1) < 64
    for u in range(4):
        s7[:, u * 128 : (u + 1) * 128] = jnp.where(left, totals[2 * u], totals[2 * u + 1])

    core_parts = start(12, "y", whole(s7), slab(cg), cg.at[pl.ds(0, 15)])
    cg[py] = s7[...]

    back_maps = pair(back_map)

    def emit(x, carry):
        output[:, pl.ds(x, 1)] = mul3(back_maps, (grids[x, 0], grids[x, 1])).reshape(64, 1, 8, 128).astype(BF16)
        return carry

    lax.fori_loop(0, 4, emit, 0)

    tail.wait_recv()
    total = r5[0]
    for q in range(1, 16):
        total = total + r5[q]
    t2[...] = total
    tail = start(15, "x", whole(t2), slab(r6), r6.at[pl.ds(0, 15)])
    r6[px] = t2[...]
    lax.fori_loop(4, 8, emit, 0)
    done = [pltpu.make_async_copy(output, output_h, loads.at[0])]
    done[0].start()
    core_parts.wait_recv()
    done.append(pltpu.make_async_copy(cg, packed_h, loads.at[1]))
    done[1].start()
    tail.wait_recv()
    total = r6[0]
    for q in range(1, 16):
        total = total + r6[q]
    small[0:16] = total
    done.append(pltpu.make_async_copy(small, small_h, loads.at[2]))
    done[2].start()
    for c in waits:
        c.wait_send()
    for c in done:
        c.wait()


def finish(
    output_i, packed_i, small_i,
    output_h, core_h, in_h, out_h, first_h, second_h, third_h,
    output, packed, small, core, grad_in, grad_out, grad_first, grad_second, grad_third, done,
):
    loads = (
        pltpu.make_async_copy(packed_i, packed, done.at[22]),
        pltpu.make_async_copy(small_i, small, done.at[23]),
        pltpu.make_async_copy(output_i, output, done.at[24]),
    )
    for c in loads:
        c.start()
    loads[0].wait()
    copies = []
    for a in range(16):
        rows = packed[:, a].T.reshape(8, 8, 8, 16)
        for s in range(8):
            for r in range(8):
                core[a, (r * 8 + s) * 8 : (r * 8 + s) * 8 + 8] = rows[s, r]
        copies.append(pltpu.make_async_copy(core.at[a], core_h.at[a], done.at[1 + a]))
        copies[-1].start()
        if a == 8:
            loads[1].wait()
            loads[2].wait()
            copies.append(pltpu.make_async_copy(output, output_h, done.at[0]))
            copies[-1].start()
    grad_in[...] = small[0:16, 0:64]
    grad_out[...] = small[0:16, 64:128]
    grad_first[...] = small[16:24, 0:32]
    grad_second[...] = small[16:24, 32:64]
    grad_third[...] = small[16:24, 64:96]
    pairs = ((grad_in, in_h), (grad_out, out_h), (grad_first, first_h), (grad_second, second_h), (grad_third, third_h))
    for i, (near, far) in enumerate(pairs):
        copies.append(pltpu.make_async_copy(near, far, done.at[17 + i]))
        copies[-1].start()
    for c in copies:
        c.wait()


def shards(field, cot, core, in_factor, out_factor, first, second, third):
    constants = [
        jnp.asarray(c)
        for c in (
            halves(depth_rows()),
            halves(second_rows()),
            halves(second_rows().T),
            halves(first_rows()),
            halves(first_rows().T),
            twiddles(),
            np.ascontiguousarray(gather_lanes().T),
            gather_lanes(),
        )
    ]
    operands = (
        field,
        cot,
        core.transpose(0, 2, 3, 4, 1).reshape(16, 512, 16),
        in_factor.T,
        out_factor.T,
        first.T,
        second.T,
        third.T,
        *constants,
    )
    hbm = pl.BlockSpec(memory_space=pltpu.HBM)
    scratch = [pltpu.VMEM(v.shape, v.dtype) for v in operands] + [
        pltpu.VMEM((16, 16, 512), F32),
        pltpu.VMEM((2, 256, 512), BF16),
        pltpu.VMEM((2, 512, 128), BF16),
        pltpu.VMEM((2, 512, 1024), BF16),
        pltpu.VMEM((128, 1024), F32),
        pltpu.VMEM((128, 1024), F32),
        pltpu.VMEM((2, 2, 8, 8, 128), F32),
        pltpu.VMEM((16, 2, 8, 128), F32),
        pltpu.VMEM((16, 2, 8, 128), F32),
        pltpu.VMEM((2, 2, 8, 8, 128), F32),
        pltpu.VMEM((128, 1024), F32),
        pltpu.VMEM((128, 1024), F32),
        pltpu.VMEM((16, 16, 128), F32),
        pltpu.VMEM((16, 16, 128), F32),
        pltpu.VMEM((16, 24, 128), F32),
        pltpu.VMEM((16, 24, 128), F32),
        pltpu.VMEM((24, 128), F32),
        pltpu.VMEM((16, 24, 128), F32),
        pltpu.VMEM((16, 512), F32),
        pltpu.VMEM((16, 16, 512), F32),
        pltpu.VMEM((8, 2048), F32),
        pltpu.VMEM((8, 2, 128, 128), BF16),
        pltpu.VMEM((64, 8, 8, 128), BF16),
        pltpu.VMEM((16, 128), F32),
        pltpu.VMEM((16, 16, 128), F32),
        pltpu.VMEM((16, 128), F32),
        pltpu.VMEM((16, 16, 128), F32),
        pltpu.VMEM((24, 128), F32),
        pltpu.SemaphoreType.DMA((16,)),
        pltpu.SemaphoreType.DMA((16,)),
        pltpu.SemaphoreType.DMA((len(operands),)),
    ]
    stages = (
        jax.ShapeDtypeStruct((64, 8, 8, 128), BF16),
        jax.ShapeDtypeStruct((16, 16, 512), F32),
        jax.ShapeDtypeStruct((24, 128), F32),
    )
    step = pl.pallas_call(
        kernel,
        out_shape=stages,
        in_specs=[hbm] * len(operands),
        out_specs=[hbm] * 3,
        scratch_shapes=scratch,
        compiler_params=pltpu.CompilerParams(
            collective_id=0, has_side_effects=True, vmem_limit_bytes=67043328
        ),
        name="tucker_step",
    )(*operands)
    shapes = ((64, 8, 8, 128), (16, 512, 16), (16, 64), (16, 64), (8, 32), (8, 32), (8, 32))
    output, grad_core, *grads = pl.pallas_call(
        finish,
        out_shape=tuple(jax.ShapeDtypeStruct(v, BF16 if i == 0 else F32) for i, v in enumerate(shapes)),
        in_specs=[hbm] * 3,
        out_specs=[hbm] * 7,
        scratch_shapes=[pltpu.VMEM(v.shape, v.dtype) for v in stages]
        + [pltpu.VMEM(v, F32) for v in shapes[1:]]
        + [pltpu.SemaphoreType.DMA((25,))],
        compiler_params=pltpu.CompilerParams(vmem_limit_bytes=67043328),
        name="finish",
    )(*step)
    grad_core = grad_core.reshape(16, 8, 8, 8, 16).transpose(0, 4, 1, 2, 3)
    return (output, grad_core, *[g.T for g in grads])


def solution(mesh):
    grid = P(None, "px", "py", None)
    return jax.shard_map(
        shards,
        mesh=mesh,
        in_specs=(grid, grid) + (P(),) * 6,
        out_specs=(grid,) + (P(),) * 6,
        check_vma=False,
    )
```

```python
import functools
import math

import jax
import jax.numpy as jnp
import numpy as np
from jax import lax
from jax.experimental import pallas as pl
from jax.experimental.pallas import tpu as pltpu
from jax.sharding import PartitionSpec as P

F32 = jnp.float32
BF16 = jnp.bfloat16
HIGHEST = lax.Precision.HIGHEST
MESH = pl.DeviceIdType.MESH
COUNT = 16
CELLS = 128
SCALE = 1.0 / (CELLS * CELLS * CELLS)
NN = ((1,), (0,))
FAR_FIRST_Y = sorted(
    ((x, y, c) for x in range(4) for y in range(2) for c in range(2) if x or y or c),
    key=lambda o: -(min(o[0], 4 - o[0]) + o[1]),
)
FAR_FIRST_X = sorted(
    ((z, y) for z in range(8) for y in range(2) if z or y),
    key=lambda o: -(min(o[0], 8 - o[0]) + 2 * o[1]),
)
NT = ((1,), (1,))


def halves(table):
    high = table.astype(np.float32).astype(jnp.bfloat16)
    low = (table - high.astype(np.float64)).astype(np.float32).astype(jnp.bfloat16)
    return np.stack([high, low])


def depth_rows():
    row = np.arange(128)[:, None]
    lane = np.arange(256)[None, :]
    mode = row // 8 * 2 + row % 2
    angle = 2.0 * math.pi / CELLS * (mode * (lane % 128) % CELLS)
    value = np.where(row // 2 % 2 == 0, np.cos(angle), -np.sin(angle))
    return np.where(row // 4 % 2 == lane // 128, value, 0.0)


def short_transform(rows, row_of, col_of):
    row = np.arange(rows)[:, None]
    col = np.arange(rows)[None, :]
    part_out, freq, rest_out = row_of(row)
    part_in, block, rest_in = col_of(col)
    angle = 2.0 * math.pi / 16 * (freq * block % 16)
    sine = np.where(part_out == 0, 1.0, -1.0) * np.sin(angle)
    value = np.where(part_out == part_in, np.cos(angle), sine)
    return np.where(rest_out == rest_in, value, 0.0)


def second_rows():
    return short_transform(
        128,
        lambda r: (r // 64, r // 4 % 16, r % 4),
        lambda c: (c // 2 % 2, c // 8, c // 4 % 2 * 2 + c % 2),
    )


def first_rows():
    return short_transform(
        256,
        lambda r: (r // 128, r // 4 % 16, r // 64 % 2 * 4 + r % 4),
        lambda c: (c // 8 % 2, c // 16, c // 2 % 2 * 4 + c // 4 % 2 * 2 + c % 2),
    )


def twiddles():
    row = np.arange(64)[:, None]
    lane = np.arange(128)[None, :]
    tables = []
    for high in range(2):
        angle = 2.0 * math.pi / CELLS * ((row // 4 - 16 * high) * (lane // 16))
        tables.append(np.stack([np.cos(angle), np.sin(angle)]))
    return np.stack(tables).astype(np.float32)


def gather_lanes():
    row = np.arange(1024)[:, None]
    lane = np.arange(128)[None, :]
    return ((row // 128 == lane // 16) & (row % 16 == lane % 16)).astype(np.float32).astype(jnp.bfloat16)


def split(value):
    high = value.astype(BF16)
    return high, (value - high.astype(F32)).astype(BF16)


def mul(a, b, dims=NN):
    return lax.dot_general(a, b, (dims, ((), ())), preferred_element_type=F32)


def exact(a, b, dims=NN):
    return lax.dot_general(a, b, (dims, ((), ())), precision=HIGHEST, preferred_element_type=F32)


def mul3(a, b, dims=NN):
    return mul(a[0], b[0], dims) + mul(a[0], b[1], dims) + mul(a[1], b[0], dims)


def pair(ref):
    return ref[0], ref[1]


def iota(shape, axis):
    return lax.broadcasted_iota(jnp.int32, shape, axis)


def hot(test):
    return jnp.where(test, 1.0, 0.0).astype(F32)


def kernel(
    field_h, cot_h, core_h, in_h, out_h, first_h, second_h, third_h,
    tz_h, a1_h, a1t_h, a2_h, a2t_h, tw_h, spread_h, collect_h,
    output_h, packed_h, small_h,
    field, cot, core_n, in_t, out_t, first_t, second_t, third_t,
    tz, a1, a1t, a2, a2t, tw, spread, collect, core,
    m_in, back_map, given, s1, r1, s2, r2, s3, r3, s4, r4,
    kern, grad, s5, r8, s6, r9, s7, cg, spread_second, grids, output, ts, r5, t2, r6, small,
    send, recv, loads,
):
    px = lax.axis_index("px")
    py = lax.axis_index("py")
    barrier = pltpu.get_barrier_semaphore()

    def along_y(peer):
        return (px, peer)

    def along_x(peer):
        return (peer, py)

    staged = (
        (in_h, in_t), (out_h, out_t), (field_h, field), (cot_h, cot), (tz_h, tz),
        (first_h, first_t), (second_h, second_t), (third_h, third_t), (a1_h, a1), (tw_h, tw), (collect_h, collect),
        (core_h, core_n), (a2_h, a2), (a2t_h, a2t), (spread_h, spread), (a1t_h, a1t),
    )
    copies = [pltpu.make_async_copy(far, near, loads.at[i]) for i, (far, near) in enumerate(staged)]
    for c in copies:
        c.start()

    def greet(d, carry):
        pl.semaphore_signal(barrier, inc=1, device_id=along_y(lax.rem(py + d, COUNT)), device_id_type=MESH)
        pl.semaphore_signal(barrier, inc=1, device_id=along_x(lax.rem(px + d, COUNT)), device_id_type=MESH)
        return carry

    lax.fori_loop(1, COUNT, greet, 0)
    waits = []

    x_at = [lax.rem(lax.div(py, 4) + d, 4) * 4 for d in range(4)]
    y_at = [lax.rem(lax.rem(lax.div(py, 2), 2) + d, 2) * 2 for d in range(2)]
    core_at = [lax.rem(lax.rem(py, 2) + d, 2) for d in range(2)]
    z_at = [lax.rem(lax.div(px, 2) + d, 8) * 2 for d in range(8)]
    far_at = [lax.rem(lax.rem(px, 2) + d, 2) for d in range(2)]
    peers_y = [x_at[x] + y_at[y] + core_at[c] for x, y, c in FAR_FIRST_Y]
    peers_x = [z_at[z] + far_at[y] for z, y in FAR_FIRST_X]

    def start(phase, axis, source, target, every, some=None):
        me, device, peers = (py, along_y, some or peers_y) if axis == "y" else (px, along_x, peers_x)
        for peer in peers:
            pltpu.make_async_remote_copy(
                src_ref=source(peer),
                dst_ref=target(me),
                send_sem=send.at[phase],
                recv_sem=recv.at[phase],
                device_id=device(peer),
                device_id_type=MESH,
            ).start()
        total = pltpu.make_async_remote_copy(
            src_ref=every,
            dst_ref=every,
            send_sem=send.at[phase],
            recv_sem=recv.at[phase],
            device_id=device(peers[0]),
            device_id_type=MESH,
        )
        waits.append(total)
        return total

    def rows8(ref, lanes):
        return lambda i: ref.at[pl.ds(pl.multiple_of(i * 8, 8), 8), lanes]

    def slab(ref, *rest):
        return lambda i: ref.at[(i, *rest)] if rest else ref.at[i]

    def block(ref):
        return lambda i: ref.at[lax.div(i, 8), :, lax.rem(i, 8)]

    def whole(ref):
        return lambda i: ref

    chunks = [pl.ds(c * 256, 256) for c in range(4)]
    own = pl.ds(pl.multiple_of(py * 8, 8), 8)

    copies[0].wait()
    copies[1].wait()
    lane = iota((16, 512), 1)
    repeat = hot(iota((64, 512), 1) // 8 == iota((64, 512), 0))
    maps = []
    for f, factor in enumerate((in_t, out_t)):
        wide_factor = exact(factor[...], repeat)
        maps.append(jnp.concatenate([jnp.where(lane % 8 == y, wide_factor, 0.0) for y in range(8)], axis=0))
        high, low = split(maps[f])
        m_in[f, 0:128] = high
        m_in[f, 128:256] = low

    for c in copies[2:5]:
        c.wait()
    tz_pair = pair(tz)
    outward = []
    for c in range(4):
        lifted = []
        for f, source in enumerate((field, cot)):
            for x in range(2):
                rows = source[:, 2 * c + x].astype(F32).reshape(512, 128).astype(BF16)
                given[f, :, (2 * c + x) * 128 : (2 * c + x + 1) * 128] = rows
            both = mul(m_in[f], given[f, :, c * 256 : (c + 1) * 256])
            lifted.append(both[0:128] + both[128:256])
        for x in range(2):
            both = jnp.concatenate([v[:, x * 128 : (x + 1) * 128] for v in lifted], axis=1)
            s1[:, (2 * c + x) * 128 : (2 * c + x + 1) * 128] = mul3(tz_pair, split(both), NT)
        if c == 0:
            pl.semaphore_wait(barrier, 2 * (COUNT - 1))
        outward.append(
            start(c, "y", rows8(s1, chunks[c]), rows8(r1, chunks[c]), r1.at[pl.ds(0, 120), chunks[c]])
        )
        r1[own, c * 256 : (c + 1) * 256] = s1[own, c * 256 : (c + 1) * 256]
    for c in copies[5:]:
        c.wait()

    mode = iota((32, 128), 1)
    row32 = iota((32, 128), 0)
    t1 = exact(first_t[...], hot(mode // 4 == row32))
    t2f = exact(second_t[...], hot(mode // 2 % 2 + 2 * px == row32))
    t3f = exact(third_t[...], hot(mode % 2 + 2 * py == row32))
    tiles = []
    for r in range(8):
        for s in range(8):
            tiles.append(t3f * (t1[r : r + 1] * t2f[s : s + 1]))
    phi_pair = split(jnp.concatenate(tiles, axis=0))
    for a in range(16):
        core[:, a] = core_n[a].T
    kern[...] = mul3(split(core[...].reshape(256, 512)), phi_pair).reshape(16, 16, 128)
    spread_second[...] = exact(second_t[...], hot(iota((32, 2048), 1) // 64 == iota((32, 2048), 0)))
    high, low = split(maps[1].T)
    back_map[0] = high
    back_map[1] = low

    a1_pair = pair(a1)
    gathered = jnp.zeros((256, 128), F32)
    for c in range(4):
        outward[c].wait_recv()
        middle = mul3(a1_pair, split(r1[:, c * 256 : (c + 1) * 256]))
        turned = []
        for x in range(2):
            real = middle[0:64, x * 128 : (x + 1) * 128]
            imag = middle[64:128, x * 128 : (x + 1) * 128]
            parts = []
            for h in range(2):
                cosine, sine = tw[h, 0], tw[h, 1]
                parts += [cosine * real + sine * imag, cosine * imag - sine * real]
            turned.append(jnp.concatenate(parts, axis=0))
        high, low = split(jnp.concatenate(turned, axis=1))
        places = collect[c * 256 : (c + 1) * 256]
        gathered = gathered + (mul(high, places) + mul(low, places))
    s2[...] = gathered.reshape(2, 2, 8, 8, 128)
    across = start(4, "x", block(s2), slab(r2), r2.at[pl.ds(0, 15)])
    r2[px] = s2[lax.div(px, 8), :, lax.rem(px, 8)]

    across.wait_recv()
    middle = mul3(pair(a2), split(r2[...].reshape(256, 128)))
    parts = []
    for p in range(2):
        for f in range(2):
            real = middle[f * 64 : f * 64 + 64]
            imag = middle[128 + f * 64 : 128 + f * 64 + 64]
            for h in range(2):
                cosine, sine = tw[h, 0], tw[h, 1]
                parts.append(cosine * real + sine * imag if p == 0 else cosine * imag - sine * real)
    high, low = split(jnp.concatenate(parts, axis=0))
    ones = hot(iota((16, 128), 1) % 16 == iota((16, 128), 0)).astype(BF16)
    modes = mul(ones, high, NT) + mul(ones, low, NT)

    depth_mode = iota((1, 128), 1) % 2 + 2 * py
    scale = jnp.where(depth_mode == 0, 1.0, 2.0).astype(F32) * SCALE
    lifted = [modes[:, p * 256 : p * 256 + 128] for p in range(2)]
    back = [modes[:, p * 256 + 128 : p * 256 + 256] * scale for p in range(2)]
    mixed = [jnp.zeros((16, 128), F32) for p in range(2)]
    lifted_back = [jnp.zeros((16, 128), F32) for p in range(2)]
    for i in range(16):
        over_a = kern[:, i]
        over_b = kern[i]
        for p in range(2):
            mixed[p] = mixed[p] + over_a * lifted[p][i : i + 1]
            lifted_back[p] = lifted_back[p] + over_b * back[p][i : i + 1]
    modes = jnp.concatenate([mixed[0] * scale, lifted_back[0], mixed[1] * scale, lifted_back[1]], axis=1)

    opened = jnp.concatenate([modes] * 8, axis=0).T
    parts = []
    for p in range(2):
        for f in range(2):
            total = None
            for h in range(2):
                cosine, sine = tw[h, 0], tw[h, 1]
                real = opened[f * 128 + h * 64 : f * 128 + h * 64 + 64]
                imag = opened[256 + f * 128 + h * 64 : 256 + f * 128 + h * 64 + 64]
                term = cosine * real - sine * imag if p == 0 else sine * real + cosine * imag
                total = term if total is None else total + term
            parts.append(total)
    s3[...] = mul3(pair(a2t), split(jnp.concatenate(parts, axis=0))).reshape(16, 2, 8, 128)
    across = start(5, "x", slab(s3), block(r3), s3.at[pl.ds(0, 15)])
    r3[lax.div(px, 8), :, lax.rem(px, 8)] = s3[px]

    for b in range(16):
        grad[b] = lifted[0] * back[0][b : b + 1] + lifted[1] * back[1][b : b + 1]
    grad_pair = split(grad[...].reshape(256, 128))
    tiles = []
    for k in range(2):
        kept = hot(iota((8, 128), 1) // 2 % 2 == k) * t3f
        for r in range(8):
            tiles.append(kept * t1[r : r + 1])
    s5[...] = mul3(grad_pair, split(jnp.concatenate(tiles, axis=0)), NT).reshape(16, 16, 128)
    shares = start(6, "y", slab(s5), slab(r8), r8.at[pl.ds(0, 15)])
    r8[py] = s5[py]

    pulled = mul3(split(core[...].reshape(256, 512).T), grad_pair)
    by_first = []
    by_second = [jnp.zeros((8, 128), F32) for s in range(8)]
    by_third = jnp.zeros((8, 128), F32)
    for r in range(8):
        total = jnp.zeros((8, 128), F32)
        for s in range(8):
            tile = pulled[(r * 8 + s) * 8 : (r * 8 + s) * 8 + 8]
            total = total + tile * t2f[s : s + 1]
            by_second[s] = by_second[s] + tile * t1[r : r + 1]
        by_first.append(total)
        by_third = by_third + total * t1[r : r + 1]
    fold = hot(iota((8, 64), 1) // 8 == iota((8, 64), 0))
    first_rows8 = exact(fold, jnp.concatenate([t * t3f for t in by_first], axis=0))
    second_rows8 = exact(fold, jnp.concatenate([t * t3f for t in by_second], axis=0))
    row = iota((128, 128), 0)
    col = iota((128, 128), 1)
    factor_grads = (
        exact(first_rows8, hot(row // 4 == col))
        + exact(second_rows8, hot(row // 2 % 2 + 2 * px + 32 == col))
        + exact(by_third, hot(row % 2 + 2 * py + 64 == col))
    )

    across.wait_recv()
    back_pair = split(r3[...].reshape(256, 128))
    a1t_pair = pair(a1t)
    inward = []
    for c in range(4):
        places = spread[:, c * 256 : (c + 1) * 256]
        opened = mul(back_pair[0], places) + mul(back_pair[1], places)
        turned = []
        for x in range(2):
            parts = []
            for p in range(2):
                total = None
                for h in range(2):
                    cosine, sine = tw[h, 0], tw[h, 1]
                    real = opened[h * 128 : h * 128 + 64, x * 128 : (x + 1) * 128]
                    imag = opened[h * 128 + 64 : h * 128 + 128, x * 128 : (x + 1) * 128]
                    term = cosine * real - sine * imag if p == 0 else sine * real + cosine * imag
                    total = term if total is None else total + term
                parts.append(total)
            turned.append(jnp.concatenate(parts, axis=0))
        s4[:, c * 256 : (c + 1) * 256] = mul3(a1t_pair, split(jnp.concatenate(turned, axis=1)))
        inward.append(
            start(7 + c, "y", rows8(s4, chunks[c]), rows8(r4, chunks[c]), r4.at[pl.ds(0, 120), chunks[c]])
        )
        r4[own, c * 256 : (c + 1) * 256] = s4[own, c * 256 : (c + 1) * 256]

        if c == 0:
            shares.wait_recv()
            total = r8[0]
            for q in range(1, 16):
                total = total + r8[q]
            s6[...] = total
            r9[px] = total
    halves_in = start(11, "x", whole(s6), slab(r9), r9.at[pl.ds(0, 15)])

    sums = [jnp.zeros((512, 128), F32) for f in range(2)]
    for c in range(4):
        inward[c].wait_recv()
        values = [[], []]
        for x in range(2):
            rows = r4[:, (2 * c + x) * 128 : (2 * c + x + 1) * 128].T
            both = mul3(split(rows), tz_pair)
            for f in range(2):
                values[f].append(split(both[:, (1 - f) * 128 : (2 - f) * 128]))
            grids[2 * c + x, 0], grids[2 * c + x, 1] = values[1][x]
        for f in range(2):
            rows = given[f, :, c * 256 : (c + 1) * 256]
            for h in range(2):
                sums[f] = sums[f] + mul(rows, jnp.concatenate([v[h] for v in values[f]], axis=1), NT)
    kept = hot(iota((512, 128), 0) % 8 == iota((512, 128), 1) // 16)
    sums = [jnp.sum((v * kept).reshape(64, 8, 128), axis=1) for v in sums]
    high, low = split(jnp.concatenate(sums, axis=0))
    ts[0:16] = mul(ones, high, NT) + mul(ones, low, NT)
    ts[16:24] = factor_grads
    tail = start(14, "y", whole(ts), slab(r5), r5.at[pl.ds(0, 15)])
    r5[py] = ts[...]

    halves_in.wait_recv()
    totals = [jnp.zeros((16, 128), F32) for s in range(8)]
    for q in range(16):
        received = r9[q]
        for s in range(8):
            totals[s] = totals[s] + received * spread_second[s : s + 1, q * 128 : (q + 1) * 128]
    totals = [t + pltpu.roll(t, 64, 1) for t in totals]
    left = iota((16, 128), 1) < 64
    for u in range(4):
        s7[:, u * 128 : (u + 1) * 128] = jnp.where(left, totals[2 * u], totals[2 * u + 1])

    mine, chip = lax.rem(py, 2), lax.div(py, 2)
    core_parts = start(
        12, "y", whole(s7), lambda i: cg.at[mine, chip], cg.at[0, pl.ds(0, 7)], [p for p, o in zip(peers_y, FAR_FIRST_Y) if o[2] == 0]
    )
    cg[mine, chip] = s7[...]

    back_maps = pair(back_map)

    def emit(x, carry):
        output[:, pl.ds(x, 1)] = mul3(back_maps, (grids[x, 0], grids[x, 1])).reshape(64, 1, 8, 128).astype(BF16)
        return carry

    lax.fori_loop(0, 4, emit, 0)

    tail.wait_recv()
    total = r5[0]
    for q in range(1, 16):
        total = total + r5[q]
    t2[...] = total
    tail = start(15, "x", whole(t2), slab(r6), r6.at[pl.ds(0, 15)])
    r6[px] = t2[...]
    lax.fori_loop(4, 8, emit, 0)
    done = [pltpu.make_async_copy(output, output_h, loads.at[0])]
    done[0].start()
    core_parts.wait_recv()
    mate = [p for p, o in zip(peers_y, FAR_FIRST_Y) if o == (0, 0, 1)]
    core_parts = start(13, "y", lambda i: cg.at[mine], lambda i: cg.at[mine], cg.at[0], mate)
    core_parts.wait_recv()
    for c in range(2):
        done.append(pltpu.make_async_copy(cg.at[c], packed_h.at[:, c], loads.at[3 + c]))
        done[-1].start()
    tail.wait_recv()
    total = r6[0]
    for q in range(1, 16):
        total = total + r6[q]
    small[...] = total
    done.append(pltpu.make_async_copy(small, small_h, loads.at[2]))
    done[-1].start()
    for c in waits:
        c.wait_send()
    for c in done:
        c.wait()


def finish(
    output_i, packed_i, small_i,
    output_h, core_h, in_h, out_h, first_h, second_h, third_h,
    output, packed, small, core, grad_in, grad_out, grad_first, grad_second, grad_third, done,
):
    loads = (
        pltpu.make_async_copy(packed_i, packed, done.at[22]),
        pltpu.make_async_copy(small_i, small, done.at[23]),
        pltpu.make_async_copy(output_i, output, done.at[24]),
    )
    for c in loads:
        c.start()
    loads[0].wait()
    copies = []
    for a in range(16):
        rows = packed[:, :, a].reshape(16, 512).T.reshape(8, 8, 8, 16)
        for s in range(8):
            for r in range(8):
                core[a, (r * 8 + s) * 8 : (r * 8 + s) * 8 + 8] = rows[s, r]
        copies.append(pltpu.make_async_copy(core.at[a], core_h.at[a], done.at[1 + a]))
        copies[-1].start()
        if a == 8:
            loads[1].wait()
            loads[2].wait()
            copies.append(pltpu.make_async_copy(output, output_h, done.at[0]))
            copies[-1].start()
    grad_in[...] = small[0:16, 0:64]
    grad_out[...] = small[0:16, 64:128]
    grad_first[...] = small[16:24, 0:32]
    grad_second[...] = small[16:24, 32:64]
    grad_third[...] = small[16:24, 64:96]
    pairs = ((grad_in, in_h), (grad_out, out_h), (grad_first, first_h), (grad_second, second_h), (grad_third, third_h))
    for i, (near, far) in enumerate(pairs):
        copies.append(pltpu.make_async_copy(near, far, done.at[17 + i]))
        copies[-1].start()
    for c in copies:
        c.wait()


def shards(field, cot, core, in_factor, out_factor, first, second, third):
    constants = [
        jnp.asarray(c)
        for c in (
            halves(depth_rows()),
            halves(second_rows()),
            halves(second_rows().T),
            halves(first_rows()),
            halves(first_rows().T),
            twiddles(),
            np.ascontiguousarray(gather_lanes().T),
            gather_lanes(),
        )
    ]
    operands = (
        field,
        cot,
        core.transpose(0, 2, 3, 4, 1).reshape(16, 512, 16),
        in_factor.T,
        out_factor.T,
        first.T,
        second.T,
        third.T,
        *constants,
    )
    hbm = pl.BlockSpec(memory_space=pltpu.HBM)
    scratch = [pltpu.VMEM(v.shape, v.dtype) for v in operands] + [
        pltpu.VMEM((16, 16, 512), F32),
        pltpu.VMEM((2, 256, 512), BF16),
        pltpu.VMEM((2, 512, 128), BF16),
        pltpu.VMEM((2, 512, 1024), BF16),
        pltpu.VMEM((128, 1024), F32),
        pltpu.VMEM((128, 1024), F32),
        pltpu.VMEM((2, 2, 8, 8, 128), F32),
        pltpu.VMEM((16, 2, 8, 128), F32),
        pltpu.VMEM((16, 2, 8, 128), F32),
        pltpu.VMEM((2, 2, 8, 8, 128), F32),
        pltpu.VMEM((128, 1024), F32),
        pltpu.VMEM((128, 1024), F32),
        pltpu.VMEM((16, 16, 128), F32),
        pltpu.VMEM((16, 16, 128), F32),
        pltpu.VMEM((16, 16, 128), F32),
        pltpu.VMEM((16, 16, 128), F32),
        pltpu.VMEM((16, 128), F32),
        pltpu.VMEM((16, 16, 128), F32),
        pltpu.VMEM((16, 512), F32),
        pltpu.VMEM((2, 8, 16, 512), F32),
        pltpu.VMEM((8, 2048), F32),
        pltpu.VMEM((8, 2, 128, 128), BF16),
        pltpu.VMEM((64, 8, 8, 128), BF16),
        pltpu.VMEM((24, 128), F32),
        pltpu.VMEM((16, 24, 128), F32),
        pltpu.VMEM((24, 128), F32),
        pltpu.VMEM((16, 24, 128), F32),
        pltpu.VMEM((24, 128), F32),
        pltpu.SemaphoreType.DMA((16,)),
        pltpu.SemaphoreType.DMA((16,)),
        pltpu.SemaphoreType.DMA((len(operands),)),
    ]
    stages = (
        jax.ShapeDtypeStruct((64, 8, 8, 128), BF16),
        jax.ShapeDtypeStruct((8, 2, 16, 512), F32),
        jax.ShapeDtypeStruct((24, 128), F32),
    )
    step = pl.pallas_call(
        kernel,
        out_shape=stages,
        in_specs=[hbm] * len(operands),
        out_specs=[hbm] * 3,
        scratch_shapes=scratch,
        compiler_params=pltpu.CompilerParams(
            collective_id=0, has_side_effects=True, vmem_limit_bytes=67043328
        ),
        name="tucker_step",
    )(*operands)
    shapes = ((64, 8, 8, 128), (16, 512, 16), (16, 64), (16, 64), (8, 32), (8, 32), (8, 32))
    output, grad_core, *grads = pl.pallas_call(
        finish,
        out_shape=tuple(jax.ShapeDtypeStruct(v, BF16 if i == 0 else F32) for i, v in enumerate(shapes)),
        in_specs=[hbm] * 3,
        out_specs=[hbm] * 7,
        scratch_shapes=[pltpu.VMEM(v.shape, v.dtype) for v in stages]
        + [pltpu.VMEM(v, F32) for v in shapes[1:]]
        + [pltpu.SemaphoreType.DMA((25,))],
        compiler_params=pltpu.CompilerParams(vmem_limit_bytes=67043328),
        name="finish",
    )(*step)
    grad_core = grad_core.reshape(16, 8, 8, 8, 16).transpose(0, 4, 1, 2, 3)
    return (output, grad_core, *[g.T for g in grads])


def solution(mesh):
    grid = P(None, "px", "py", None)
    return jax.shard_map(
        shards,
        mesh=mesh,
        in_specs=(grid, grid) + (P(),) * 6,
        out_specs=(grid,) + (P(),) * 6,
        check_vma=False,
    )
```

```python
import functools
import math

import jax
import jax.numpy as jnp
import numpy as np
from jax import lax
from jax.experimental import pallas as pl
from jax.experimental.pallas import tpu as pltpu
from jax.sharding import PartitionSpec as P

F32 = jnp.float32
BF16 = jnp.bfloat16
HIGHEST = lax.Precision.HIGHEST
MESH = pl.DeviceIdType.MESH
COUNT = 16
CELLS = 128
SCALE = 1.0 / (CELLS * CELLS * CELLS)
NN = ((1,), (0,))
FAR_FIRST_Y = sorted(
    ((x, y, c) for x in range(4) for y in range(2) for c in range(2) if x or y or c),
    key=lambda o: -(min(o[0], 4 - o[0]) + o[1]),
)
FAR_FIRST_X = sorted(
    ((z, y) for z in range(8) for y in range(2) if z or y),
    key=lambda o: -(min(o[0], 8 - o[0]) + 2 * o[1]),
)
NT = ((1,), (1,))


def halves(table):
    high = table.astype(np.float32).astype(jnp.bfloat16)
    low = (table - high.astype(np.float64)).astype(np.float32).astype(jnp.bfloat16)
    return np.stack([high, low])


def depth_rows():
    row = np.arange(128)[:, None]
    lane = np.arange(256)[None, :]
    mode = row // 8 * 2 + row % 2
    angle = 2.0 * math.pi / CELLS * (mode * (lane % 128) % CELLS)
    value = np.where(row // 2 % 2 == 0, np.cos(angle), -np.sin(angle))
    return np.where(row // 4 % 2 == lane // 128, value, 0.0)


def short_transform(rows, row_of, col_of):
    row = np.arange(rows)[:, None]
    col = np.arange(rows)[None, :]
    part_out, freq, rest_out = row_of(row)
    part_in, block, rest_in = col_of(col)
    angle = 2.0 * math.pi / 16 * (freq * block % 16)
    sine = np.where(part_out == 0, 1.0, -1.0) * np.sin(angle)
    value = np.where(part_out == part_in, np.cos(angle), sine)
    return np.where(rest_out == rest_in, value, 0.0)


def second_rows():
    return short_transform(
        128,
        lambda r: (r // 64, r // 4 % 16, r % 4),
        lambda c: (c // 2 % 2, c // 8, c // 4 % 2 * 2 + c % 2),
    )


def first_rows():
    return short_transform(
        256,
        lambda r: (r // 128, r // 4 % 16, r // 64 % 2 * 4 + r % 4),
        lambda c: (c // 8 % 2, c // 16, c // 2 % 2 * 4 + c // 4 % 2 * 2 + c % 2),
    )


def twiddles():
    row = np.arange(64)[:, None]
    lane = np.arange(128)[None, :]
    tables = []
    for high in range(2):
        angle = 2.0 * math.pi / CELLS * ((row // 4 - 16 * high) * (lane // 16))
        tables.append(np.stack([np.cos(angle), np.sin(angle)]))
    return np.stack(tables).astype(np.float32)


def gather_lanes():
    row = np.arange(1024)[:, None]
    lane = np.arange(128)[None, :]
    return ((row // 128 == lane // 16) & (row % 16 == lane % 16)).astype(np.float32).astype(jnp.bfloat16)


def split(value):
    high = value.astype(BF16)
    return high, (value - high.astype(F32)).astype(BF16)


def mul(a, b, dims=NN):
    return lax.dot_general(a, b, (dims, ((), ())), preferred_element_type=F32)


def exact(a, b, dims=NN):
    return lax.dot_general(a, b, (dims, ((), ())), precision=HIGHEST, preferred_element_type=F32)


def mul3(a, b, dims=NN):
    return mul(a[0], b[0], dims) + mul(a[0], b[1], dims) + mul(a[1], b[0], dims)


def pair(ref):
    return ref[0], ref[1]


def iota(shape, axis):
    return lax.broadcasted_iota(jnp.int32, shape, axis)


def hot(test):
    return jnp.where(test, 1.0, 0.0).astype(F32)


def kernel(
    field_h, cot_h, core_h, in_h, out_h, first_h, second_h, third_h,
    tz_h, a1_h, a1t_h, a2_h, a2t_h, tw_h, spread_h, collect_h,
    output_h, packed_h, small_h,
    field, cot, core_n, in_t, out_t, first_t, second_t, third_t,
    tz, a1, a1t, a2, a2t, tw, spread, collect, core,
    m_in, back_map, given, s1, r1, s2, r2, s3, r3, s4, r4,
    kern, grad, s5, r8, s6, r9, s7, cg, spread_second, grids, output, ts, r5, t2,
    send, recv, loads,
):
    px = lax.axis_index("px")
    py = lax.axis_index("py")
    barrier = pltpu.get_barrier_semaphore()

    def along_y(peer):
        return (px, peer)

    def along_x(peer):
        return (peer, py)

    staged = (
        (in_h, in_t), (out_h, out_t), (field_h, field), (cot_h, cot), (tz_h, tz),
        (first_h, first_t), (second_h, second_t), (third_h, third_t), (a1_h, a1), (tw_h, tw), (collect_h, collect),
        (core_h, core_n), (a2_h, a2), (a2t_h, a2t), (spread_h, spread), (a1t_h, a1t),
    )
    copies = [pltpu.make_async_copy(far, near, loads.at[i]) for i, (far, near) in enumerate(staged)]
    for c in copies:
        c.start()

    def greet(d, carry):
        pl.semaphore_signal(barrier, inc=1, device_id=along_y(lax.rem(py + d, COUNT)), device_id_type=MESH)
        pl.semaphore_signal(barrier, inc=1, device_id=along_x(lax.rem(px + d, COUNT)), device_id_type=MESH)
        return carry

    lax.fori_loop(1, COUNT, greet, 0)
    waits = []

    x_at = [lax.rem(lax.div(py, 4) + d, 4) * 4 for d in range(4)]
    y_at = [lax.rem(lax.rem(lax.div(py, 2), 2) + d, 2) * 2 for d in range(2)]
    core_at = [lax.rem(lax.rem(py, 2) + d, 2) for d in range(2)]
    z_at = [lax.rem(lax.div(px, 2) + d, 8) * 2 for d in range(8)]
    far_at = [lax.rem(lax.rem(px, 2) + d, 2) for d in range(2)]
    peers_y = [x_at[x] + y_at[y] + core_at[c] for x, y, c in FAR_FIRST_Y]
    peers_x = [z_at[z] + far_at[y] for z, y in FAR_FIRST_X]

    def start(phase, axis, source, target, every, some=None):
        me, device, peers = (py, along_y, some or peers_y) if axis == "y" else (px, along_x, peers_x)
        for peer in peers:
            pltpu.make_async_remote_copy(
                src_ref=source(peer),
                dst_ref=target(me),
                send_sem=send.at[phase],
                recv_sem=recv.at[phase],
                device_id=device(peer),
                device_id_type=MESH,
            ).start()
        total = pltpu.make_async_remote_copy(
            src_ref=every,
            dst_ref=every,
            send_sem=send.at[phase],
            recv_sem=recv.at[phase],
            device_id=device(peers[0]),
            device_id_type=MESH,
        )
        waits.append(total)
        return total

    def rows8(ref, lanes):
        return lambda i: ref.at[pl.ds(pl.multiple_of(i * 8, 8), 8), lanes]

    def slab(ref, *rest):
        return lambda i: ref.at[(i, *rest)] if rest else ref.at[i]

    def block(ref):
        return lambda i: ref.at[lax.div(i, 8), :, lax.rem(i, 8)]

    def whole(ref):
        return lambda i: ref

    chunks = [pl.ds(c * 256, 256) for c in range(4)]
    own = pl.ds(pl.multiple_of(py * 8, 8), 8)

    copies[0].wait()
    copies[1].wait()
    lane = iota((16, 512), 1)
    repeat = hot(iota((64, 512), 1) // 8 == iota((64, 512), 0))
    maps = []
    for f, factor in enumerate((in_t, out_t)):
        wide_factor = exact(factor[...], repeat)
        maps.append(jnp.concatenate([jnp.where(lane % 8 == y, wide_factor, 0.0) for y in range(8)], axis=0))
        high, low = split(maps[f])
        m_in[f, 0:128] = high
        m_in[f, 128:256] = low

    for c in copies[2:5]:
        c.wait()
    tz_pair = pair(tz)
    outward = []
    for c in range(4):
        lifted = []
        for f, source in enumerate((field, cot)):
            for x in range(2):
                rows = source[:, 2 * c + x].astype(F32).reshape(512, 128).astype(BF16)
                given[f, :, (2 * c + x) * 128 : (2 * c + x + 1) * 128] = rows
            both = mul(m_in[f], given[f, :, c * 256 : (c + 1) * 256])
            lifted.append(both[0:128] + both[128:256])
        for x in range(2):
            both = jnp.concatenate([v[:, x * 128 : (x + 1) * 128] for v in lifted], axis=1)
            s1[:, (2 * c + x) * 128 : (2 * c + x + 1) * 128] = mul3(tz_pair, split(both), NT)
        if c == 0:
            pl.semaphore_wait(barrier, 2 * (COUNT - 1))
        outward.append(
            start(c, "y", rows8(s1, chunks[c]), rows8(r1, chunks[c]), r1.at[pl.ds(0, 120), chunks[c]])
        )
        r1[own, c * 256 : (c + 1) * 256] = s1[own, c * 256 : (c + 1) * 256]
    for c in copies[5:]:
        c.wait()

    mode = iota((32, 128), 1)
    row32 = iota((32, 128), 0)
    t1 = exact(first_t[...], hot(mode // 4 == row32))
    t2f = exact(second_t[...], hot(mode // 2 % 2 + 2 * px == row32))
    t3f = exact(third_t[...], hot(mode % 2 + 2 * py == row32))
    tiles = []
    for r in range(8):
        for s in range(8):
            tiles.append(t3f * (t1[r : r + 1] * t2f[s : s + 1]))
    phi_pair = split(jnp.concatenate(tiles, axis=0))
    for a in range(16):
        core[:, a] = core_n[a].T
    kern[...] = mul3(split(core[...].reshape(256, 512)), phi_pair).reshape(16, 16, 128)
    spread_second[...] = exact(second_t[...], hot(iota((32, 2048), 1) // 64 == iota((32, 2048), 0)))
    high, low = split(maps[1].T)
    back_map[0] = high
    back_map[1] = low

    a1_pair = pair(a1)
    gathered = jnp.zeros((256, 128), F32)
    for c in range(4):
        outward[c].wait_recv()
        middle = mul3(a1_pair, split(r1[:, c * 256 : (c + 1) * 256]))
        turned = []
        for x in range(2):
            real = middle[0:64, x * 128 : (x + 1) * 128]
            imag = middle[64:128, x * 128 : (x + 1) * 128]
            parts = []
            for h in range(2):
                cosine, sine = tw[h, 0], tw[h, 1]
                parts += [cosine * real + sine * imag, cosine * imag - sine * real]
            turned.append(jnp.concatenate(parts, axis=0))
        high, low = split(jnp.concatenate(turned, axis=1))
        places = collect[c * 256 : (c + 1) * 256]
        gathered = gathered + (mul(high, places) + mul(low, places))
    s2[...] = gathered.reshape(2, 2, 8, 8, 128)
    across = start(4, "x", block(s2), slab(r2), r2.at[pl.ds(0, 15)])
    r2[px] = s2[lax.div(px, 8), :, lax.rem(px, 8)]

    across.wait_recv()
    middle = mul3(pair(a2), split(r2[...].reshape(256, 128)))
    parts = []
    for p in range(2):
        for f in range(2):
            real = middle[f * 64 : f * 64 + 64]
            imag = middle[128 + f * 64 : 128 + f * 64 + 64]
            for h in range(2):
                cosine, sine = tw[h, 0], tw[h, 1]
                parts.append(cosine * real + sine * imag if p == 0 else cosine * imag - sine * real)
    high, low = split(jnp.concatenate(parts, axis=0))
    ones = hot(iota((16, 128), 1) % 16 == iota((16, 128), 0)).astype(BF16)
    modes = mul(ones, high, NT) + mul(ones, low, NT)

    depth_mode = iota((1, 128), 1) % 2 + 2 * py
    scale = jnp.where(depth_mode == 0, 1.0, 2.0).astype(F32) * SCALE
    lifted = [modes[:, p * 256 : p * 256 + 128] for p in range(2)]
    back = [modes[:, p * 256 + 128 : p * 256 + 256] * scale for p in range(2)]
    mixed = [jnp.zeros((16, 128), F32) for p in range(2)]
    lifted_back = [jnp.zeros((16, 128), F32) for p in range(2)]
    for i in range(16):
        over_a = kern[:, i]
        over_b = kern[i]
        for p in range(2):
            mixed[p] = mixed[p] + over_a * lifted[p][i : i + 1]
            lifted_back[p] = lifted_back[p] + over_b * back[p][i : i + 1]
    modes = jnp.concatenate([mixed[0] * scale, lifted_back[0], mixed[1] * scale, lifted_back[1]], axis=1)

    opened = jnp.concatenate([modes] * 8, axis=0).T
    parts = []
    for p in range(2):
        for f in range(2):
            total = None
            for h in range(2):
                cosine, sine = tw[h, 0], tw[h, 1]
                real = opened[f * 128 + h * 64 : f * 128 + h * 64 + 64]
                imag = opened[256 + f * 128 + h * 64 : 256 + f * 128 + h * 64 + 64]
                term = cosine * real - sine * imag if p == 0 else sine * real + cosine * imag
                total = term if total is None else total + term
            parts.append(total)
    s3[...] = mul3(pair(a2t), split(jnp.concatenate(parts, axis=0))).reshape(16, 2, 8, 128)
    across = start(5, "x", slab(s3), block(r3), s3.at[pl.ds(0, 15)])
    r3[lax.div(px, 8), :, lax.rem(px, 8)] = s3[px]

    for b in range(16):
        grad[b] = lifted[0] * back[0][b : b + 1] + lifted[1] * back[1][b : b + 1]
    grad_pair = split(grad[...].reshape(256, 128))
    tiles = []
    for k in range(2):
        kept = hot(iota((8, 128), 1) // 2 % 2 == k) * t3f
        for r in range(8):
            tiles.append(kept * t1[r : r + 1])
    s5[...] = mul3(grad_pair, split(jnp.concatenate(tiles, axis=0)), NT).reshape(16, 16, 128)
    shares = start(6, "y", slab(s5), slab(r8), r8.at[pl.ds(0, 15)])
    r8[py] = s5[py]

    pulled = mul3(split(core[...].reshape(256, 512).T), grad_pair)
    by_first = []
    by_second = [jnp.zeros((8, 128), F32) for s in range(8)]
    by_third = jnp.zeros((8, 128), F32)
    for r in range(8):
        total = jnp.zeros((8, 128), F32)
        for s in range(8):
            tile = pulled[(r * 8 + s) * 8 : (r * 8 + s) * 8 + 8]
            total = total + tile * t2f[s : s + 1]
            by_second[s] = by_second[s] + tile * t1[r : r + 1]
        by_first.append(total)
        by_third = by_third + total * t1[r : r + 1]
    fold = hot(iota((8, 64), 1) // 8 == iota((8, 64), 0))
    first_rows8 = exact(fold, jnp.concatenate([t * t3f for t in by_first], axis=0))
    second_rows8 = exact(fold, jnp.concatenate([t * t3f for t in by_second], axis=0))
    row = iota((128, 128), 0)
    col = iota((128, 128), 1)
    factor_grads = (
        exact(first_rows8, hot(row // 4 == col))
        + exact(second_rows8, hot(row // 2 % 2 + 2 * px + 32 == col))
        + exact(by_third, hot(row % 2 + 2 * py + 64 == col))
    )

    across.wait_recv()
    back_pair = split(r3[...].reshape(256, 128))
    a1t_pair = pair(a1t)
    inward = []
    for c in range(4):
        places = spread[:, c * 256 : (c + 1) * 256]
        opened = mul(back_pair[0], places) + mul(back_pair[1], places)
        turned = []
        for x in range(2):
            parts = []
            for p in range(2):
                total = None
                for h in range(2):
                    cosine, sine = tw[h, 0], tw[h, 1]
                    real = opened[h * 128 : h * 128 + 64, x * 128 : (x + 1) * 128]
                    imag = opened[h * 128 + 64 : h * 128 + 128, x * 128 : (x + 1) * 128]
                    term = cosine * real - sine * imag if p == 0 else sine * real + cosine * imag
                    total = term if total is None else total + term
                parts.append(total)
            turned.append(jnp.concatenate(parts, axis=0))
        s4[:, c * 256 : (c + 1) * 256] = mul3(a1t_pair, split(jnp.concatenate(turned, axis=1)))
        inward.append(
            start(7 + c, "y", rows8(s4, chunks[c]), rows8(r4, chunks[c]), r4.at[pl.ds(0, 120), chunks[c]])
        )
        r4[own, c * 256 : (c + 1) * 256] = s4[own, c * 256 : (c + 1) * 256]

    sums = [jnp.zeros((512, 128), F32) for f in range(2)]
    for c in range(4):
        inward[c].wait_recv()
        if c == 3:
            column = start(11, "x", whole(s6), slab(r9), r9.at[pl.ds(0, 15)])
            r9[px] = s6[...]
        values = [[], []]
        for x in range(2):
            rows = r4[:, (2 * c + x) * 128 : (2 * c + x + 1) * 128].T
            both = mul3(split(rows), tz_pair)
            for f in range(2):
                values[f].append(split(both[:, (1 - f) * 128 : (2 - f) * 128]))
            grids[2 * c + x, 0], grids[2 * c + x, 1] = values[1][x]
        for f in range(2):
            rows = given[f, :, c * 256 : (c + 1) * 256]
            for h in range(2):
                sums[f] = sums[f] + mul(rows, jnp.concatenate([v[h] for v in values[f]], axis=1), NT)
        if c == 1:
            shares.wait_recv()
            total = r8[0]
            for q in range(1, 16):
                total = total + r8[q]
            s6[...] = total
    kept = hot(iota((512, 128), 0) % 8 == iota((512, 128), 1) // 16)
    sums = [jnp.sum((v * kept).reshape(64, 8, 128), axis=1) for v in sums]
    high, low = split(jnp.concatenate(sums, axis=0))
    ts[0:16] = mul(ones, high, NT) + mul(ones, low, NT)
    ts[16:24] = factor_grads
    tail = start(14, "y", whole(ts), slab(r5), r5.at[pl.ds(0, 15)])
    r5[py] = ts[...]

    back_maps = pair(back_map)

    def emit(x, carry):
        output[:, pl.ds(x, 1)] = mul3(back_maps, (grids[x, 0], grids[x, 1])).reshape(64, 1, 8, 128).astype(BF16)
        return carry

    lax.fori_loop(0, 4, emit, 0)

    column.wait_recv()
    totals = [jnp.zeros((16, 128), F32) for s in range(8)]
    for q in range(16):
        received = r9[q]
        for s in range(8):
            totals[s] = totals[s] + received * spread_second[s : s + 1, q * 128 : (q + 1) * 128]
    totals = [t + pltpu.roll(t, 64, 1) for t in totals]
    left = iota((16, 128), 1) < 64
    for u in range(4):
        s7[:, u * 128 : (u + 1) * 128] = jnp.where(left, totals[2 * u], totals[2 * u + 1])

    mine, chip = lax.rem(py, 2), lax.div(py, 2)
    core_parts = start(
        12, "y", whole(s7), lambda i: cg.at[mine, chip], cg.at[0, pl.ds(0, 7)], [p for p, o in zip(peers_y, FAR_FIRST_Y) if o[2] == 0]
    )
    cg[mine, chip] = s7[...]

    tail.wait_recv()
    total = r5[0]
    for q in range(1, 16):
        total = total + r5[q]
    t2[...] = total
    tail = start(15, "x", whole(t2), slab(small_h), small_h.at[pl.ds(0, 15)])
    done = [pltpu.make_async_copy(t2, small_h.at[px], loads.at[2])]
    done[0].start()
    lax.fori_loop(4, 8, emit, 0)
    done.append(pltpu.make_async_copy(output, output_h, loads.at[0]))
    done[1].start()
    core_parts.wait_recv()
    mate = [p for p, o in zip(peers_y, FAR_FIRST_Y) if o == (0, 0, 1)]
    core_parts = start(13, "y", lambda i: cg.at[mine], lambda i: cg.at[mine], cg.at[0], mate)
    core_parts.wait_recv()
    for c in range(2):
        done.append(pltpu.make_async_copy(cg.at[c], packed_h.at[:, c], loads.at[3 + c]))
        done[-1].start()
    tail.wait_recv()
    for c in waits:
        c.wait_send()
    for c in done:
        c.wait()


def finish(
    output_i, packed_i, small_i,
    output_h, core_h, in_h, out_h, first_h, second_h, third_h,
    output, packed, parts, core, grad_in, grad_out, grad_first, grad_second, grad_third, done,
):
    loads = (
        pltpu.make_async_copy(packed_i, packed, done.at[22]),
        pltpu.make_async_copy(small_i, parts, done.at[23]),
        pltpu.make_async_copy(output_i, output, done.at[24]),
    )
    for c in loads:
        c.start()
    loads[0].wait()
    copies = []
    for a in range(16):
        rows = packed[:, :, a].reshape(16, 512).T.reshape(8, 8, 8, 16)
        for s in range(8):
            for r in range(8):
                core[a, (r * 8 + s) * 8 : (r * 8 + s) * 8 + 8] = rows[s, r]
        copies.append(pltpu.make_async_copy(core.at[a], core_h.at[a], done.at[1 + a]))
        copies[-1].start()
        if a == 8:
            loads[1].wait()
            loads[2].wait()
            copies.append(pltpu.make_async_copy(output, output_h, done.at[0]))
            copies[-1].start()
    small = parts[0]
    for q in range(1, 16):
        small = small + parts[q]
    grad_in[...] = small[0:16, 0:64]
    grad_out[...] = small[0:16, 64:128]
    grad_first[...] = small[16:24, 0:32]
    grad_second[...] = small[16:24, 32:64]
    grad_third[...] = small[16:24, 64:96]
    pairs = ((grad_in, in_h), (grad_out, out_h), (grad_first, first_h), (grad_second, second_h), (grad_third, third_h))
    for i, (near, far) in enumerate(pairs):
        copies.append(pltpu.make_async_copy(near, far, done.at[17 + i]))
        copies[-1].start()
    for c in copies:
        c.wait()


def shards(field, cot, core, in_factor, out_factor, first, second, third):
    constants = [
        jnp.asarray(c)
        for c in (
            halves(depth_rows()),
            halves(second_rows()),
            halves(second_rows().T),
            halves(first_rows()),
            halves(first_rows().T),
            twiddles(),
            np.ascontiguousarray(gather_lanes().T),
            gather_lanes(),
        )
    ]
    operands = (
        field,
        cot,
        core.transpose(0, 2, 3, 4, 1).reshape(16, 512, 16),
        in_factor.T,
        out_factor.T,
        first.T,
        second.T,
        third.T,
        *constants,
    )
    hbm = pl.BlockSpec(memory_space=pltpu.HBM)
    scratch = [pltpu.VMEM(v.shape, v.dtype) for v in operands] + [
        pltpu.VMEM((16, 16, 512), F32),
        pltpu.VMEM((2, 256, 512), BF16),
        pltpu.VMEM((2, 512, 128), BF16),
        pltpu.VMEM((2, 512, 1024), BF16),
        pltpu.VMEM((128, 1024), F32),
        pltpu.VMEM((128, 1024), F32),
        pltpu.VMEM((2, 2, 8, 8, 128), F32),
        pltpu.VMEM((16, 2, 8, 128), F32),
        pltpu.VMEM((16, 2, 8, 128), F32),
        pltpu.VMEM((2, 2, 8, 8, 128), F32),
        pltpu.VMEM((128, 1024), F32),
        pltpu.VMEM((128, 1024), F32),
        pltpu.VMEM((16, 16, 128), F32),
        pltpu.VMEM((16, 16, 128), F32),
        pltpu.VMEM((16, 16, 128), F32),
        pltpu.VMEM((16, 16, 128), F32),
        pltpu.VMEM((16, 128), F32),
        pltpu.VMEM((16, 16, 128), F32),
        pltpu.VMEM((16, 512), F32),
        pltpu.VMEM((2, 8, 16, 512), F32),
        pltpu.VMEM((8, 2048), F32),
        pltpu.VMEM((8, 2, 128, 128), BF16),
        pltpu.VMEM((64, 8, 8, 128), BF16),
        pltpu.VMEM((24, 128), F32),
        pltpu.VMEM((16, 24, 128), F32),
        pltpu.VMEM((24, 128), F32),
        pltpu.SemaphoreType.DMA((16,)),
        pltpu.SemaphoreType.DMA((16,)),
        pltpu.SemaphoreType.DMA((len(operands),)),
    ]
    stages = (
        jax.ShapeDtypeStruct((64, 8, 8, 128), BF16),
        jax.ShapeDtypeStruct((8, 2, 16, 512), F32),
        jax.ShapeDtypeStruct((16, 24, 128), F32),
    )
    step = pl.pallas_call(
        kernel,
        out_shape=stages,
        in_specs=[hbm] * len(operands),
        out_specs=[hbm] * 3,
        scratch_shapes=scratch,
        compiler_params=pltpu.CompilerParams(
            collective_id=0, has_side_effects=True, vmem_limit_bytes=67043328
        ),
        name="tucker_step",
    )(*operands)
    shapes = ((64, 8, 8, 128), (16, 512, 16), (16, 64), (16, 64), (8, 32), (8, 32), (8, 32))
    output, grad_core, *grads = pl.pallas_call(
        finish,
        out_shape=tuple(jax.ShapeDtypeStruct(v, BF16 if i == 0 else F32) for i, v in enumerate(shapes)),
        in_specs=[hbm] * 3,
        out_specs=[hbm] * 7,
        scratch_shapes=[pltpu.VMEM(v.shape, v.dtype) for v in stages]
        + [pltpu.VMEM(v, F32) for v in shapes[1:]]
        + [pltpu.SemaphoreType.DMA((25,))],
        compiler_params=pltpu.CompilerParams(vmem_limit_bytes=67043328),
        name="finish",
    )(*step)
    grad_core = grad_core.reshape(16, 8, 8, 8, 16).transpose(0, 4, 1, 2, 3)
    return (output, grad_core, *[g.T for g in grads])


def solution(mesh):
    grid = P(None, "px", "py", None)
    return jax.shard_map(
        shards,
        mesh=mesh,
        in_specs=(grid, grid) + (P(),) * 6,
        out_specs=(grid,) + (P(),) * 6,
        check_vma=False,
    )
```

```python
import functools
import math

import jax
import jax.numpy as jnp
import numpy as np
from jax import lax
from jax.experimental import pallas as pl
from jax.experimental.pallas import tpu as pltpu
from jax.sharding import PartitionSpec as P

F32 = jnp.float32
BF16 = jnp.bfloat16
HIGHEST = lax.Precision.HIGHEST
MESH = pl.DeviceIdType.MESH
COUNT = 16
CELLS = 128
SCALE = 1.0 / (CELLS * CELLS * CELLS)
NN = ((1,), (0,))
FAR_FIRST_Y = sorted(
    ((x, y, c) for x in range(4) for y in range(2) for c in range(2) if x or y or c),
    key=lambda o: -(min(o[0], 4 - o[0]) + o[1]),
)
FAR_FIRST_X = sorted(
    ((z, y) for z in range(8) for y in range(2) if z or y),
    key=lambda o: -(min(o[0], 8 - o[0]) + 2 * o[1]),
)
NT = ((1,), (1,))


def halves(table):
    high = table.astype(np.float32).astype(jnp.bfloat16)
    low = (table - high.astype(np.float64)).astype(np.float32).astype(jnp.bfloat16)
    return np.stack([high, low])


def depth_rows():
    row = np.arange(128)[:, None]
    lane = np.arange(256)[None, :]
    mode = row // 8 * 2 + row % 2
    angle = 2.0 * math.pi / CELLS * (mode * (lane % 128) % CELLS)
    value = np.where(row // 2 % 2 == 0, np.cos(angle), -np.sin(angle))
    return np.where(row // 4 % 2 == lane // 128, value, 0.0)


def short_transform(rows, row_of, col_of):
    row = np.arange(rows)[:, None]
    col = np.arange(rows)[None, :]
    part_out, freq, rest_out = row_of(row)
    part_in, block, rest_in = col_of(col)
    angle = 2.0 * math.pi / 16 * (freq * block % 16)
    sine = np.where(part_out == 0, 1.0, -1.0) * np.sin(angle)
    value = np.where(part_out == part_in, np.cos(angle), sine)
    return np.where(rest_out == rest_in, value, 0.0)


def second_rows():
    return short_transform(
        128,
        lambda r: (r // 64, r // 4 % 16, r % 4),
        lambda c: (c // 2 % 2, c // 8, c // 4 % 2 * 2 + c % 2),
    )


def first_rows():
    return short_transform(
        256,
        lambda r: (r // 128, r // 4 % 16, r // 64 % 2 * 4 + r % 4),
        lambda c: (c // 8 % 2, c // 16, c // 2 % 2 * 4 + c // 4 % 2 * 2 + c % 2),
    )


def twiddles():
    row = np.arange(64)[:, None]
    lane = np.arange(128)[None, :]
    tables = []
    for high in range(2):
        angle = 2.0 * math.pi / CELLS * ((row // 4 - 16 * high) * (lane // 16))
        tables.append(np.stack([np.cos(angle), np.sin(angle)]))
    return np.stack(tables).astype(np.float32)


def gather_lanes():
    row = np.arange(1024)[:, None]
    lane = np.arange(128)[None, :]
    return ((row // 128 == lane // 16) & (row % 16 == lane % 16)).astype(np.float32).astype(jnp.bfloat16)


def split(value):
    high = value.astype(BF16)
    return high, (value - high.astype(F32)).astype(BF16)


def mul(a, b, dims=NN):
    return lax.dot_general(a, b, (dims, ((), ())), preferred_element_type=F32)


def exact(a, b, dims=NN):
    return lax.dot_general(a, b, (dims, ((), ())), precision=HIGHEST, preferred_element_type=F32)


def mul3(a, b, dims=NN):
    return mul(a[0], b[0], dims) + mul(a[0], b[1], dims) + mul(a[1], b[0], dims)


def pair(ref):
    return ref[0], ref[1]


def iota(shape, axis):
    return lax.broadcasted_iota(jnp.int32, shape, axis)


def hot(test):
    return jnp.where(test, 1.0, 0.0).astype(F32)


def kernel(
    field_h, cot_h, core_h, in_h, out_h, first_h, second_h, third_h,
    tz_h, a1_h, a1t_h, a2_h, a2t_h, tw_h, spread_h, collect_h,
    output_h, packed_h, small_h,
    field, cot, core_n, in_t, out_t, first_t, second_t, third_t,
    tz, a1, a1t, a2, a2t, tw, spread, collect, core,
    m_in, back_map, given, s1, r1, s2, r2, s3, r3, s4, r4,
    kern, grad, s5, r8, s6, r9, s7, cg, spread_second, grids, output, ts, r5, t2,
    send, recv, loads,
):
    px = lax.axis_index("px")
    py = lax.axis_index("py")
    barrier = pltpu.get_barrier_semaphore()

    def along_y(peer):
        return (px, peer)

    def along_x(peer):
        return (peer, py)

    staged = (
        (in_h, in_t), (out_h, out_t), (field_h, field), (cot_h, cot), (tz_h, tz),
        (first_h, first_t), (second_h, second_t), (third_h, third_t), (a1_h, a1), (tw_h, tw), (collect_h, collect),
        (core_h, core_n), (a2_h, a2), (a2t_h, a2t), (spread_h, spread), (a1t_h, a1t),
    )
    copies = [pltpu.make_async_copy(far, near, loads.at[i]) for i, (far, near) in enumerate(staged)]
    for c in copies:
        c.start()

    x_at = [lax.rem(lax.div(py, 4) + d, 4) * 4 for d in range(4)]
    y_at = [lax.rem(lax.rem(lax.div(py, 2), 2) + d, 2) * 2 for d in range(2)]
    core_at = [lax.rem(lax.rem(py, 2) + d, 2) for d in range(2)]
    z_at = [lax.rem(lax.div(px, 2) + d, 8) * 2 for d in range(8)]
    far_at = [lax.rem(lax.rem(px, 2) + d, 2) for d in range(2)]
    peers_y = [x_at[x] + y_at[y] + core_at[c] for x, y, c in FAR_FIRST_Y]
    peers_x = [z_at[z] + far_at[y] for z, y in FAR_FIRST_X]
    for peer in peers_x:
        pl.semaphore_signal(barrier, inc=1, device_id=along_x(peer), device_id_type=MESH)
    for peer in peers_y:
        pl.semaphore_signal(barrier, inc=1, device_id=along_y(peer), device_id_type=MESH)
    waits = []

    def start(phase, axis, source, target, every, some=None):
        me, device, peers = (py, along_y, some or peers_y) if axis == "y" else (px, along_x, peers_x)
        for peer in peers:
            pltpu.make_async_remote_copy(
                src_ref=source(peer),
                dst_ref=target(me),
                send_sem=send.at[phase],
                recv_sem=recv.at[phase],
                device_id=device(peer),
                device_id_type=MESH,
            ).start()
        total = pltpu.make_async_remote_copy(
            src_ref=every,
            dst_ref=every,
            send_sem=send.at[phase],
            recv_sem=recv.at[phase],
            device_id=device(peers[0]),
            device_id_type=MESH,
        )
        waits.append(total)
        return total

    def rows8(ref, lanes):
        return lambda i: ref.at[pl.ds(pl.multiple_of(i * 8, 8), 8), lanes]

    def slab(ref, *rest):
        return lambda i: ref.at[(i, *rest)] if rest else ref.at[i]

    def block(ref):
        return lambda i: ref.at[lax.div(i, 8), :, lax.rem(i, 8)]

    def whole(ref):
        return lambda i: ref

    chunks = [pl.ds(c * 256, 256) for c in range(4)]
    own = pl.ds(pl.multiple_of(py * 8, 8), 8)

    copies[0].wait()
    copies[1].wait()
    lane = iota((16, 512), 1)
    repeat = hot(iota((64, 512), 1) // 8 == iota((64, 512), 0))
    maps = []
    for f, factor in enumerate((in_t, out_t)):
        wide_factor = exact(factor[...], repeat)
        maps.append(jnp.concatenate([jnp.where(lane % 8 == y, wide_factor, 0.0) for y in range(8)], axis=0))
        high, low = split(maps[f])
        m_in[f, 0:128] = high
        m_in[f, 128:256] = low

    for c in copies[2:5]:
        c.wait()
    tz_pair = pair(tz)
    outward = []
    for c in range(4):
        lifted = []
        for f, source in enumerate((field, cot)):
            for x in range(2):
                rows = source[:, 2 * c + x].astype(F32).reshape(512, 128).astype(BF16)
                given[f, :, (2 * c + x) * 128 : (2 * c + x + 1) * 128] = rows
            both = mul(m_in[f], given[f, :, c * 256 : (c + 1) * 256])
            lifted.append(both[0:128] + both[128:256])
        for x in range(2):
            both = jnp.concatenate([v[:, x * 128 : (x + 1) * 128] for v in lifted], axis=1)
            s1[:, (2 * c + x) * 128 : (2 * c + x + 1) * 128] = mul3(tz_pair, split(both), NT)
        if c == 0:
            pl.semaphore_wait(barrier, 2 * (COUNT - 1))
        outward.append(
            start(c, "y", rows8(s1, chunks[c]), rows8(r1, chunks[c]), r1.at[pl.ds(0, 120), chunks[c]])
        )
        r1[own, c * 256 : (c + 1) * 256] = s1[own, c * 256 : (c + 1) * 256]
    for c in copies[5:]:
        c.wait()

    mode = iota((32, 128), 1)
    row32 = iota((32, 128), 0)
    t1 = exact(first_t[...], hot(mode // 4 == row32))
    t2f = exact(second_t[...], hot(mode // 2 % 2 + 2 * px == row32))
    t3f = exact(third_t[...], hot(mode % 2 + 2 * py == row32))
    tiles = []
    for r in range(8):
        for s in range(8):
            tiles.append(t3f * (t1[r : r + 1] * t2f[s : s + 1]))
    phi_pair = split(jnp.concatenate(tiles, axis=0))
    for a in range(16):
        core[:, a] = core_n[a].T
    kern[...] = mul3(split(core[...].reshape(256, 512)), phi_pair).reshape(16, 16, 128)
    spread_second[...] = exact(second_t[...], hot(iota((32, 2048), 1) // 64 == iota((32, 2048), 0)))
    high, low = split(maps[1].T)
    back_map[0] = high
    back_map[1] = low

    a1_pair = pair(a1)
    gathered = jnp.zeros((256, 128), F32)
    for c in range(4):
        outward[c].wait_recv()
        middle = mul3(a1_pair, split(r1[:, c * 256 : (c + 1) * 256]))
        turned = []
        for x in range(2):
            real = middle[0:64, x * 128 : (x + 1) * 128]
            imag = middle[64:128, x * 128 : (x + 1) * 128]
            parts = []
            for h in range(2):
                cosine, sine = tw[h, 0], tw[h, 1]
                parts += [cosine * real + sine * imag, cosine * imag - sine * real]
            turned.append(jnp.concatenate(parts, axis=0))
        high, low = split(jnp.concatenate(turned, axis=1))
        places = collect[c * 256 : (c + 1) * 256]
        gathered = gathered + (mul(high, places) + mul(low, places))
    s2[...] = gathered.reshape(2, 2, 8, 8, 128)
    across = start(4, "x", block(s2), slab(r2), r2.at[pl.ds(0, 15)])
    r2[px] = s2[lax.div(px, 8), :, lax.rem(px, 8)]

    across.wait_recv()
    middle = mul3(pair(a2), split(r2[...].reshape(256, 128)))
    parts = []
    for p in range(2):
        for f in range(2):
            real = middle[f * 64 : f * 64 + 64]
            imag = middle[128 + f * 64 : 128 + f * 64 + 64]
            for h in range(2):
                cosine, sine = tw[h, 0], tw[h, 1]
                parts.append(cosine * real + sine * imag if p == 0 else cosine * imag - sine * real)
    high, low = split(jnp.concatenate(parts, axis=0))
    ones = hot(iota((16, 128), 1) % 16 == iota((16, 128), 0)).astype(BF16)
    modes = mul(ones, high, NT) + mul(ones, low, NT)

    depth_mode = iota((1, 128), 1) % 2 + 2 * py
    scale = jnp.where(depth_mode == 0, 1.0, 2.0).astype(F32) * SCALE
    lifted = [modes[:, p * 256 : p * 256 + 128] for p in range(2)]
    back = [modes[:, p * 256 + 128 : p * 256 + 256] * scale for p in range(2)]
    mixed = [jnp.zeros((16, 128), F32) for p in range(2)]
    lifted_back = [jnp.zeros((16, 128), F32) for p in range(2)]
    for i in range(16):
        over_a = kern[:, i]
        over_b = kern[i]
        for p in range(2):
            mixed[p] = mixed[p] + over_a * lifted[p][i : i + 1]
            lifted_back[p] = lifted_back[p] + over_b * back[p][i : i + 1]
    modes = jnp.concatenate([mixed[0] * scale, lifted_back[0], mixed[1] * scale, lifted_back[1]], axis=1)

    opened = jnp.concatenate([modes] * 8, axis=0).T
    parts = []
    for p in range(2):
        for f in range(2):
            total = None
            for h in range(2):
                cosine, sine = tw[h, 0], tw[h, 1]
                real = opened[f * 128 + h * 64 : f * 128 + h * 64 + 64]
                imag = opened[256 + f * 128 + h * 64 : 256 + f * 128 + h * 64 + 64]
                term = cosine * real - sine * imag if p == 0 else sine * real + cosine * imag
                total = term if total is None else total + term
            parts.append(total)
    s3[...] = mul3(pair(a2t), split(jnp.concatenate(parts, axis=0))).reshape(16, 2, 8, 128)
    across = start(5, "x", slab(s3), block(r3), s3.at[pl.ds(0, 15)])
    r3[lax.div(px, 8), :, lax.rem(px, 8)] = s3[px]

    for b in range(16):
        grad[b] = lifted[0] * back[0][b : b + 1] + lifted[1] * back[1][b : b + 1]
    grad_pair = split(grad[...].reshape(256, 128))
    tiles = []
    for k in range(2):
        kept = hot(iota((8, 128), 1) // 2 % 2 == k) * t3f
        for r in range(8):
            tiles.append(kept * t1[r : r + 1])
    s5[...] = mul3(grad_pair, split(jnp.concatenate(tiles, axis=0)), NT).reshape(16, 16, 128)
    shares = start(6, "y", slab(s5), slab(r8), r8.at[pl.ds(0, 15)])
    r8[py] = s5[py]

    pulled = mul3(split(core[...].reshape(256, 512).T), grad_pair)
    by_first = []
    by_second = [jnp.zeros((8, 128), F32) for s in range(8)]
    by_third = jnp.zeros((8, 128), F32)
    for r in range(8):
        total = jnp.zeros((8, 128), F32)
        for s in range(8):
            tile = pulled[(r * 8 + s) * 8 : (r * 8 + s) * 8 + 8]
            total = total + tile * t2f[s : s + 1]
            by_second[s] = by_second[s] + tile * t1[r : r + 1]
        by_first.append(total)
        by_third = by_third + total * t1[r : r + 1]
    fold = hot(iota((8, 64), 1) // 8 == iota((8, 64), 0))
    first_rows8 = exact(fold, jnp.concatenate([t * t3f for t in by_first], axis=0))
    second_rows8 = exact(fold, jnp.concatenate([t * t3f for t in by_second], axis=0))
    row = iota((128, 128), 0)
    col = iota((128, 128), 1)
    factor_grads = (
        exact(first_rows8, hot(row // 4 == col))
        + exact(second_rows8, hot(row // 2 % 2 + 2 * px + 32 == col))
        + exact(by_third, hot(row % 2 + 2 * py + 64 == col))
    )

    across.wait_recv()
    back_pair = split(r3[...].reshape(256, 128))
    a1t_pair = pair(a1t)
    inward = []
    for c in range(4):
        places = spread[:, c * 256 : (c + 1) * 256]
        opened = mul(back_pair[0], places) + mul(back_pair[1], places)
        turned = []
        for x in range(2):
            parts = []
            for p in range(2):
                total = None
                for h in range(2):
                    cosine, sine = tw[h, 0], tw[h, 1]
                    real = opened[h * 128 : h * 128 + 64, x * 128 : (x + 1) * 128]
                    imag = opened[h * 128 + 64 : h * 128 + 128, x * 128 : (x + 1) * 128]
                    term = cosine * real - sine * imag if p == 0 else sine * real + cosine * imag
                    total = term if total is None else total + term
                parts.append(total)
            turned.append(jnp.concatenate(parts, axis=0))
        s4[:, c * 256 : (c + 1) * 256] = mul3(a1t_pair, split(jnp.concatenate(turned, axis=1)))
        inward.append(
            start(7 + c, "y", rows8(s4, chunks[c]), rows8(r4, chunks[c]), r4.at[pl.ds(0, 120), chunks[c]])
        )
        r4[own, c * 256 : (c + 1) * 256] = s4[own, c * 256 : (c + 1) * 256]

    sums = [jnp.zeros((512, 128), F32) for f in range(2)]
    for c in range(4):
        inward[c].wait_recv()
        if c == 2:
            column = start(11, "x", whole(s6), slab(r9), r9.at[pl.ds(0, 15)])
            r9[px] = s6[...]
        values = [[], []]
        for x in range(2):
            rows = r4[:, (2 * c + x) * 128 : (2 * c + x + 1) * 128].T
            both = mul3(split(rows), tz_pair)
            for f in range(2):
                values[f].append(split(both[:, (1 - f) * 128 : (2 - f) * 128]))
            grids[2 * c + x, 0], grids[2 * c + x, 1] = values[1][x]
        for f in range(2):
            rows = given[f, :, c * 256 : (c + 1) * 256]
            for h in range(2):
                sums[f] = sums[f] + mul(rows, jnp.concatenate([v[h] for v in values[f]], axis=1), NT)
        if c == 1:
            shares.wait_recv()
            total = r8[0]
            for q in range(1, 16):
                total = total + r8[q]
            s6[...] = total
    kept = hot(iota((512, 128), 0) % 8 == iota((512, 128), 1) // 16)
    sums = [jnp.sum((v * kept).reshape(64, 8, 128), axis=1) for v in sums]
    high, low = split(jnp.concatenate(sums, axis=0))
    ts[0:16] = mul(ones, high, NT) + mul(ones, low, NT)
    ts[16:24] = factor_grads
    tail = start(14, "y", whole(ts), slab(r5), r5.at[pl.ds(0, 15)])
    r5[py] = ts[...]

    back_maps = pair(back_map)

    def emit(x, carry):
        output[:, pl.ds(x, 1)] = mul3(back_maps, (grids[x, 0], grids[x, 1])).reshape(64, 1, 8, 128).astype(BF16)
        return carry

    lax.fori_loop(0, 4, emit, 0)

    column.wait_recv()
    totals = [jnp.zeros((16, 128), F32) for s in range(8)]
    for q in range(16):
        received = r9[q]
        for s in range(8):
            totals[s] = totals[s] + received * spread_second[s : s + 1, q * 128 : (q + 1) * 128]
    totals = [t + pltpu.roll(t, 64, 1) for t in totals]
    left = iota((16, 128), 1) < 64
    for u in range(4):
        s7[:, u * 128 : (u + 1) * 128] = jnp.where(left, totals[2 * u], totals[2 * u + 1])

    mine, chip = lax.rem(py, 2), lax.div(py, 2)
    core_parts = start(
        12, "y", whole(s7), lambda i: cg.at[mine, chip], cg.at[0, pl.ds(0, 7)], [p for p, o in zip(peers_y, FAR_FIRST_Y) if o[2] == 0]
    )
    cg[mine, chip] = s7[...]

    tail.wait_recv()
    total = r5[0]
    for q in range(1, 16):
        total = total + r5[q]
    t2[...] = total
    tail = start(15, "x", whole(t2), slab(small_h), small_h.at[pl.ds(0, 15)])
    done = [pltpu.make_async_copy(t2, small_h.at[px], loads.at[2])]
    done[0].start()
    lax.fori_loop(4, 8, emit, 0)
    done.append(pltpu.make_async_copy(output, output_h, loads.at[0]))
    done[1].start()
    core_parts.wait_recv()
    mate = [p for p, o in zip(peers_y, FAR_FIRST_Y) if o == (0, 0, 1)]
    core_parts = start(13, "y", lambda i: cg.at[mine], lambda i: packed_h.at[:, mine], cg.at[0], mate)
    done.append(pltpu.make_async_copy(cg.at[mine], packed_h.at[:, mine], loads.at[3]))
    done[-1].start()
    core_parts.wait_recv()
    tail.wait_recv()
    for c in waits:
        c.wait_send()
    for c in done:
        c.wait()


def finish(
    output_i, packed_i, small_i,
    output_h, core_h, in_h, out_h, first_h, second_h, third_h,
    output, packed, parts, core, grad_in, grad_out, grad_first, grad_second, grad_third, done,
):
    loads = (
        pltpu.make_async_copy(packed_i, packed, done.at[22]),
        pltpu.make_async_copy(small_i, parts, done.at[23]),
        pltpu.make_async_copy(output_i, output, done.at[24]),
    )
    for c in loads:
        c.start()
    loads[0].wait()
    copies = []
    for a in range(16):
        rows = packed[:, :, a].reshape(16, 512).T.reshape(8, 8, 8, 16)
        for s in range(8):
            for r in range(8):
                core[a, (r * 8 + s) * 8 : (r * 8 + s) * 8 + 8] = rows[s, r]
        copies.append(pltpu.make_async_copy(core.at[a], core_h.at[a], done.at[1 + a]))
        copies[-1].start()
        if a == 8:
            loads[1].wait()
            loads[2].wait()
            copies.append(pltpu.make_async_copy(output, output_h, done.at[0]))
            copies[-1].start()
    small = parts[0]
    for q in range(1, 16):
        small = small + parts[q]
    grad_in[...] = small[0:16, 0:64]
    grad_out[...] = small[0:16, 64:128]
    grad_first[...] = small[16:24, 0:32]
    grad_second[...] = small[16:24, 32:64]
    grad_third[...] = small[16:24, 64:96]
    pairs = ((grad_in, in_h), (grad_out, out_h), (grad_first, first_h), (grad_second, second_h), (grad_third, third_h))
    for i, (near, far) in enumerate(pairs):
        copies.append(pltpu.make_async_copy(near, far, done.at[17 + i]))
        copies[-1].start()
    for c in copies:
        c.wait()


def shards(field, cot, core, in_factor, out_factor, first, second, third):
    constants = [
        jnp.asarray(c)
        for c in (
            halves(depth_rows()),
            halves(second_rows()),
            halves(second_rows().T),
            halves(first_rows()),
            halves(first_rows().T),
            twiddles(),
            np.ascontiguousarray(gather_lanes().T),
            gather_lanes(),
        )
    ]
    operands = (
        field,
        cot,
        core.transpose(0, 2, 3, 4, 1).reshape(16, 512, 16),
        in_factor.T,
        out_factor.T,
        first.T,
        second.T,
        third.T,
        *constants,
    )
    hbm = pl.BlockSpec(memory_space=pltpu.HBM)
    scratch = [pltpu.VMEM(v.shape, v.dtype) for v in operands] + [
        pltpu.VMEM((16, 16, 512), F32),
        pltpu.VMEM((2, 256, 512), BF16),
        pltpu.VMEM((2, 512, 128), BF16),
        pltpu.VMEM((2, 512, 1024), BF16),
        pltpu.VMEM((128, 1024), F32),
        pltpu.VMEM((128, 1024), F32),
        pltpu.VMEM((2, 2, 8, 8, 128), F32),
        pltpu.VMEM((16, 2, 8, 128), F32),
        pltpu.VMEM((16, 2, 8, 128), F32),
        pltpu.VMEM((2, 2, 8, 8, 128), F32),
        pltpu.VMEM((128, 1024), F32),
        pltpu.VMEM((128, 1024), F32),
        pltpu.VMEM((16, 16, 128), F32),
        pltpu.VMEM((16, 16, 128), F32),
        pltpu.VMEM((16, 16, 128), F32),
        pltpu.VMEM((16, 16, 128), F32),
        pltpu.VMEM((16, 128), F32),
        pltpu.VMEM((16, 16, 128), F32),
        pltpu.VMEM((16, 512), F32),
        pltpu.VMEM((2, 8, 16, 512), F32),
        pltpu.VMEM((8, 2048), F32),
        pltpu.VMEM((8, 2, 128, 128), BF16),
        pltpu.VMEM((64, 8, 8, 128), BF16),
        pltpu.VMEM((24, 128), F32),
        pltpu.VMEM((16, 24, 128), F32),
        pltpu.VMEM((24, 128), F32),
        pltpu.SemaphoreType.DMA((16,)),
        pltpu.SemaphoreType.DMA((16,)),
        pltpu.SemaphoreType.DMA((len(operands),)),
    ]
    stages = (
        jax.ShapeDtypeStruct((64, 8, 8, 128), BF16),
        jax.ShapeDtypeStruct((8, 2, 16, 512), F32),
        jax.ShapeDtypeStruct((16, 24, 128), F32),
    )
    step = pl.pallas_call(
        kernel,
        out_shape=stages,
        in_specs=[hbm] * len(operands),
        out_specs=[hbm] * 3,
        scratch_shapes=scratch,
        compiler_params=pltpu.CompilerParams(
            collective_id=0, has_side_effects=True, vmem_limit_bytes=67043328
        ),
        name="tucker_step",
    )(*operands)
    shapes = ((64, 8, 8, 128), (16, 512, 16), (16, 64), (16, 64), (8, 32), (8, 32), (8, 32))
    output, grad_core, *grads = pl.pallas_call(
        finish,
        out_shape=tuple(jax.ShapeDtypeStruct(v, BF16 if i == 0 else F32) for i, v in enumerate(shapes)),
        in_specs=[hbm] * 3,
        out_specs=[hbm] * 7,
        scratch_shapes=[pltpu.VMEM(v.shape, v.dtype) for v in stages]
        + [pltpu.VMEM(v, F32) for v in shapes[1:]]
        + [pltpu.SemaphoreType.DMA((25,))],
        compiler_params=pltpu.CompilerParams(vmem_limit_bytes=67043328),
        name="finish",
    )(*step)
    grad_core = grad_core.reshape(16, 8, 8, 8, 16).transpose(0, 4, 1, 2, 3)
    return (output, grad_core, *[g.T for g in grads])


def solution(mesh):
    grid = P(None, "px", "py", None)
    return jax.shard_map(
        shards,
        mesh=mesh,
        in_specs=(grid, grid) + (P(),) * 6,
        out_specs=(grid,) + (P(),) * 6,
        check_vma=False,
    )
```

```python
import functools
import math

import jax
import jax.numpy as jnp
import numpy as np
from jax import lax
from jax.experimental import pallas as pl
from jax.experimental.pallas import tpu as pltpu
from jax.sharding import PartitionSpec as P

F32 = jnp.float32
BF16 = jnp.bfloat16
HIGHEST = lax.Precision.HIGHEST
MESH = pl.DeviceIdType.MESH
COUNT = 16
CELLS = 128
SCALE = 1.0 / (CELLS * CELLS * CELLS)
NN = ((1,), (0,))
FAR_FIRST_Y = sorted(
    ((x, y, c) for x in range(4) for y in range(2) for c in range(2) if x or y or c),
    key=lambda o: -(min(o[0], 4 - o[0]) + o[1]),
)
FAR_FIRST_X = sorted(
    ((z, y) for z in range(8) for y in range(2) if z or y),
    key=lambda o: -(min(o[0], 8 - o[0]) + 2 * o[1]),
)
NT = ((1,), (1,))


def halves(table):
    high = table.astype(np.float32).astype(jnp.bfloat16)
    low = (table - high.astype(np.float64)).astype(np.float32).astype(jnp.bfloat16)
    return np.stack([high, low])


def depth_rows():
    row = np.arange(128)[:, None]
    lane = np.arange(256)[None, :]
    mode = row // 8 * 2 + row % 2
    angle = 2.0 * math.pi / CELLS * (mode * (lane % 128) % CELLS)
    value = np.where(row // 2 % 2 == 0, np.cos(angle), -np.sin(angle))
    return np.where(row // 4 % 2 == lane // 128, value, 0.0)


def short_transform(rows, row_of, col_of):
    row = np.arange(rows)[:, None]
    col = np.arange(rows)[None, :]
    part_out, freq, rest_out = row_of(row)
    part_in, block, rest_in = col_of(col)
    angle = 2.0 * math.pi / 16 * (freq * block % 16)
    sine = np.where(part_out == 0, 1.0, -1.0) * np.sin(angle)
    value = np.where(part_out == part_in, np.cos(angle), sine)
    return np.where(rest_out == rest_in, value, 0.0)


def second_rows():
    return short_transform(
        128,
        lambda r: (r // 64, r // 4 % 16, r % 4),
        lambda c: (c // 2 % 2, c // 8, c // 4 % 2 * 2 + c % 2),
    )


def first_rows():
    return short_transform(
        256,
        lambda r: (r // 128, r // 4 % 16, r // 64 % 2 * 4 + r % 4),
        lambda c: (c // 8 % 2, c // 16, c // 2 % 2 * 4 + c // 4 % 2 * 2 + c % 2),
    )


def twiddles():
    row = np.arange(64)[:, None]
    lane = np.arange(128)[None, :]
    tables = []
    for high in range(2):
        angle = 2.0 * math.pi / CELLS * ((row // 4 - 16 * high) * (lane // 16))
        tables.append(np.stack([np.cos(angle), np.sin(angle)]))
    return np.stack(tables).astype(np.float32)


def gather_lanes():
    row = np.arange(1024)[:, None]
    lane = np.arange(128)[None, :]
    return ((row // 128 == lane // 16) & (row % 16 == lane % 16)).astype(np.float32).astype(jnp.bfloat16)


def split(value):
    high = value.astype(BF16)
    return high, (value - high.astype(F32)).astype(BF16)


def mul(a, b, dims=NN):
    return lax.dot_general(a, b, (dims, ((), ())), preferred_element_type=F32)


def exact(a, b, dims=NN):
    return lax.dot_general(a, b, (dims, ((), ())), precision=HIGHEST, preferred_element_type=F32)


def mul3(a, b, dims=NN):
    return mul(a[0], b[0], dims) + mul(a[0], b[1], dims) + mul(a[1], b[0], dims)


def pair(ref):
    return ref[0], ref[1]


def iota(shape, axis):
    return lax.broadcasted_iota(jnp.int32, shape, axis)


def hot(test):
    return jnp.where(test, 1.0, 0.0).astype(F32)


def kernel(
    field_h, cot_h, core_h, in_h, out_h, first_h, second_h, third_h,
    tz_h, a1_h, a1t_h, a2_h, a2t_h, tw_h, spread_h, collect_h,
    output_h, packed_h, small_h,
    field, cot, core_n, in_t, out_t, first_t, second_t, third_t,
    tz, a1, a1t, a2, a2t, tw, spread, collect, core,
    m_in, back_map, given, s1, r1, s2, r2, s3, r3, s4, r4,
    kern, grad, s5, r8, s6, r9, s7, cg, spread_second, grids, output, ts, r5, t2,
    send, recv, loads,
):
    px = lax.axis_index("px")
    py = lax.axis_index("py")
    barrier = pltpu.get_barrier_semaphore()

    def along_y(peer):
        return (px, peer)

    def along_x(peer):
        return (peer, py)

    staged = (
        (in_h, in_t), (out_h, out_t), (field_h, field), (cot_h, cot), (tz_h, tz),
        (first_h, first_t), (second_h, second_t), (third_h, third_t), (a1_h, a1), (tw_h, tw), (collect_h, collect),
        (core_h, core_n), (a2_h, a2), (a2t_h, a2t), (spread_h, spread), (a1t_h, a1t),
    )
    copies = [pltpu.make_async_copy(far, near, loads.at[i]) for i, (far, near) in enumerate(staged)]
    for c in copies:
        c.start()

    x_at = [lax.rem(lax.div(py, 4) + d, 4) * 4 for d in range(4)]
    y_at = [lax.rem(lax.rem(lax.div(py, 2), 2) + d, 2) * 2 for d in range(2)]
    core_at = [lax.rem(lax.rem(py, 2) + d, 2) for d in range(2)]
    z_at = [lax.rem(lax.div(px, 2) + d, 8) * 2 for d in range(8)]
    far_at = [lax.rem(lax.rem(px, 2) + d, 2) for d in range(2)]
    peers_y = [x_at[x] + y_at[y] + core_at[c] for x, y, c in FAR_FIRST_Y]
    peers_x = [z_at[z] + far_at[y] for z, y in FAR_FIRST_X]
    for peer in peers_x:
        pl.semaphore_signal(barrier, inc=1, device_id=along_x(peer), device_id_type=MESH)
    for peer in peers_y:
        pl.semaphore_signal(barrier, inc=1, device_id=along_y(peer), device_id_type=MESH)
    waits = []

    def start(phase, axis, source, target, every, some=None):
        me, device, peers = (py, along_y, some or peers_y) if axis == "y" else (px, along_x, peers_x)
        for peer in peers:
            pltpu.make_async_remote_copy(
                src_ref=source(peer),
                dst_ref=target(me),
                send_sem=send.at[phase],
                recv_sem=recv.at[phase],
                device_id=device(peer),
                device_id_type=MESH,
            ).start()
        total = pltpu.make_async_remote_copy(
            src_ref=every,
            dst_ref=every,
            send_sem=send.at[phase],
            recv_sem=recv.at[phase],
            device_id=device(peers[0]),
            device_id_type=MESH,
        )
        waits.append(total)
        return total

    def rows8(ref, lanes):
        return lambda i: ref.at[pl.ds(pl.multiple_of(i * 8, 8), 8), lanes]

    def slab(ref, *rest):
        return lambda i: ref.at[(i, *rest)] if rest else ref.at[i]

    def block(ref):
        return lambda i: ref.at[lax.div(i, 8), :, lax.rem(i, 8)]

    def whole(ref):
        return lambda i: ref

    chunks = [pl.ds(c * 256, 256) for c in range(4)]
    own = pl.ds(pl.multiple_of(py * 8, 8), 8)

    copies[0].wait()
    copies[1].wait()
    lane = iota((16, 512), 1)
    repeat = hot(iota((64, 512), 1) // 8 == iota((64, 512), 0))
    maps = []
    for f, factor in enumerate((in_t, out_t)):
        wide_factor = exact(factor[...], repeat)
        maps.append(jnp.concatenate([jnp.where(lane % 8 == y, wide_factor, 0.0) for y in range(8)], axis=0))
        high, low = split(maps[f])
        m_in[f, 0:128] = high
        m_in[f, 128:256] = low

    for c in copies[2:5]:
        c.wait()
    tz_pair = pair(tz)
    outward = []
    for c in range(4):
        lifted = []
        for f, source in enumerate((field, cot)):
            for x in range(2):
                rows = source[:, 2 * c + x].astype(F32).reshape(512, 128).astype(BF16)
                given[f, :, (2 * c + x) * 128 : (2 * c + x + 1) * 128] = rows
            both = mul(m_in[f], given[f, :, c * 256 : (c + 1) * 256])
            lifted.append(both[0:128] + both[128:256])
        for x in range(2):
            both = jnp.concatenate([v[:, x * 128 : (x + 1) * 128] for v in lifted], axis=1)
            s1[:, (2 * c + x) * 128 : (2 * c + x + 1) * 128] = mul3(tz_pair, split(both), NT)
        if c == 0:
            pl.semaphore_wait(barrier, 2 * (COUNT - 1))
        outward.append(
            start(c, "y", rows8(s1, chunks[c]), rows8(r1, chunks[c]), r1.at[pl.ds(0, 120), chunks[c]])
        )
        r1[own, c * 256 : (c + 1) * 256] = s1[own, c * 256 : (c + 1) * 256]
    for c in copies[5:]:
        c.wait()

    mode = iota((32, 128), 1)
    row32 = iota((32, 128), 0)
    t1 = exact(first_t[...], hot(mode // 4 == row32))
    t2f = exact(second_t[...], hot(mode // 2 % 2 + 2 * px == row32))
    t3f = exact(third_t[...], hot(mode % 2 + 2 * py == row32))
    tiles = []
    for r in range(8):
        for s in range(8):
            tiles.append(t3f * (t1[r : r + 1] * t2f[s : s + 1]))
    phi_pair = split(jnp.concatenate(tiles, axis=0))
    for a in range(16):
        core[:, a] = core_n[a].T
    kern[...] = mul3(split(core[...].reshape(256, 512)), phi_pair).reshape(16, 16, 128)
    spread_second[...] = exact(second_t[...], hot(iota((32, 2048), 1) // 64 == iota((32, 2048), 0)))
    high, low = split(maps[1].T)
    back_map[0] = high
    back_map[1] = low

    a1_pair = pair(a1)
    gathered = jnp.zeros((256, 128), F32)
    for c in range(4):
        outward[c].wait_recv()
        middle = mul3(a1_pair, split(r1[:, c * 256 : (c + 1) * 256]))
        turned = []
        for x in range(2):
            real = middle[0:64, x * 128 : (x + 1) * 128]
            imag = middle[64:128, x * 128 : (x + 1) * 128]
            parts = []
            for h in range(2):
                cosine, sine = tw[h, 0], tw[h, 1]
                parts += [cosine * real + sine * imag, cosine * imag - sine * real]
            turned.append(jnp.concatenate(parts, axis=0))
        high, low = split(jnp.concatenate(turned, axis=1))
        places = collect[c * 256 : (c + 1) * 256]
        gathered = gathered + (mul(high, places) + mul(low, places))
    s2[...] = gathered.reshape(2, 2, 8, 8, 128)
    across = start(4, "x", block(s2), slab(r2), r2.at[pl.ds(0, 15)])
    r2[px] = s2[lax.div(px, 8), :, lax.rem(px, 8)]

    across.wait_recv()
    middle = mul3(pair(a2), split(r2[...].reshape(256, 128)))
    parts = []
    for p in range(2):
        for f in range(2):
            real = middle[f * 64 : f * 64 + 64]
            imag = middle[128 + f * 64 : 128 + f * 64 + 64]
            for h in range(2):
                cosine, sine = tw[h, 0], tw[h, 1]
                parts.append(cosine * real + sine * imag if p == 0 else cosine * imag - sine * real)
    high, low = split(jnp.concatenate(parts, axis=0))
    ones = hot(iota((16, 128), 1) % 16 == iota((16, 128), 0)).astype(BF16)
    modes = mul(ones, high, NT) + mul(ones, low, NT)

    depth_mode = iota((1, 128), 1) % 2 + 2 * py
    scale = jnp.where(depth_mode == 0, 1.0, 2.0).astype(F32) * SCALE
    lifted = [modes[:, p * 256 : p * 256 + 128] for p in range(2)]
    back = [modes[:, p * 256 + 128 : p * 256 + 256] * scale for p in range(2)]
    mixed = [jnp.zeros((16, 128), F32) for p in range(2)]
    lifted_back = [jnp.zeros((16, 128), F32) for p in range(2)]
    for i in range(16):
        over_a = kern[:, i]
        over_b = kern[i]
        for p in range(2):
            mixed[p] = mixed[p] + over_a * lifted[p][i : i + 1]
            lifted_back[p] = lifted_back[p] + over_b * back[p][i : i + 1]
    modes = jnp.concatenate([mixed[0] * scale, lifted_back[0], mixed[1] * scale, lifted_back[1]], axis=1)

    opened = jnp.concatenate([modes] * 8, axis=0).T
    parts = []
    for p in range(2):
        for f in range(2):
            total = None
            for h in range(2):
                cosine, sine = tw[h, 0], tw[h, 1]
                real = opened[f * 128 + h * 64 : f * 128 + h * 64 + 64]
                imag = opened[256 + f * 128 + h * 64 : 256 + f * 128 + h * 64 + 64]
                term = cosine * real - sine * imag if p == 0 else sine * real + cosine * imag
                total = term if total is None else total + term
            parts.append(total)
    s3[...] = mul3(pair(a2t), split(jnp.concatenate(parts, axis=0))).reshape(16, 2, 8, 128)
    across = start(5, "x", slab(s3), block(r3), s3.at[pl.ds(0, 15)])
    r3[lax.div(px, 8), :, lax.rem(px, 8)] = s3[px]

    for b in range(16):
        grad[b] = lifted[0] * back[0][b : b + 1] + lifted[1] * back[1][b : b + 1]
    grad_pair = split(grad[...].reshape(256, 128))
    tiles = []
    for k in range(2):
        kept = hot(iota((8, 128), 1) // 2 % 2 == k) * t3f
        for r in range(8):
            tiles.append(kept * t1[r : r + 1])
    s5[...] = mul3(grad_pair, split(jnp.concatenate(tiles, axis=0)), NT).reshape(16, 16, 128)
    shares = start(6, "y", slab(s5), slab(r8), r8.at[pl.ds(0, 15)])
    r8[py] = s5[py]

    pulled = mul3(split(core[...].reshape(256, 512).T), grad_pair)
    by_first = []
    by_second = [jnp.zeros((8, 128), F32) for s in range(8)]
    by_third = jnp.zeros((8, 128), F32)
    for r in range(8):
        total = jnp.zeros((8, 128), F32)
        for s in range(8):
            tile = pulled[(r * 8 + s) * 8 : (r * 8 + s) * 8 + 8]
            total = total + tile * t2f[s : s + 1]
            by_second[s] = by_second[s] + tile * t1[r : r + 1]
        by_first.append(total)
        by_third = by_third + total * t1[r : r + 1]
    fold = hot(iota((8, 64), 1) // 8 == iota((8, 64), 0))
    first_rows8 = exact(fold, jnp.concatenate([t * t3f for t in by_first], axis=0))
    second_rows8 = exact(fold, jnp.concatenate([t * t3f for t in by_second], axis=0))
    row = iota((128, 128), 0)
    col = iota((128, 128), 1)
    factor_grads = (
        exact(first_rows8, hot(row // 4 == col))
        + exact(second_rows8, hot(row // 2 % 2 + 2 * px + 32 == col))
        + exact(by_third, hot(row % 2 + 2 * py + 64 == col))
    )

    across.wait_recv()
    back_pair = split(r3[...].reshape(256, 128))
    a1t_pair = pair(a1t)
    inward = []
    for c in range(4):
        places = spread[:, c * 256 : (c + 1) * 256]
        opened = mul(back_pair[0], places) + mul(back_pair[1], places)
        turned = []
        for x in range(2):
            parts = []
            for p in range(2):
                total = None
                for h in range(2):
                    cosine, sine = tw[h, 0], tw[h, 1]
                    real = opened[h * 128 : h * 128 + 64, x * 128 : (x + 1) * 128]
                    imag = opened[h * 128 + 64 : h * 128 + 128, x * 128 : (x + 1) * 128]
                    term = cosine * real - sine * imag if p == 0 else sine * real + cosine * imag
                    total = term if total is None else total + term
                parts.append(total)
            turned.append(jnp.concatenate(parts, axis=0))
        s4[:, c * 256 : (c + 1) * 256] = mul3(a1t_pair, split(jnp.concatenate(turned, axis=1)))
        inward.append(
            start(7 + c, "y", rows8(s4, chunks[c]), rows8(r4, chunks[c]), r4.at[pl.ds(0, 120), chunks[c]])
        )
        r4[own, c * 256 : (c + 1) * 256] = s4[own, c * 256 : (c + 1) * 256]

    sums = [jnp.zeros((512, 128), F32) for f in range(2)]
    for c in range(4):
        inward[c].wait_recv()
        if c == 1:
            column = start(11, "x", whole(s6), slab(r9), r9.at[pl.ds(0, 15)])
            r9[px] = s6[...]
        values = [[], []]
        for x in range(2):
            rows = r4[:, (2 * c + x) * 128 : (2 * c + x + 1) * 128].T
            both = mul3(split(rows), tz_pair)
            for f in range(2):
                values[f].append(split(both[:, (1 - f) * 128 : (2 - f) * 128]))
            grids[2 * c + x, 0], grids[2 * c + x, 1] = values[1][x]
        for f in range(2):
            rows = given[f, :, c * 256 : (c + 1) * 256]
            for h in range(2):
                sums[f] = sums[f] + mul(rows, jnp.concatenate([v[h] for v in values[f]], axis=1), NT)
        if c == 0:
            shares.wait_recv()
            total = r8[0]
            for q in range(1, 16):
                total = total + r8[q]
            s6[...] = total
    kept = hot(iota((512, 128), 0) % 8 == iota((512, 128), 1) // 16)
    sums = [jnp.sum((v * kept).reshape(64, 8, 128), axis=1) for v in sums]
    high, low = split(jnp.concatenate(sums, axis=0))
    ts[0:16] = mul(ones, high, NT) + mul(ones, low, NT)
    ts[16:24] = factor_grads
    tail = start(14, "y", whole(ts), slab(r5), r5.at[pl.ds(0, 15)])
    r5[py] = ts[...]

    back_maps = pair(back_map)

    def emit(x, carry):
        output[:, pl.ds(x, 1)] = mul3(back_maps, (grids[x, 0], grids[x, 1])).reshape(64, 1, 8, 128).astype(BF16)
        return carry

    lax.fori_loop(0, 4, emit, 0)

    column.wait_recv()
    totals = [jnp.zeros((16, 128), F32) for s in range(8)]
    for q in range(16):
        received = r9[q]
        for s in range(8):
            totals[s] = totals[s] + received * spread_second[s : s + 1, q * 128 : (q + 1) * 128]
    totals = [t + pltpu.roll(t, 64, 1) for t in totals]
    left = iota((16, 128), 1) < 64
    for u in range(4):
        s7[:, u * 128 : (u + 1) * 128] = jnp.where(left, totals[2 * u], totals[2 * u + 1])

    mine, chip = lax.rem(py, 2), lax.div(py, 2)
    core_parts = start(
        12, "y", whole(s7), lambda i: cg.at[mine, chip], cg.at[0, pl.ds(0, 7)], [p for p, o in zip(peers_y, FAR_FIRST_Y) if o[2] == 0]
    )
    cg[mine, chip] = s7[...]

    tail.wait_recv()
    total = r5[0]
    for q in range(1, 16):
        total = total + r5[q]
    t2[...] = total
    tail = start(15, "x", whole(t2), slab(small_h), small_h.at[pl.ds(0, 15)])
    done = [pltpu.make_async_copy(t2, small_h.at[px], loads.at[2])]
    done[0].start()
    lax.fori_loop(4, 8, emit, 0)
    done.append(pltpu.make_async_copy(output, output_h, loads.at[0]))
    done[1].start()
    core_parts.wait_recv()
    mate = [p for p, o in zip(peers_y, FAR_FIRST_Y) if o == (0, 0, 1)]
    core_parts = start(13, "y", lambda i: cg.at[mine], lambda i: packed_h.at[:, mine], cg.at[0], mate)
    done.append(pltpu.make_async_copy(cg.at[mine], packed_h.at[:, mine], loads.at[3]))
    done[-1].start()
    core_parts.wait_recv()
    tail.wait_recv()
    for c in waits:
        c.wait_send()
    for c in done:
        c.wait()


def finish(
    output_i, packed_i, small_i,
    output_h, core_h, in_h, out_h, first_h, second_h, third_h,
    output, packed, parts, core, grad_in, grad_out, grad_first, grad_second, grad_third, done,
):
    loads = (
        pltpu.make_async_copy(packed_i, packed, done.at[22]),
        pltpu.make_async_copy(small_i, parts, done.at[23]),
        pltpu.make_async_copy(output_i, output, done.at[24]),
    )
    for c in loads:
        c.start()
    loads[0].wait()
    copies = []
    for a in range(16):
        rows = packed[:, :, a].reshape(16, 512).T.reshape(8, 8, 8, 16)
        for s in range(8):
            for r in range(8):
                core[a, (r * 8 + s) * 8 : (r * 8 + s) * 8 + 8] = rows[s, r]
        copies.append(pltpu.make_async_copy(core.at[a], core_h.at[a], done.at[1 + a]))
        copies[-1].start()
        if a == 8:
            loads[1].wait()
            loads[2].wait()
            copies.append(pltpu.make_async_copy(output, output_h, done.at[0]))
            copies[-1].start()
    small = parts[0]
    for q in range(1, 16):
        small = small + parts[q]
    grad_in[...] = small[0:16, 0:64]
    grad_out[...] = small[0:16, 64:128]
    grad_first[...] = small[16:24, 0:32]
    grad_second[...] = small[16:24, 32:64]
    grad_third[...] = small[16:24, 64:96]
    pairs = ((grad_in, in_h), (grad_out, out_h), (grad_first, first_h), (grad_second, second_h), (grad_third, third_h))
    for i, (near, far) in enumerate(pairs):
        copies.append(pltpu.make_async_copy(near, far, done.at[17 + i]))
        copies[-1].start()
    for c in copies:
        c.wait()


def shards(field, cot, core, in_factor, out_factor, first, second, third):
    constants = [
        jnp.asarray(c)
        for c in (
            halves(depth_rows()),
            halves(second_rows()),
            halves(second_rows().T),
            halves(first_rows()),
            halves(first_rows().T),
            twiddles(),
            np.ascontiguousarray(gather_lanes().T),
            gather_lanes(),
        )
    ]
    operands = (
        field,
        cot,
        core.transpose(0, 2, 3, 4, 1).reshape(16, 512, 16),
        in_factor.T,
        out_factor.T,
        first.T,
        second.T,
        third.T,
        *constants,
    )
    hbm = pl.BlockSpec(memory_space=pltpu.HBM)
    scratch = [pltpu.VMEM(v.shape, v.dtype) for v in operands] + [
        pltpu.VMEM((16, 16, 512), F32),
        pltpu.VMEM((2, 256, 512), BF16),
        pltpu.VMEM((2, 512, 128), BF16),
        pltpu.VMEM((2, 512, 1024), BF16),
        pltpu.VMEM((128, 1024), F32),
        pltpu.VMEM((128, 1024), F32),
        pltpu.VMEM((2, 2, 8, 8, 128), F32),
        pltpu.VMEM((16, 2, 8, 128), F32),
        pltpu.VMEM((16, 2, 8, 128), F32),
        pltpu.VMEM((2, 2, 8, 8, 128), F32),
        pltpu.VMEM((128, 1024), F32),
        pltpu.VMEM((128, 1024), F32),
        pltpu.VMEM((16, 16, 128), F32),
        pltpu.VMEM((16, 16, 128), F32),
        pltpu.VMEM((16, 16, 128), F32),
        pltpu.VMEM((16, 16, 128), F32),
        pltpu.VMEM((16, 128), F32),
        pltpu.VMEM((16, 16, 128), F32),
        pltpu.VMEM((16, 512), F32),
        pltpu.VMEM((2, 8, 16, 512), F32),
        pltpu.VMEM((8, 2048), F32),
        pltpu.VMEM((8, 2, 128, 128), BF16),
        pltpu.VMEM((64, 8, 8, 128), BF16),
        pltpu.VMEM((24, 128), F32),
        pltpu.VMEM((16, 24, 128), F32),
        pltpu.VMEM((24, 128), F32),
        pltpu.SemaphoreType.DMA((16,)),
        pltpu.SemaphoreType.DMA((16,)),
        pltpu.SemaphoreType.DMA((len(operands),)),
    ]
    stages = (
        jax.ShapeDtypeStruct((64, 8, 8, 128), BF16),
        jax.ShapeDtypeStruct((8, 2, 16, 512), F32),
        jax.ShapeDtypeStruct((16, 24, 128), F32),
    )
    step = pl.pallas_call(
        kernel,
        out_shape=stages,
        in_specs=[hbm] * len(operands),
        out_specs=[hbm] * 3,
        scratch_shapes=scratch,
        compiler_params=pltpu.CompilerParams(
            collective_id=0, has_side_effects=True, vmem_limit_bytes=67043328
        ),
        name="tucker_step",
    )(*operands)
    shapes = ((64, 8, 8, 128), (16, 512, 16), (16, 64), (16, 64), (8, 32), (8, 32), (8, 32))
    output, grad_core, *grads = pl.pallas_call(
        finish,
        out_shape=tuple(jax.ShapeDtypeStruct(v, BF16 if i == 0 else F32) for i, v in enumerate(shapes)),
        in_specs=[hbm] * 3,
        out_specs=[hbm] * 7,
        scratch_shapes=[pltpu.VMEM(v.shape, v.dtype) for v in stages]
        + [pltpu.VMEM(v, F32) for v in shapes[1:]]
        + [pltpu.SemaphoreType.DMA((25,))],
        compiler_params=pltpu.CompilerParams(vmem_limit_bytes=67043328),
        name="finish",
    )(*step)
    grad_core = grad_core.reshape(16, 8, 8, 8, 16).transpose(0, 4, 1, 2, 3)
    return (output, grad_core, *[g.T for g in grads])


def solution(mesh):
    grid = P(None, "px", "py", None)
    return jax.shard_map(
        shards,
        mesh=mesh,
        in_specs=(grid, grid) + (P(),) * 6,
        out_specs=(grid,) + (P(),) * 6,
        check_vma=False,
    )
```

```python
import functools
import math

import jax
import jax.numpy as jnp
import numpy as np
from jax import lax
from jax.experimental import pallas as pl
from jax.experimental.pallas import tpu as pltpu
from jax.sharding import PartitionSpec as P

F32 = jnp.float32
BF16 = jnp.bfloat16
HIGHEST = lax.Precision.HIGHEST
MESH = pl.DeviceIdType.MESH
COUNT = 16
CELLS = 128
SCALE = 1.0 / (CELLS * CELLS * CELLS)
NN = ((1,), (0,))
FAR_FIRST_Y = sorted(
    ((x, y, c) for x in range(4) for y in range(2) for c in range(2) if x or y or c),
    key=lambda o: -(min(o[0], 4 - o[0]) + o[1]),
)
FAR_FIRST_X = sorted(
    ((z, y) for z in range(8) for y in range(2) if z or y),
    key=lambda o: -(min(o[0], 8 - o[0]) + 2 * o[1]),
)
NT = ((1,), (1,))


def halves(table):
    high = table.astype(np.float32).astype(jnp.bfloat16)
    low = (table - high.astype(np.float64)).astype(np.float32).astype(jnp.bfloat16)
    return np.stack([high, low])


def depth_rows():
    row = np.arange(128)[:, None]
    lane = np.arange(256)[None, :]
    mode = row // 8 * 2 + row % 2
    angle = 2.0 * math.pi / CELLS * (mode * (lane % 128) % CELLS)
    value = np.where(row // 2 % 2 == 0, np.cos(angle), -np.sin(angle))
    return np.where(row // 4 % 2 == lane // 128, value, 0.0)


def short_transform(rows, row_of, col_of):
    row = np.arange(rows)[:, None]
    col = np.arange(rows)[None, :]
    part_out, freq, rest_out = row_of(row)
    part_in, block, rest_in = col_of(col)
    angle = 2.0 * math.pi / 16 * (freq * block % 16)
    sine = np.where(part_out == 0, 1.0, -1.0) * np.sin(angle)
    value = np.where(part_out == part_in, np.cos(angle), sine)
    return np.where(rest_out == rest_in, value, 0.0)


def second_rows():
    return short_transform(
        128,
        lambda r: (r // 64, r // 4 % 16, r % 4),
        lambda c: (c // 2 % 2, c // 8, c // 4 % 2 * 2 + c % 2),
    )


def first_rows():
    return short_transform(
        256,
        lambda r: (r // 128, r // 4 % 16, r // 64 % 2 * 4 + r % 4),
        lambda c: (c // 8 % 2, c // 16, c // 2 % 2 * 4 + c // 4 % 2 * 2 + c % 2),
    )


def twiddles():
    row = np.arange(64)[:, None]
    lane = np.arange(128)[None, :]
    tables = []
    for high in range(2):
        angle = 2.0 * math.pi / CELLS * ((row // 4 - 16 * high) * (lane // 16))
        tables.append(np.stack([np.cos(angle), np.sin(angle)]))
    return np.stack(tables).astype(np.float32)


def gather_lanes():
    row = np.arange(1024)[:, None]
    lane = np.arange(128)[None, :]
    return ((row // 128 == lane // 16) & (row % 16 == lane % 16)).astype(np.float32).astype(jnp.bfloat16)


def split(value):
    high = value.astype(BF16)
    return high, (value - high.astype(F32)).astype(BF16)


def mul(a, b, dims=NN):
    return lax.dot_general(a, b, (dims, ((), ())), preferred_element_type=F32)


def exact(a, b, dims=NN):
    return lax.dot_general(a, b, (dims, ((), ())), precision=HIGHEST, preferred_element_type=F32)


def mul3(a, b, dims=NN):
    return mul(a[0], b[0], dims) + mul(a[0], b[1], dims) + mul(a[1], b[0], dims)


def pair(ref):
    return ref[0], ref[1]


def iota(shape, axis):
    return lax.broadcasted_iota(jnp.int32, shape, axis)


def hot(test):
    return jnp.where(test, 1.0, 0.0).astype(F32)


def kernel(
    field_h, cot_h, core_h, in_h, out_h, first_h, second_h, third_h,
    tz_h, a1_h, a1t_h, a2_h, a2t_h, tw_h, spread_h, collect_h,
    output_h, packed_h, small_h,
    field, cot, core_n, in_t, out_t, first_t, second_t, third_t,
    tz, a1, a1t, a2, a2t, tw, spread, collect, core,
    m_in, back_map, given, s1, r1, s2, r2, s3, r3, s4, r4,
    kern, grad, s5, r8, s6, r9, s7, cg, spread_second, grids, output, ts, r5, t2,
    send, recv, loads,
):
    px = lax.axis_index("px")
    py = lax.axis_index("py")
    barrier = pltpu.get_barrier_semaphore()

    def along_y(peer):
        return (px, peer)

    def along_x(peer):
        return (peer, py)

    staged = (
        (in_h, in_t), (out_h, out_t), (field_h, field), (cot_h, cot), (tz_h, tz),
        (first_h, first_t), (second_h, second_t), (third_h, third_t), (a1_h, a1), (tw_h, tw), (collect_h, collect),
        (core_h, core_n), (a2_h, a2), (a2t_h, a2t), (spread_h, spread), (a1t_h, a1t),
    )
    copies = [pltpu.make_async_copy(far, near, loads.at[i]) for i, (far, near) in enumerate(staged)]
    for c in copies:
        c.start()

    x_at = [lax.rem(lax.div(py, 4) + d, 4) * 4 for d in range(4)]
    y_at = [lax.rem(lax.rem(lax.div(py, 2), 2) + d, 2) * 2 for d in range(2)]
    core_at = [lax.rem(lax.rem(py, 2) + d, 2) for d in range(2)]
    z_at = [lax.rem(lax.div(px, 2) + d, 8) * 2 for d in range(8)]
    far_at = [lax.rem(lax.rem(px, 2) + d, 2) for d in range(2)]
    peers_y = [x_at[x] + y_at[y] + core_at[c] for x, y, c in FAR_FIRST_Y]
    peers_x = [z_at[z] + far_at[y] for z, y in FAR_FIRST_X]
    for peer in peers_x:
        pl.semaphore_signal(barrier, inc=1, device_id=along_x(peer), device_id_type=MESH)
    for peer in peers_y:
        pl.semaphore_signal(barrier, inc=1, device_id=along_y(peer), device_id_type=MESH)
    waits = []

    def start(phase, axis, source, target, every, some=None):
        me, device, peers = (py, along_y, some or peers_y) if axis == "y" else (px, along_x, peers_x)
        for peer in peers:
            pltpu.make_async_remote_copy(
                src_ref=source(peer),
                dst_ref=target(me),
                send_sem=send.at[phase],
                recv_sem=recv.at[phase],
                device_id=device(peer),
                device_id_type=MESH,
            ).start()
        total = pltpu.make_async_remote_copy(
            src_ref=every,
            dst_ref=every,
            send_sem=send.at[phase],
            recv_sem=recv.at[phase],
            device_id=device(peers[0]),
            device_id_type=MESH,
        )
        waits.append(total)
        return total

    def rows8(ref, lanes):
        return lambda i: ref.at[pl.ds(pl.multiple_of(i * 8, 8), 8), lanes]

    def slab(ref, *rest):
        return lambda i: ref.at[(i, *rest)] if rest else ref.at[i]

    def block(ref):
        return lambda i: ref.at[lax.div(i, 8), :, lax.rem(i, 8)]

    def whole(ref):
        return lambda i: ref

    chunks = [pl.ds(c * 256, 256) for c in range(4)]
    own = pl.ds(pl.multiple_of(py * 8, 8), 8)

    copies[0].wait()
    copies[1].wait()
    lane = iota((16, 512), 1)
    repeat = hot(iota((64, 512), 1) // 8 == iota((64, 512), 0))
    maps = []
    for f, factor in enumerate((in_t, out_t)):
        wide_factor = exact(factor[...], repeat)
        maps.append(jnp.concatenate([jnp.where(lane % 8 == y, wide_factor, 0.0) for y in range(8)], axis=0))
        high, low = split(maps[f])
        m_in[f, 0:128] = high
        m_in[f, 128:256] = low

    for c in copies[2:5]:
        c.wait()
    tz_pair = pair(tz)
    outward = []
    for c in range(4):
        lifted = []
        for f, source in enumerate((field, cot)):
            for x in range(2):
                rows = source[:, 2 * c + x].astype(F32).reshape(512, 128).astype(BF16)
                given[f, :, (2 * c + x) * 128 : (2 * c + x + 1) * 128] = rows
            both = mul(m_in[f], given[f, :, c * 256 : (c + 1) * 256])
            lifted.append(both[0:128] + both[128:256])
        for x in range(2):
            both = jnp.concatenate([v[:, x * 128 : (x + 1) * 128] for v in lifted], axis=1)
            s1[:, (2 * c + x) * 128 : (2 * c + x + 1) * 128] = mul3(tz_pair, split(both), NT)
        if c == 0:
            pl.semaphore_wait(barrier, 2 * (COUNT - 1))
        outward.append(
            start(c, "y", rows8(s1, chunks[c]), rows8(r1, chunks[c]), r1.at[pl.ds(0, 120), chunks[c]])
        )
        r1[own, c * 256 : (c + 1) * 256] = s1[own, c * 256 : (c + 1) * 256]
    for c in copies[5:]:
        c.wait()

    mode = iota((32, 128), 1)
    row32 = iota((32, 128), 0)
    t1 = exact(first_t[...], hot(mode // 4 == row32))
    t2f = exact(second_t[...], hot(mode // 2 % 2 + 2 * px == row32))
    t3f = exact(third_t[...], hot(mode % 2 + 2 * py == row32))
    tiles = []
    for r in range(8):
        for s in range(8):
            tiles.append(t3f * (t1[r : r + 1] * t2f[s : s + 1]))
    phi_pair = split(jnp.concatenate(tiles, axis=0))
    for a in range(16):
        core[:, a] = core_n[a].T
    kern[...] = mul3(split(core[...].reshape(256, 512)), phi_pair).reshape(16, 16, 128)
    spread_second[...] = exact(second_t[...], hot(iota((32, 2048), 1) // 64 == iota((32, 2048), 0)))
    high, low = split(maps[1].T)
    back_map[0] = high
    back_map[1] = low

    a1_pair = pair(a1)
    gathered = jnp.zeros((256, 128), F32)
    for c in range(4):
        outward[c].wait_recv()
        middle = mul3(a1_pair, split(r1[:, c * 256 : (c + 1) * 256]))
        turned = []
        for x in range(2):
            real = middle[0:64, x * 128 : (x + 1) * 128]
            imag = middle[64:128, x * 128 : (x + 1) * 128]
            parts = []
            for h in range(2):
                cosine, sine = tw[h, 0], tw[h, 1]
                parts += [cosine * real + sine * imag, cosine * imag - sine * real]
            turned.append(jnp.concatenate(parts, axis=0))
        high, low = split(jnp.concatenate(turned, axis=1))
        places = collect[c * 256 : (c + 1) * 256]
        gathered = gathered + (mul(high, places) + mul(low, places))
    s2[...] = gathered.reshape(2, 2, 8, 8, 128)
    across = start(4, "x", block(s2), slab(r2), r2.at[pl.ds(0, 15)])
    r2[px] = s2[lax.div(px, 8), :, lax.rem(px, 8)]

    across.wait_recv()
    middle = mul3(pair(a2), split(r2[...].reshape(256, 128)))
    parts = []
    for p in range(2):
        for f in range(2):
            real = middle[f * 64 : f * 64 + 64]
            imag = middle[128 + f * 64 : 128 + f * 64 + 64]
            for h in range(2):
                cosine, sine = tw[h, 0], tw[h, 1]
                parts.append(cosine * real + sine * imag if p == 0 else cosine * imag - sine * real)
    high, low = split(jnp.concatenate(parts, axis=0))
    ones = hot(iota((16, 128), 1) % 16 == iota((16, 128), 0)).astype(BF16)
    modes = mul(ones, high, NT) + mul(ones, low, NT)

    depth_mode = iota((1, 128), 1) % 2 + 2 * py
    scale = jnp.where(depth_mode == 0, 1.0, 2.0).astype(F32) * SCALE
    lifted = [modes[:, p * 256 : p * 256 + 128] for p in range(2)]
    back = [modes[:, p * 256 + 128 : p * 256 + 256] * scale for p in range(2)]
    mixed = [jnp.zeros((16, 128), F32) for p in range(2)]
    lifted_back = [jnp.zeros((16, 128), F32) for p in range(2)]
    for i in range(16):
        over_a = kern[:, i]
        over_b = kern[i]
        for p in range(2):
            mixed[p] = mixed[p] + over_a * lifted[p][i : i + 1]
            lifted_back[p] = lifted_back[p] + over_b * back[p][i : i + 1]
    modes = jnp.concatenate([mixed[0] * scale, lifted_back[0], mixed[1] * scale, lifted_back[1]], axis=1)

    opened = jnp.concatenate([modes] * 8, axis=0).T
    parts = []
    for p in range(2):
        for f in range(2):
            total = None
            for h in range(2):
                cosine, sine = tw[h, 0], tw[h, 1]
                real = opened[f * 128 + h * 64 : f * 128 + h * 64 + 64]
                imag = opened[256 + f * 128 + h * 64 : 256 + f * 128 + h * 64 + 64]
                term = cosine * real - sine * imag if p == 0 else sine * real + cosine * imag
                total = term if total is None else total + term
            parts.append(total)
    s3[...] = mul3(pair(a2t), split(jnp.concatenate(parts, axis=0))).reshape(16, 2, 8, 128)
    across = start(5, "x", slab(s3), block(r3), s3.at[pl.ds(0, 15)])
    r3[lax.div(px, 8), :, lax.rem(px, 8)] = s3[px]

    for b in range(16):
        grad[b] = lifted[0] * back[0][b : b + 1] + lifted[1] * back[1][b : b + 1]
    grad_pair = split(grad[...].reshape(256, 128))
    tiles = []
    for k in range(2):
        kept = hot(iota((8, 128), 1) // 2 % 2 == k) * t3f
        for r in range(8):
            tiles.append(kept * t1[r : r + 1])
    s5[...] = mul3(grad_pair, split(jnp.concatenate(tiles, axis=0)), NT).reshape(16, 16, 128)
    shares = start(6, "y", slab(s5), slab(r8), r8.at[pl.ds(0, 15)])
    r8[py] = s5[py]

    pulled = mul3(split(core[...].reshape(256, 512).T), grad_pair)
    by_first = []
    by_second = [jnp.zeros((8, 128), F32) for s in range(8)]
    by_third = jnp.zeros((8, 128), F32)
    for r in range(8):
        total = jnp.zeros((8, 128), F32)
        for s in range(8):
            tile = pulled[(r * 8 + s) * 8 : (r * 8 + s) * 8 + 8]
            total = total + tile * t2f[s : s + 1]
            by_second[s] = by_second[s] + tile * t1[r : r + 1]
        by_first.append(total)
        by_third = by_third + total * t1[r : r + 1]
    fold = hot(iota((8, 64), 1) // 8 == iota((8, 64), 0))
    first_rows8 = exact(fold, jnp.concatenate([t * t3f for t in by_first], axis=0))
    second_rows8 = exact(fold, jnp.concatenate([t * t3f for t in by_second], axis=0))
    row = iota((128, 128), 0)
    col = iota((128, 128), 1)
    factor_grads = (
        exact(first_rows8, hot(row // 4 == col))
        + exact(second_rows8, hot(row // 2 % 2 + 2 * px + 32 == col))
        + exact(by_third, hot(row % 2 + 2 * py + 64 == col))
    )

    across.wait_recv()
    back_pair = split(r3[...].reshape(256, 128))
    a1t_pair = pair(a1t)
    inward = []
    for c in range(4):
        places = spread[:, c * 256 : (c + 1) * 256]
        opened = mul(back_pair[0], places) + mul(back_pair[1], places)
        turned = []
        for x in range(2):
            parts = []
            for p in range(2):
                total = None
                for h in range(2):
                    cosine, sine = tw[h, 0], tw[h, 1]
                    real = opened[h * 128 : h * 128 + 64, x * 128 : (x + 1) * 128]
                    imag = opened[h * 128 + 64 : h * 128 + 128, x * 128 : (x + 1) * 128]
                    term = cosine * real - sine * imag if p == 0 else sine * real + cosine * imag
                    total = term if total is None else total + term
                parts.append(total)
            turned.append(jnp.concatenate(parts, axis=0))
        s4[:, c * 256 : (c + 1) * 256] = mul3(a1t_pair, split(jnp.concatenate(turned, axis=1)))
        inward.append(
            start(7 + c, "y", rows8(s4, chunks[c]), rows8(r4, chunks[c]), r4.at[pl.ds(0, 120), chunks[c]])
        )
        r4[own, c * 256 : (c + 1) * 256] = s4[own, c * 256 : (c + 1) * 256]

    shares.wait_recv()
    total = r8[0]
    for q in range(1, 16):
        total = total + r8[q]
    s6[...] = total

    sums = [jnp.zeros((512, 128), F32) for f in range(2)]
    for c in range(4):
        inward[c].wait_recv()
        if c == 0:
            column = start(11, "x", whole(s6), slab(r9), r9.at[pl.ds(0, 15)])
            r9[px] = s6[...]
        values = [[], []]
        for x in range(2):
            rows = r4[:, (2 * c + x) * 128 : (2 * c + x + 1) * 128].T
            both = mul3(split(rows), tz_pair)
            for f in range(2):
                values[f].append(split(both[:, (1 - f) * 128 : (2 - f) * 128]))
            grids[2 * c + x, 0], grids[2 * c + x, 1] = values[1][x]
        for f in range(2):
            rows = given[f, :, c * 256 : (c + 1) * 256]
            for h in range(2):
                sums[f] = sums[f] + mul(rows, jnp.concatenate([v[h] for v in values[f]], axis=1), NT)
    kept = hot(iota((512, 128), 0) % 8 == iota((512, 128), 1) // 16)
    sums = [jnp.sum((v * kept).reshape(64, 8, 128), axis=1) for v in sums]
    high, low = split(jnp.concatenate(sums, axis=0))
    ts[0:16] = mul(ones, high, NT) + mul(ones, low, NT)
    ts[16:24] = factor_grads
    tail = start(14, "y", whole(ts), slab(r5), r5.at[pl.ds(0, 15)])
    r5[py] = ts[...]

    back_maps = pair(back_map)

    def emit(x, carry):
        output[:, pl.ds(x, 1)] = mul3(back_maps, (grids[x, 0], grids[x, 1])).reshape(64, 1, 8, 128).astype(BF16)
        return carry

    column.wait_recv()
    totals = [jnp.zeros((16, 128), F32) for s in range(8)]
    for q in range(16):
        received = r9[q]
        for s in range(8):
            totals[s] = totals[s] + received * spread_second[s : s + 1, q * 128 : (q + 1) * 128]
    totals = [t + pltpu.roll(t, 64, 1) for t in totals]
    left = iota((16, 128), 1) < 64
    for u in range(4):
        s7[:, u * 128 : (u + 1) * 128] = jnp.where(left, totals[2 * u], totals[2 * u + 1])

    mine, chip = lax.rem(py, 2), lax.div(py, 2)
    core_parts = start(
        12, "y", whole(s7), lambda i: cg.at[mine, chip], cg.at[0, pl.ds(0, 7)], [p for p, o in zip(peers_y, FAR_FIRST_Y) if o[2] == 0]
    )
    cg[mine, chip] = s7[...]

    lax.fori_loop(0, 4, emit, 0)

    tail.wait_recv()
    total = r5[0]
    for q in range(1, 16):
        total = total + r5[q]
    t2[...] = total
    tail = start(15, "x", whole(t2), slab(small_h), small_h.at[pl.ds(0, 15)])
    done = [pltpu.make_async_copy(t2, small_h.at[px], loads.at[2])]
    done[0].start()
    lax.fori_loop(4, 8, emit, 0)
    done.append(pltpu.make_async_copy(output, output_h, loads.at[0]))
    done[1].start()
    core_parts.wait_recv()
    mate = [p for p, o in zip(peers_y, FAR_FIRST_Y) if o == (0, 0, 1)]
    core_parts = start(13, "y", lambda i: cg.at[mine], lambda i: packed_h.at[:, mine], cg.at[0], mate)
    done.append(pltpu.make_async_copy(cg.at[mine], packed_h.at[:, mine], loads.at[3]))
    done[-1].start()
    core_parts.wait_recv()
    tail.wait_recv()
    for c in waits:
        c.wait_send()
    for c in done:
        c.wait()


def finish(
    output_i, packed_i, small_i,
    output_h, core_h, in_h, out_h, first_h, second_h, third_h,
    output, packed, parts, core, grad_in, grad_out, grad_first, grad_second, grad_third, done,
):
    loads = (
        pltpu.make_async_copy(packed_i, packed, done.at[22]),
        pltpu.make_async_copy(small_i, parts, done.at[23]),
        pltpu.make_async_copy(output_i, output, done.at[24]),
    )
    for c in loads:
        c.start()
    loads[0].wait()
    copies = []
    for a in range(16):
        rows = packed[:, :, a].reshape(16, 512).T.reshape(8, 8, 8, 16)
        for s in range(8):
            for r in range(8):
                core[a, (r * 8 + s) * 8 : (r * 8 + s) * 8 + 8] = rows[s, r]
        copies.append(pltpu.make_async_copy(core.at[a], core_h.at[a], done.at[1 + a]))
        copies[-1].start()
        if a == 8:
            loads[1].wait()
            loads[2].wait()
            copies.append(pltpu.make_async_copy(output, output_h, done.at[0]))
            copies[-1].start()
    small = parts[0]
    for q in range(1, 16):
        small = small + parts[q]
    grad_in[...] = small[0:16, 0:64]
    grad_out[...] = small[0:16, 64:128]
    grad_first[...] = small[16:24, 0:32]
    grad_second[...] = small[16:24, 32:64]
    grad_third[...] = small[16:24, 64:96]
    pairs = ((grad_in, in_h), (grad_out, out_h), (grad_first, first_h), (grad_second, second_h), (grad_third, third_h))
    for i, (near, far) in enumerate(pairs):
        copies.append(pltpu.make_async_copy(near, far, done.at[17 + i]))
        copies[-1].start()
    for c in copies:
        c.wait()


def shards(field, cot, core, in_factor, out_factor, first, second, third):
    constants = [
        jnp.asarray(c)
        for c in (
            halves(depth_rows()),
            halves(second_rows()),
            halves(second_rows().T),
            halves(first_rows()),
            halves(first_rows().T),
            twiddles(),
            np.ascontiguousarray(gather_lanes().T),
            gather_lanes(),
        )
    ]
    operands = (
        field,
        cot,
        core.transpose(0, 2, 3, 4, 1).reshape(16, 512, 16),
        in_factor.T,
        out_factor.T,
        first.T,
        second.T,
        third.T,
        *constants,
    )
    hbm = pl.BlockSpec(memory_space=pltpu.HBM)
    scratch = [pltpu.VMEM(v.shape, v.dtype) for v in operands] + [
        pltpu.VMEM((16, 16, 512), F32),
        pltpu.VMEM((2, 256, 512), BF16),
        pltpu.VMEM((2, 512, 128), BF16),
        pltpu.VMEM((2, 512, 1024), BF16),
        pltpu.VMEM((128, 1024), F32),
        pltpu.VMEM((128, 1024), F32),
        pltpu.VMEM((2, 2, 8, 8, 128), F32),
        pltpu.VMEM((16, 2, 8, 128), F32),
        pltpu.VMEM((16, 2, 8, 128), F32),
        pltpu.VMEM((2, 2, 8, 8, 128), F32),
        pltpu.VMEM((128, 1024), F32),
        pltpu.VMEM((128, 1024), F32),
        pltpu.VMEM((16, 16, 128), F32),
        pltpu.VMEM((16, 16, 128), F32),
        pltpu.VMEM((16, 16, 128), F32),
        pltpu.VMEM((16, 16, 128), F32),
        pltpu.VMEM((16, 128), F32),
        pltpu.VMEM((16, 16, 128), F32),
        pltpu.VMEM((16, 512), F32),
        pltpu.VMEM((2, 8, 16, 512), F32),
        pltpu.VMEM((8, 2048), F32),
        pltpu.VMEM((8, 2, 128, 128), BF16),
        pltpu.VMEM((64, 8, 8, 128), BF16),
        pltpu.VMEM((24, 128), F32),
        pltpu.VMEM((16, 24, 128), F32),
        pltpu.VMEM((24, 128), F32),
        pltpu.SemaphoreType.DMA((16,)),
        pltpu.SemaphoreType.DMA((16,)),
        pltpu.SemaphoreType.DMA((len(operands),)),
    ]
    stages = (
        jax.ShapeDtypeStruct((64, 8, 8, 128), BF16),
        jax.ShapeDtypeStruct((8, 2, 16, 512), F32),
        jax.ShapeDtypeStruct((16, 24, 128), F32),
    )
    step = pl.pallas_call(
        kernel,
        out_shape=stages,
        in_specs=[hbm] * len(operands),
        out_specs=[hbm] * 3,
        scratch_shapes=scratch,
        compiler_params=pltpu.CompilerParams(
            collective_id=0, has_side_effects=True, vmem_limit_bytes=67043328
        ),
        name="tucker_step",
    )(*operands)
    shapes = ((64, 8, 8, 128), (16, 512, 16), (16, 64), (16, 64), (8, 32), (8, 32), (8, 32))
    output, grad_core, *grads = pl.pallas_call(
        finish,
        out_shape=tuple(jax.ShapeDtypeStruct(v, BF16 if i == 0 else F32) for i, v in enumerate(shapes)),
        in_specs=[hbm] * 3,
        out_specs=[hbm] * 7,
        scratch_shapes=[pltpu.VMEM(v.shape, v.dtype) for v in stages]
        + [pltpu.VMEM(v, F32) for v in shapes[1:]]
        + [pltpu.SemaphoreType.DMA((25,))],
        compiler_params=pltpu.CompilerParams(vmem_limit_bytes=67043328),
        name="finish",
    )(*step)
    grad_core = grad_core.reshape(16, 8, 8, 8, 16).transpose(0, 4, 1, 2, 3)
    return (output, grad_core, *[g.T for g in grads])


def solution(mesh):
    grid = P(None, "px", "py", None)
    return jax.shard_map(
        shards,
        mesh=mesh,
        in_specs=(grid, grid) + (P(),) * 6,
        out_specs=(grid,) + (P(),) * 6,
        check_vma=False,
    )
```
